256 devices in a mesh: section: 8 (over z), ep: 32 (over x, y, core).
Axes of the slice: x: 4, y: 4, z: 8, core: 2. Of those that a mesh axis runs over, the one named last changes fastest.
Arguments:
- saved_inputs: bfloat16 [8, 4096, 4096], P('section', 'ep'), may hold values from -6 to 6
- expert_ids: int32 [8, 4096, 2], P('section', 'ep'), may hold values from 0 to 7, as said below
- gate_weights: float32 [8, 4096, 2], P('section', 'ep'), may hold values from 0.1 to 0.9
- out_grad: bfloat16 [4096, 4096], P('ep', 'section'), may hold values from -6 to 6
- gate_w: bfloat16 [8, 7168, 4096], P('section', 'ep'), may hold values from -0.09375 to 0.09375
- up_w: bfloat16 [8, 7168, 4096], P('section', 'ep'), may hold values from -0.09375 to 0.09375
- down_w: bfloat16 [8, 7168, 4096], P('section', 'ep'), may hold values from -0.0625 to 0.0625
Outputs:
- input_grads: bfloat16 [8, 4096, 4096], P('section', 'ep')
- grad_gate: bfloat16 [8, 7168, 4096], P('section', 'ep')
- grad_up: bfloat16 [8, 7168, 4096], P('section', 'ep')
- grad_down: bfloat16 [8, 7168, 4096], P('section', 'ep')
The draws below stay inside these ranges and needn't reach their ends.
Inputs may be any that keep to these rules, and one draw needn't show every extreme that they name: `expert_ids`: the two ids of a token differ. Among the 128 tokens of one device in one layer, at most 4 name expert 0, and in every layer some device's tokens name it exactly 4 times.
All inputs are finite; a program needn't handle non-finite values.
Results may differ from the reference program's by a relative error of at most 0.0058.
Values may be sent and summed in bfloat16 or wider, within the bound.
A program may use at most 128 MiB of HBM per device.

```python
import jax
import jax.numpy as jnp
from jax import lax

D = 4096
EXPERTS = 8
TOK_DEV = 128
CAP = 4
FFW = 7168
SECTIONS = 8
TOKENS = 4096
N_EP = 32


def draw_expert_ids(key, part):
    groups = TOKENS // TOK_DEV
    blocks = SECTIONS * groups
    keys = jax.random.split(key, 7)
    first_count = jax.random.randint(keys[0], (SECTIONS, groups), 1, CAP + 1)
    second_count = jax.random.randint(keys[1], (SECTIONS, groups), 1, CAP + 1)
    counts = jnp.minimum(first_count, second_count)
    fullest = jax.random.randint(keys[2], (SECTIONS, 1), 0, groups)
    counts = jnp.where(jnp.arange(groups)[None, :] == fullest, CAP, counts).reshape(blocks, 1)
    ranks = jax.vmap(lambda block_key: jax.random.permutation(block_key, TOK_DEV))(jax.random.split(keys[3], blocks))
    is_live = ranks < counts
    other_first = jax.random.randint(keys[4], (blocks, TOK_DEV), 1, EXPERTS)
    other_second = jax.random.randint(keys[5], (blocks, TOK_DEV), 1, EXPERTS - 1)
    other_second = other_second + (other_second >= other_first).astype(jnp.int32)
    which_side = jax.random.randint(keys[6], (blocks, TOK_DEV), 0, 2)
    id_zero = jnp.where(is_live, jnp.where(which_side == 0, 0, other_first), other_first)
    id_one = jnp.where(is_live, jnp.where(which_side == 0, other_first, 0), other_second)
    return jnp.stack([id_zero, id_one], -1).reshape(SECTIONS, TOKENS, 2).astype(jnp.int32)


def steps_of(key, shape, cuts, least, top_value):
    level, own = 1.0, jax.random.fold_in(key, 6)
    for dim, blocks in cuts:
        draws = jnp.exp(jax.random.uniform(jax.random.fold_in(own, dim), (blocks,), jnp.float32, least / len(cuts), top_value / len(cuts)))
        level = level * jnp.repeat(draws, shape[dim] // blocks).reshape([-1 if axis == dim else 1 for axis in range(len(shape))])
    return level


def gaussian(own_key, extent, scale, limit, cuts=(), held_as=jnp.bfloat16):
    values = scale * jax.random.normal(own_key, extent, jnp.float32)
    if cuts:
        values = values * steps_of(own_key, extent, cuts, -0.22, 0.18)
    return jnp.clip(values, -limit, limit).astype(held_as)


def setup_inputs(seed: int = 0) -> dict:
    key_list = jax.random.split(jax.random.key(seed), 8)
    return {
        "saved_inputs": gaussian(key_list[0], (SECTIONS, TOKENS, D), 1.0, 6.0, ((0, 8), (1, 32))),
        "expert_ids": draw_expert_ids(jax.random.fold_in(key_list[7], 71), 0),
        "gate_weights": jnp.clip(0.1 + 0.79999997 * jax.random.uniform(key_list[2], (SECTIONS, TOKENS, 2), jnp.float32) ** steps_of(key_list[2], (SECTIONS, TOKENS, 2), ((0, 8), (1, 32)), -0.2, 0.2), 0.1, 0.9),
        "out_grad": gaussian(key_list[3], (TOKENS, D), 1.0, 6.0, ((0, 32), (1, 8))),
        "gate_w": gaussian(key_list[4], (SECTIONS, FFW, D), D ** -0.5, 0.09375, ((0, 8), (1, 32))),
        "up_w": gaussian(key_list[5], (SECTIONS, FFW, D), D ** -0.5, 0.09375, ((0, 8), (1, 32))),
        "down_w": gaussian(key_list[6], (SECTIONS, FFW, D), FFW ** -0.5, 0.0625, ((0, 8), (1, 32))),
    }


def reference(saved_inputs, expert_ids, gate_weights, out_grad, gate_w, up_w, down_w):
    device_of = (jnp.arange(TOKENS, dtype=jnp.int32) // TOK_DEV).astype(jnp.int32)

    def section_backward(upstream, operands):
        tokens, routes, gate_share, w_gate, w_up, w_down = operands
        is_live = routes == 0
        live_count = jnp.sum(is_live.astype(jnp.int32), axis=1).astype(jnp.int32)
        pair_weight = jnp.sum(jnp.where(is_live, gate_share, 0.0), axis=1)
        per_device = live_count.reshape(N_EP, TOK_DEV)
        slot_index = (jnp.cumsum(per_device, axis=1) - per_device).reshape(TOKENS).astype(jnp.int32)
        target = (device_of * (CAP + 1) + jnp.where(live_count == 1, slot_index, CAP)).astype(jnp.int32)

        def pack_rows(row_data):
            buffer = jnp.zeros((N_EP * (CAP + 1), D), row_data.dtype).at[target].set(row_data)
            return buffer.reshape(N_EP, CAP + 1, D)[:, :CAP].reshape(N_EP * CAP, D)

        scaled = (pair_weight[:, None] * upstream.astype(jnp.float32)).astype(jnp.bfloat16)
        x_rows = pack_rows(tokens)
        y_rows = pack_rows(scaled)
        gate_pre = jnp.dot(x_rows, w_gate.T, preferred_element_type=jnp.float32)
        up_pre = jnp.dot(x_rows, w_up.T, preferred_element_type=jnp.float32)
        sigmoid_gate = jax.nn.sigmoid(gate_pre)
        activated = gate_pre * sigmoid_gate
        hidden = (activated * up_pre).astype(jnp.bfloat16)
        grad_hidden = jnp.dot(y_rows, w_down.T, preferred_element_type=jnp.float32)
        d_up = (grad_hidden * activated).astype(jnp.bfloat16)
        d_gate = (grad_hidden * up_pre * sigmoid_gate * (1.0 + gate_pre * (1.0 - sigmoid_gate))).astype(jnp.bfloat16)
        back_rows = (jnp.dot(d_gate, w_gate, preferred_element_type=jnp.float32)
                     + jnp.dot(d_up, w_up, preferred_element_type=jnp.float32))
        padded = jnp.concatenate([back_rows.reshape(N_EP, CAP, D),
                                  jnp.zeros((N_EP, 1, D), back_rows.dtype)], 1).reshape(N_EP * (CAP + 1), D)
        input_grad = (upstream.astype(jnp.float32) + padded[target]).astype(jnp.bfloat16)
        grad_gate = jnp.dot(d_gate.T, x_rows, preferred_element_type=jnp.float32).astype(jnp.bfloat16)
        grad_up = jnp.dot(d_up.T, x_rows, preferred_element_type=jnp.float32).astype(jnp.bfloat16)
        grad_down = jnp.dot(hidden.T, y_rows, preferred_element_type=jnp.float32).astype(jnp.bfloat16)
        return input_grad, (input_grad, grad_gate, grad_up, grad_down)

    final_grad, outputs = lax.scan(section_backward, out_grad,
                                   (saved_inputs, expert_ids, gate_weights, gate_w, up_w, down_w), reverse=True)
    return (outputs[0], outputs[1], outputs[2], outputs[3])
```

```python
import functools

import jax
import jax.numpy as jnp
from jax import lax
from jax.experimental import pallas as pl
from jax.experimental.pallas import tpu as pltpu
from jax.sharding import PartitionSpec as P

MESH = pl.DeviceIdType.MESH
CAP = 4
NX, NY = 4, 4
CHIPS = NX * NY
QUARTERS = 4
ROWS = QUARTERS * CAP
MARK = 128
BF, F32 = jnp.bfloat16, jnp.float32


def iota(shape, dim):
    return lax.broadcasted_iota(jnp.int32, shape, dim)


def rows_at(index, size):
    return pl.ds(pl.multiple_of(index * size, size), size)


def swap_matrix():
    i, m = iota((64, 64), 0), iota((64, 64), 1)
    swapped = (lax.rem(lax.div(m, 4), 4) * 16) + (lax.div(m, 16) * 4) + lax.rem(m, 4)
    return jnp.where(i == swapped, 1.0, 0.0).astype(BF)


def nt(a, b):
    return lax.dot_general(a, b, (((1,), (1,)), ((), ())), preferred_element_type=F32)


def nn(a, b):
    return lax.dot_general(a, b, (((1,), (0,)), ((), ())), preferred_element_type=F32)


class Place:
    def __init__(self):
        self.s = lax.axis_index("section")
        self.sections = lax.axis_size("section")
        ep = lax.axis_index("ep")
        self.core = lax.rem(ep, 2)
        self.chip = lax.div(ep, 2)
        self.x = lax.div(self.chip, NY)
        self.y = lax.rem(self.chip, NY)
        self.partner = {"ep": self.chip * 2 + 1 - self.core}

    def ahead(self, k):
        i, j = lax.div(k, NY), lax.rem(k, NY)
        return lax.rem(self.x + i, NX) * NY + lax.rem(self.y + j, NY)

    def behind(self, k):
        i, j = lax.div(k, NY), lax.rem(k, NY)
        return lax.rem(self.x + NX - i, NX) * NY + lax.rem(self.y + NY - j, NY)

    def peer(self, chip):
        return {"ep": chip * 2 + self.core}

    def block(self, core, chip):
        return rows_at(core * CHIPS + chip, ROWS)


def remote(src, dst, send, recv, device):
    return pltpu.make_async_remote_copy(
        src_ref=src, dst_ref=dst, send_sem=send, recv_sem=recv, device_id=device, device_id_type=MESH
    )


def each(lo, hi, body):
    lax.fori_loop(lo, hi, lambda k, carry: (body(k), carry)[1], 0)


def gather_start(at, own, buf, send, recv):
    mine = at.block(at.core, at.chip)

    def go(k):
        remote(own, buf.at[mine], send.at[k], recv.at[k], at.peer(at.ahead(k))).start()

    each(1, CHIPS, go)
    remote(own, buf.at[mine], send.at[0], recv.at[0], at.partner).start()
    buf[mine, :] = own[...]


def gather_finish(at, own, buf, send, recv, relay_send, relay_recv):
    def forward(k):
        piece = at.block(at.core, at.behind(k))
        remote(own, buf.at[piece], send.at[k], recv.at[k], at.partner).wait_recv()
        remote(buf.at[piece], buf.at[piece], relay_send.at[k], relay_recv.at[k], at.partner).start()

    each(1, CHIPS, forward)
    other = at.block(1 - at.core, at.chip)
    remote(own, buf.at[other], send.at[0], recv.at[0], at.partner).wait_recv()

    def take(k):
        piece = at.block(1 - at.core, at.behind(k))
        remote(buf.at[piece], buf.at[piece], relay_send.at[k], relay_recv.at[k], at.partner).wait_recv()

    each(1, CHIPS, take)


def gather_drain(at, own, buf, send, recv, relay_send, relay_recv):
    def drain(k):
        remote(own, buf.at[at.block(at.core, at.chip)], send.at[k], recv.at[k], at.partner).wait_send()

    each(0, CHIPS, drain)

    def drain_relay(k):
        piece = at.block(at.core, at.behind(k))
        remote(buf.at[piece], buf.at[piece], relay_send.at[k], relay_recv.at[k], at.partner).wait_send()

    each(1, CHIPS, drain_relay)


def to_rows(buf, nat, width):
    swap = swap_matrix()

    def one(j):
        tile = nn(swap, buf[rows_at(j, 64), :width]).astype(BF)
        for q in range(QUARTERS):
            nat[rows_at(j, ROWS), q * width : (q + 1) * width] = tile[q * ROWS : (q + 1) * ROWS]

    each(0, 2 * CHIPS // 4, one)


def project(nat, weight, width):
    def step(q, acc):
        cols = rows_at(q, width)
        return acc + nt(nat[:, cols], weight[:, cols])

    return lax.fori_loop(0, QUARTERS, step, jnp.zeros((nat.shape[0], weight.shape[0]), F32))


def one_round(at, r, width, upstream, yown, ybuf, ynat, stack, pbuf, drecv, sbuf, rbuf, rown, rstack,
              wg, wu, wd, coef_up, coef_gate, dg, du, sems, before_rows=None, after_gather=None, weights_ready=None):
    (ag_s, ag_r, rel_s, rel_r, dd_s, dd_r, rs_s, rs_r, z_s, z_r) = sems
    ag = (at, yown.at[r], ybuf.at[r], ag_s.at[r], ag_r.at[r], rel_s.at[r], rel_r.at[r])
    gather_start(*ag[:5])
    if before_rows is not None:
        before_rows()
    gather_finish(*ag)
    if after_gather is not None:
        after_gather()
    to_rows(ybuf.at[r], ynat, width)
    if weights_ready is not None:
        weights_ready()
    grad_hidden = project(ynat, wd, width)
    du[...] = (grad_hidden * coef_up[...]).astype(BF)
    dg[...] = (grad_hidden * coef_gate[...]).astype(BF)

    def back(q):
        cols = rows_at(q, width)
        value = (nn(dg[...], wg[:, cols]) + nn(du[...], wu[:, cols])).astype(BF)
        for j in range(2 * CHIPS // 4):
            stack[rows_at(j * QUARTERS + q, ROWS), :] = value[j * ROWS : (j + 1) * ROWS]

    each(0, QUARTERS, back)
    swap = swap_matrix()

    def to_partner(jj):
        j = lax.rem(at.x + jj, NX)
        part = rows_at(j, 64)
        pbuf[r, part, :] = nn(swap, stack[rows_at((1 - at.core) * NX + j, 64), :]).astype(BF)
        remote(pbuf.at[r, part], drecv.at[r, part], dd_s.at[r, jj], dd_r.at[r, jj], at.partner).start()

    each(0, NX, to_partner)

    def to_homes(jj):
        j = lax.rem(at.x + jj, NX)
        part = rows_at(j, 64)
        mine = nn(swap, stack[rows_at(at.core * NX + j, 64), :])
        remote(pbuf.at[r, part], drecv.at[r, part], dd_s.at[r, jj], dd_r.at[r, jj], at.partner).wait_recv()
        sbuf[r, part, :] = (mine + drecv[r, part, :].astype(F32)).astype(BF)

        def send(m):
            k = jj * NY + m

            @pl.when(k > 0)
            def _():
                chip = at.ahead(k)
                remote(sbuf.at[r, rows_at(chip, ROWS)], rbuf.at[r, rows_at(k, ROWS)], rs_s.at[r, k], rs_r.at[r, k],
                       at.peer(chip)).start()

        each(0, NY, send)

    each(0, NX, to_homes)

    def add(k, acc):
        here = rows_at(k, ROWS)
        remote(sbuf.at[r, here], rbuf.at[r, here], rs_s.at[r, k], rs_r.at[r, k], at.partner).wait_recv()
        return acc + rbuf[r, here, :].astype(F32)

    total = lax.fori_loop(1, CHIPS, add, sbuf[r, rows_at(at.chip, ROWS), :].astype(F32))
    row = (upstream() + total).astype(BF)
    rown[r] = row
    mine = rows_at(at.s, ROWS)
    rstack[r, mine, :] = row

    def down(d):
        @pl.when(at.s >= d)
        def _():
            remote(rown.at[r], rstack.at[r, mine], z_s.at[r, d], z_r.at[r, d], {"section": at.s - d}).start()

    each(1, at.sections, down)

    def up(d):
        @pl.when(at.s + d < at.sections)
        def _():
            remote(rown.at[r], rstack.at[r, rows_at(at.s + d, ROWS)], z_s.at[r, d], z_r.at[r, d],
                   {"section": at.s + d}).wait_recv()

    each(1, at.sections, up)


def round_drain(at, r, yown, ybuf, pbuf, drecv, sbuf, rbuf, rown, rstack, sems):
    (ag_s, ag_r, rel_s, rel_r, dd_s, dd_r, rs_s, rs_r, z_s, z_r) = sems
    gather_drain(at, yown.at[r], ybuf.at[r], ag_s.at[r], ag_r.at[r], rel_s.at[r], rel_r.at[r])

    def drain_partner(jj):
        part = rows_at(jj, 64)
        remote(pbuf.at[r, part], drecv.at[r, part], dd_s.at[r, jj], dd_r.at[r, jj], at.partner).wait_send()

    each(0, NX, drain_partner)

    def drain_homes(k):
        here = rows_at(k, ROWS)
        remote(sbuf.at[r, here], rbuf.at[r, here], rs_s.at[r, k], rs_r.at[r, k], at.partner).wait_send()

    each(1, CHIPS, drain_homes)

    def drain_z(d):
        @pl.when(at.s >= d)
        def _():
            remote(rown.at[r], rstack.at[r, rows_at(at.s, ROWS)], z_s.at[r, d], z_r.at[r, d],
                   {"section": at.s - d}).wait_send()

    each(1, at.sections, drain_z)


def signal_to(device):
    pl.semaphore_signal(pltpu.get_barrier_semaphore(), inc=1, device_id=device, device_id_type=MESH)


def first_kernel(tok_ref, w_ref, tokens_hbm, og_hbm, wg_hbm, wu_hbm, wd_hbm,
                 u_out, base0_out, sel_out, cu_out, cg_out, hid_out, dg_out, du_out, r_out, level_out, ftok_out,
                 xnat_hbm, ynat_hbm, base_hbm,
                 tokv, ogv, wg, wu, wd, xown, xbuf, xnat, tokall, psend, precv, base,
                 yown, ybuf, ynat, stack, pbuf, drecv, sbuf, rbuf, rown, rstack,
                 loc, x_s, x_r, xrel_s, xrel_r, id_s, id_r, pc_s, pc_r, bs_s, bs_r, *sems):
    at = Place()
    width = u_out.shape[1]
    s, sections = at.s, at.sections
    half = ogv.shape[1]

    load_tokens = pltpu.make_async_copy(tokens_hbm, tokv, loc.at[0])
    load_og = pltpu.make_async_copy(og_hbm, ogv, loc.at[1])
    load_g = pltpu.make_async_copy(wg_hbm, wg, loc.at[2])
    load_u = pltpu.make_async_copy(wu_hbm, wu, loc.at[3])
    load_d = pltpu.make_async_copy(wd_hbm, wd, loc.at[4])
    for load in (load_tokens, load_og, load_g, load_u, load_d):
        load.start()

    rstack[...] = jnp.zeros_like(rstack)

    def greet(k):
        signal_to(at.peer(at.ahead(k)))

    each(1, CHIPS, greet)
    signal_to(at.partner)

    def greet_z(d):
        signal_to({"section": lax.rem(s + d, sections)})

    each(1, sections, greet_z)

    mine_z = rows_at(s, ROWS)
    pl.semaphore_wait(pltpu.get_barrier_semaphore(), CHIPS + sections - 1)

    def send_ids(d):
        remote(tok_ref, tokall.at[mine_z], id_s.at[d], id_r.at[d], {"section": lax.rem(s + d, sections)}).start()

    each(1, sections, send_ids)
    tokall[mine_z, :] = tok_ref[...]

    load_tokens.wait()
    lane16, row16 = iota((ROWS, 128), 1), iota((ROWS, 128), 0)
    hit = tok_ref[...] == lane16
    block = jnp.zeros((ROWS, width), F32)
    for q in range(QUARTERS):
        select = jnp.where(hit & (lax.div(row16, CAP) == q), 1.0, 0.0).astype(BF)
        block = block + nn(select, tokv[:, q * width : (q + 1) * width])
    xown[...] = block.astype(BF)
    xg = (at, xown, xbuf, x_s, x_r, xrel_s, xrel_r)
    gather_start(*xg[:5])

    load_og.wait()

    def wait_ids(d):
        source = lax.rem(s + sections - d, sections)
        remote(tok_ref, tokall.at[rows_at(source, ROWS)], id_s.at[d], id_r.at[d], at.partner).wait_recv()

    each(1, sections, wait_ids)
    tok = tokall[...]
    row, lane = iota((128, 128), 0), iota((128, 128), 1)
    pick = (tok == lane) & (lax.rem(lax.div(row, CAP), QUARTERS) == lax.div(s, 2))
    psend[...] = nn(jnp.where(pick, 1.0, 0.0).astype(BF), ogv[...]).astype(BF)

    def send_piece(d):
        to = lax.rem(s + d, sections)
        remote(psend.at[rows_at(to, ROWS)], precv.at[mine_z], pc_s.at[d], pc_r.at[d], {"section": to}).start()

    each(1, sections, send_piece)
    precv[mine_z, :] = psend[mine_z, :]

    tok_f = tok.astype(F32)
    other = tok_f.T
    layer_r, layer_l = lax.div(row, ROWS), lax.div(lane, ROWS)
    same = (tok_f == other) & (tok_f >= 0.0) & (lax.rem(lax.div(row, CAP), QUARTERS) == lax.rem(lax.div(lane, CAP), QUARTERS))
    above = jnp.where(same & (layer_l > layer_r), 1.0, 0.0)
    level_r = jnp.sum(above, axis=1, keepdims=True)
    level_l = jnp.sum(jnp.where(same & (layer_r > layer_l), 1.0, 0.0), axis=0, keepdims=True)
    chosen = jnp.where(level_l == level_r - 1.0, above, 0.0)
    own_row = layer_r == s
    take = jnp.where(iota((ROWS, 128), 1) == iota((ROWS, 128), 0) + s * ROWS, 1.0, 0.0).astype(BF)
    select_up = nn(take, chosen.astype(BF))
    level_own = nn(take, jnp.broadcast_to(level_r, (128, 128)).astype(BF))
    sel_out[...] = select_up.astype(BF)
    later = jnp.sum(jnp.where(same & (layer_r < layer_l) & (layer_r >= s), 1.0, 0.0), axis=0, keepdims=True)
    tok_l = jnp.max(other, axis=0, keepdims=True)
    lane1 = iota((1, 128), 1)
    ftok = jnp.where((later == 0.0) & (lax.div(lane1, ROWS) >= s), tok_l, -1.0)
    ftok_out[...] = jnp.broadcast_to(ftok, ftok_out.shape)
    deepest = jnp.max(level_r, axis=0, keepdims=True)

    def wait_piece(d):
        source = lax.rem(s + sections - d, sections)
        remote(psend.at[mine_z], precv.at[rows_at(source, ROWS)], pc_s.at[d], pc_r.at[d], at.partner).wait_recv()

    each(1, sections, wait_piece)

    for h in range(2):
        total = jnp.zeros((ROWS, half), F32)
        for p in range(h, 8, 2):
            total = total + precv[p * ROWS : (p + 1) * ROWS, :].astype(F32)
        base[:, h * half : (h + 1) * half] = total
    root = level_own[:, :1] == 0.0
    base0_out[...] = jnp.where(root, base[...], 0.0).astype(BF)
    weight = w_ref[:, :1]
    yown[0, :, :width] = (weight * base[...]).astype(BF)
    yown[0, :, width:] = jnp.broadcast_to(deepest, (ROWS, MARK)).astype(BF)

    def send_base():
        def go(d):
            to = lax.rem(s + d, sections)
            remote(ogv, base_hbm.at[:, rows_at(s, half)], bs_s.at[d], bs_r.at[d], {"section": to}).start()

        each(1, sections, go)
        pltpu.make_async_copy(ogv, base_hbm.at[:, rows_at(s, half)], loc.at[5]).start()

    def activations():
        send_base()
        gather_finish(*xg)
        to_rows(xbuf, xnat, width)
        pltpu.make_async_copy(xnat, xnat_hbm, loc.at[6]).start()
        load_g.wait()
        load_u.wait()
        gate = project(xnat, wg, width)
        up = project(xnat, wu, width)
        sig = 1.0 / (1.0 + jnp.exp(-gate))
        act = gate * sig
        hid_out[...] = (act * up).astype(BF)
        cu_out[...] = act
        cg_out[...] = up * sig * (1.0 + gate * (1.0 - sig))

    def read_level():
        marks = ybuf[0, :, width : width + MARK].astype(F32)
        level = jnp.max(jnp.max(marks, axis=0, keepdims=True), axis=1, keepdims=True)
        level_out[...] = jnp.broadcast_to(level, level_out.shape).astype(jnp.int32)

    shared = (yown, ybuf, ynat, stack, pbuf, drecv, sbuf, rbuf, rown, rstack, wg, wu, wd, cu_out, cg_out, dg_out, du_out, sems)
    one_round(at, 0, width, lambda: base[...], *shared, before_rows=activations, after_gather=read_level,
              weights_ready=load_d.wait)

    def follow(r):
        return nn(sel_out[...], rstack[r]) + base0_out[...].astype(F32)

    u_out[...] = follow(0).astype(BF)
    yown[1, :, :width] = (weight * u_out[...].astype(F32)).astype(BF)
    yown[1, :, width:] = jnp.zeros((ROWS, MARK), BF)
    one_round(at, 1, width, lambda: u_out[...].astype(F32), *shared)
    out_y = pltpu.make_async_copy(ynat, ynat_hbm, loc.at[7])
    out_y.start()
    u_out[...] = follow(1).astype(BF)
    r_out[...] = rstack[1]

    gather_drain(*xg)

    def drain_z(d):
        to = lax.rem(s + d, sections)
        source = lax.rem(s + sections - d, sections)
        remote(tok_ref, tokall.at[mine_z], id_s.at[d], id_r.at[d], at.partner).wait_send()
        remote(psend.at[rows_at(to, ROWS)], precv.at[mine_z], pc_s.at[d], pc_r.at[d], at.partner).wait_send()
        into = remote(ogv, base_hbm.at[:, rows_at(source, half)], bs_s.at[d], bs_r.at[d], at.partner)
        into.wait_send()
        into.wait_recv()

    each(1, sections, drain_z)
    for r in range(2):
        round_drain(at, r, yown, ybuf, pbuf, drecv, sbuf, rbuf, rown, rstack, sems)
    pltpu.make_async_copy(ogv, base_hbm.at[:, rows_at(s, half)], loc.at[5]).wait()
    pltpu.make_async_copy(xnat, xnat_hbm, loc.at[6]).wait()
    out_y.wait()


def next_kernel(u_ref, w_ref, base0_ref, sel_ref, cu_ref, cg_ref, wg_hbm, wu_hbm, wd_hbm,
                u_out, dg_out, du_out, r_out, ynat_hbm,
                wg, wu, wd, yown, ybuf, ynat, stack, pbuf, drecv, sbuf, rbuf, rown, rstack, loc, *sems):
    at = Place()
    width = u_out.shape[1]
    load_g = pltpu.make_async_copy(wg_hbm, wg, loc.at[0])
    load_u = pltpu.make_async_copy(wu_hbm, wu, loc.at[1])
    load_d = pltpu.make_async_copy(wd_hbm, wd, loc.at[2])
    for load in (load_d, load_g, load_u):
        load.start()

    rstack[...] = jnp.zeros_like(rstack)

    def greet(k):
        signal_to(at.peer(at.ahead(k)))

    each(1, CHIPS, greet)
    signal_to(at.partner)

    def greet_z(d):
        @pl.when(at.s + d < at.sections)
        def _():
            signal_to({"section": at.s + d})

    each(1, at.sections, greet_z)
    yown[0, :, :width] = (w_ref[:, :1] * u_ref[...].astype(F32)).astype(BF)
    yown[0, :, width:] = jnp.zeros((ROWS, MARK), BF)
    pl.semaphore_wait(pltpu.get_barrier_semaphore(), CHIPS + at.s)

    def loaded():
        for load in (load_d, load_g, load_u):
            load.wait()

    one_round(at, 0, width, lambda: u_ref[...].astype(F32), yown, ybuf, ynat, stack, pbuf, drecv, sbuf, rbuf, rown, rstack,
              wg, wu, wd, cu_ref, cg_ref, dg_out, du_out, sems, weights_ready=loaded)
    out_y = pltpu.make_async_copy(ynat, ynat_hbm, loc.at[3])
    out_y.start()
    u_out[...] = (nn(sel_ref[...], rstack[0]) + base0_ref[...].astype(F32)).astype(BF)
    r_out[...] = rstack[0]
    round_drain(at, 0, yown, ybuf, pbuf, drecv, sbuf, rbuf, rown, rstack, sems)
    out_y.wait()


def last_kernel(dg, du, hid, x, y, rows, ftok, base, grad_in, grad_gate, grad_up, grad_down):
    q = pl.program_id(0)

    def tn(a, b):
        return lax.dot_general(a, b, (((0,), (0,)), ((), ())), preferred_element_type=F32).astype(BF)

    grad_gate[0] = tn(dg[...], x[...])
    grad_up[0] = tn(du[...], x[...])
    grad_down[0] = tn(hid[...], y[...])
    tokens = grad_in.shape[1]
    lane = iota((tokens, 128), 1)
    hit = (ftok[:1, :] == iota((tokens, 128), 0).astype(F32)) & (lax.rem(lax.div(lane, CAP), QUARTERS) == q)
    select = jnp.where(hit, 1.0, 0.0)
    live = jnp.sum(select, axis=1, keepdims=True) > 0.0
    new = nn(select.astype(BF), rows[...])
    grad_in[0] = jnp.where(live, new, base[...].astype(F32)).astype(BF)


def round_scratch(rounds, width, units, slots):
    d = width * QUARTERS
    vm = pltpu.VMEM
    blocks = 2 * CHIPS * ROWS
    return [
        vm((rounds, ROWS, width + MARK), BF),
        vm((rounds, blocks, width + MARK), BF),
        vm((slots, d), BF),
        vm((blocks, width), BF),
        vm((rounds, blocks // 2, width), BF),
        vm((rounds, blocks // 2, width), BF),
        vm((rounds, blocks // 2, width), BF),
        vm((rounds, blocks // 2, width), BF),
        vm((rounds, ROWS, width), BF),
        vm((rounds, 8 * ROWS, width), BF),
    ]


def round_sems(rounds):
    sem = pltpu.SemaphoreType.DMA
    return [sem((rounds, CHIPS))] * 4 + [sem((rounds, NX))] * 2 + [sem((rounds, CHIPS))] * 2 + [sem((rounds, 8))] * 2


def on_device(saved_inputs, expert_ids, gate_weights, out_grad, gate_w, up_w, down_w):
    tokens, wg, wu, wd = saved_inputs[0], gate_w[0], up_w[0], down_w[0]
    count, d = tokens.shape
    units = wg.shape[0]
    width = d // QUARTERS
    slots = lax.axis_size("ep") * CAP
    routes = expert_ids[0]
    live = jnp.any(routes == 0, axis=1)
    pair_weight = jnp.sum(jnp.where(routes == 0, gate_weights[0], 0.0), axis=1)
    live_i = live.astype(jnp.int32)
    slot = jnp.cumsum(live_i) - live_i
    which = lax.rem(jnp.arange(ROWS, dtype=jnp.int32), CAP)[:, None]
    sel = live[None, :] & (slot[None, :] == which)
    tok = jnp.max(jnp.where(sel, jnp.arange(count, dtype=jnp.int32)[None, :], -1), axis=1, keepdims=True)
    weight = jnp.sum(jnp.where(sel, pair_weight[None, :], 0.0), axis=1, keepdims=True)
    tok = jnp.broadcast_to(tok, (ROWS, 128))
    weight = jnp.broadcast_to(weight, (ROWS, 128))

    hbm = pl.BlockSpec(memory_space=pl.ANY)
    vmem = pl.BlockSpec(memory_space=pltpu.VMEM)
    sem = pltpu.SemaphoreType.DMA
    vm = pltpu.VMEM

    def shape(dims, dtype=BF):
        return jax.ShapeDtypeStruct(dims, dtype)

    block = (ROWS, width)
    u, base0, select_up, cu, cg, hid, dg, du, rows, level, ftok, x, y, base = pl.pallas_call(
        first_kernel,
        name="first_rounds",
        out_shape=[shape(block), shape(block), shape((ROWS, 128)), shape((slots, units), F32), shape((slots, units), F32),
                   shape((slots, units)), shape((slots, units)), shape((slots, units)), shape((128, width)),
                   shape((8, 128), jnp.int32), shape((8, 128), F32), shape((slots, d)), shape((slots, d)), shape((count, d))],
        in_specs=[vmem] * 2 + [hbm] * 5,
        out_specs=[vmem] * 11 + [hbm] * 3,
        scratch_shapes=[
            vm((count, d), BF), vm(out_grad.shape, BF), vm((units, d), BF), vm((units, d), BF), vm((units, d), BF),
            vm(block, BF), vm((2 * CHIPS * ROWS, width), BF), vm((slots, d), BF), vm((128, 128), jnp.int32),
            vm((128, out_grad.shape[1]), BF), vm((128, out_grad.shape[1]), BF), vm(block, F32),
        ] + round_scratch(2, width, units, slots) + [
            sem((8,)), sem((CHIPS,)), sem((CHIPS,)), sem((CHIPS,)), sem((CHIPS,)),
            sem((8,)), sem((8,)), sem((8,)), sem((8,)), sem((8,)), sem((8,)),
        ] + round_sems(2),
        compiler_params=pltpu.CompilerParams(collective_id=0, has_side_effects=True, vmem_limit_bytes=60 * 2**20),
    )(tok, weight, tokens, out_grad, wg, wu, wd)

    def more(_, state):
        u, dg, du, rows, y = state
        return tuple(pl.pallas_call(
            next_kernel,
            name="next_round",
            out_shape=[shape(block), shape((slots, units)), shape((slots, units)), shape((128, width)), shape((slots, d))],
            in_specs=[vmem] * 6 + [hbm] * 3,
            out_specs=[vmem] * 4 + [hbm],
            scratch_shapes=[vm((units, d), BF), vm((units, d), BF), vm((units, d), BF)]
            + round_scratch(1, width, units, slots) + [sem((4,))] + round_sems(1),
            compiler_params=pltpu.CompilerParams(collective_id=1, has_side_effects=True, vmem_limit_bytes=60 * 2**20),
        )(u, weight, base0, select_up, cu, cg, wg, wu, wd))

    u, dg, du, rows, y = lax.fori_loop(0, level[0, 0] - 1, more, (u, dg, du, rows, y))

    full = pl.BlockSpec((slots, units), lambda q: (0, 0))
    cols = pl.BlockSpec((slots, width), lambda q: (0, q))
    grad = pl.BlockSpec((1, units, width), lambda q: (0, 0, q))
    return pl.pallas_call(
        last_kernel,
        name="gradients",
        grid=(QUARTERS,),
        out_shape=[shape((1, count, d)), shape((1, units, d)), shape((1, units, d)), shape((1, units, d))],
        in_specs=[full, full, full, cols, cols, pl.BlockSpec((128, width), lambda q: (0, 0)),
                  pl.BlockSpec((8, 128), lambda q: (0, 0)), pl.BlockSpec((count, width), lambda q: (0, q))],
        out_specs=[pl.BlockSpec((1, count, width), lambda q: (0, 0, q)), grad, grad, grad],
        compiler_params=pltpu.CompilerParams(vmem_limit_bytes=60 * 2**20),
    )(dg, du, hid, x, y, rows, ftok, base)


def solution(mesh):
    split = P("section", "ep", None)
    return jax.shard_map(
        on_device,
        mesh=mesh,
        in_specs=(split, split, split, P("ep", "section"), split, split, split),
        out_specs=(split, split, split, split),
        check_vma=False,
    )
```

```python
import functools

import jax
import jax.numpy as jnp
from jax import lax
from jax.experimental import pallas as pl
from jax.experimental.pallas import tpu as pltpu
from jax.sharding import PartitionSpec as P

MESH = pl.DeviceIdType.MESH
CAP = 4
NX, NY = 4, 4
CHIPS = NX * NY
QUARTERS = 4
ROWS = QUARTERS * CAP
MARK = 128
BF, F32 = jnp.bfloat16, jnp.float32


def iota(shape, dim):
    return lax.broadcasted_iota(jnp.int32, shape, dim)


def rows_at(index, size):
    return pl.ds(pl.multiple_of(index * size, size), size)


def swap_matrix():
    i, m = iota((64, 64), 0), iota((64, 64), 1)
    swapped = (lax.rem(lax.div(m, 4), 4) * 16) + (lax.div(m, 16) * 4) + lax.rem(m, 4)
    return jnp.where(i == swapped, 1.0, 0.0).astype(BF)


def nt(a, b):
    return lax.dot_general(a, b, (((1,), (1,)), ((), ())), preferred_element_type=F32)


def nn(a, b):
    return lax.dot_general(a, b, (((1,), (0,)), ((), ())), preferred_element_type=F32)


class Place:
    def __init__(self):
        self.s = lax.axis_index("section")
        self.sections = lax.axis_size("section")
        ep = lax.axis_index("ep")
        self.core = lax.rem(ep, 2)
        self.chip = lax.div(ep, 2)
        self.x = lax.div(self.chip, NY)
        self.y = lax.rem(self.chip, NY)
        self.partner = {"ep": self.chip * 2 + 1 - self.core}

    def ahead(self, k):
        i, j = lax.div(k, NY), lax.rem(k, NY)
        return lax.rem(self.x + i, NX) * NY + lax.rem(self.y + j, NY)

    def behind(self, k):
        i, j = lax.div(k, NY), lax.rem(k, NY)
        return lax.rem(self.x + NX - i, NX) * NY + lax.rem(self.y + NY - j, NY)

    def peer(self, chip):
        return {"ep": chip * 2 + self.core}

    def block(self, core, chip):
        return rows_at(core * CHIPS + chip, ROWS)


def remote(src, dst, send, recv, device):
    return pltpu.make_async_remote_copy(
        src_ref=src, dst_ref=dst, send_sem=send, recv_sem=recv, device_id=device, device_id_type=MESH
    )


def each(lo, hi, body):
    lax.fori_loop(lo, hi, lambda k, carry: (body(k), carry)[1], 0)


def gather_start(at, own, buf, send, recv):
    mine = at.block(at.core, at.chip)

    def go(k):
        remote(own, buf.at[mine], send.at[k], recv.at[k], at.peer(at.ahead(k))).start()

    each(1, CHIPS, go)
    remote(own, buf.at[mine], send.at[0], recv.at[0], at.partner).start()
    buf[mine, :] = own[...]


def gather_finish(at, own, buf, send, recv, relay_send, relay_recv):
    def forward(k):
        piece = at.block(at.core, at.behind(k))
        remote(own, buf.at[piece], send.at[k], recv.at[k], at.partner).wait_recv()
        remote(buf.at[piece], buf.at[piece], relay_send.at[k], relay_recv.at[k], at.partner).start()

    each(1, CHIPS, forward)
    other = at.block(1 - at.core, at.chip)
    remote(own, buf.at[other], send.at[0], recv.at[0], at.partner).wait_recv()

    def take(k):
        piece = at.block(1 - at.core, at.behind(k))
        remote(buf.at[piece], buf.at[piece], relay_send.at[k], relay_recv.at[k], at.partner).wait_recv()

    each(1, CHIPS, take)


def gather_drain(at, own, buf, send, recv, relay_send, relay_recv):
    def drain(k):
        remote(own, buf.at[at.block(at.core, at.chip)], send.at[k], recv.at[k], at.partner).wait_send()

    each(0, CHIPS, drain)

    def drain_relay(k):
        piece = at.block(at.core, at.behind(k))
        remote(buf.at[piece], buf.at[piece], relay_send.at[k], relay_recv.at[k], at.partner).wait_send()

    each(1, CHIPS, drain_relay)


def to_rows(buf, nat, width):
    swap = swap_matrix()

    def one(j):
        tile = nn(swap, buf[rows_at(j, 64), :width]).astype(BF)
        for q in range(QUARTERS):
            nat[rows_at(j, ROWS), q * width : (q + 1) * width] = tile[q * ROWS : (q + 1) * ROWS]

    each(0, 2 * CHIPS // 4, one)


def project(nat, weight, width):
    def step(q, acc):
        cols = rows_at(q, width)
        return acc + nt(nat[:, cols], weight[:, cols])

    return lax.fori_loop(0, QUARTERS, step, jnp.zeros((nat.shape[0], weight.shape[0]), F32))


def one_round(at, r, width, upstream, yown, ybuf, ynat, stack, pbuf, drecv, sbuf, rbuf, rown, rstack,
              wg, wu, wd, coef_up, coef_gate, dg, du, sems, before_rows=None, after_gather=None, weights_ready=None):
    (ag_s, ag_r, rel_s, rel_r, dd_s, dd_r, rs_s, rs_r, z_s, z_r) = sems
    ag = (at, yown.at[r], ybuf.at[r], ag_s.at[r], ag_r.at[r], rel_s.at[r], rel_r.at[r])
    gather_start(*ag[:5])
    if before_rows is not None:
        before_rows()
    gather_finish(*ag)
    if after_gather is not None:
        after_gather()
    to_rows(ybuf.at[r], ynat, width)
    if weights_ready is not None:
        weights_ready()
    grad_hidden = project(ynat, wd, width)
    du[...] = (grad_hidden * coef_up[...]).astype(BF)
    dg[...] = (grad_hidden * coef_gate[...]).astype(BF)

    def back(q):
        cols = rows_at(q, width)
        value = (nn(dg[...], wg[:, cols]) + nn(du[...], wu[:, cols])).astype(BF)
        for j in range(2 * CHIPS // 4):
            stack[rows_at(j * QUARTERS + q, ROWS), :] = value[j * ROWS : (j + 1) * ROWS]

    each(0, QUARTERS, back)
    swap = swap_matrix()

    def to_partner(jj):
        j = lax.rem(at.x + jj, NX)
        part = rows_at(j, 64)
        pbuf[r, part, :] = nn(swap, stack[rows_at((1 - at.core) * NX + j, 64), :]).astype(BF)
        remote(pbuf.at[r, part], drecv.at[r, part], dd_s.at[r, jj], dd_r.at[r, jj], at.partner).start()

    each(0, NX, to_partner)

    def to_homes(jj):
        j = lax.rem(at.x + jj, NX)
        part = rows_at(j, 64)
        mine = nn(swap, stack[rows_at(at.core * NX + j, 64), :])
        remote(pbuf.at[r, part], drecv.at[r, part], dd_s.at[r, jj], dd_r.at[r, jj], at.partner).wait_recv()
        sbuf[r, part, :] = (mine + drecv[r, part, :].astype(F32)).astype(BF)

        def send(m):
            k = jj * NY + m

            @pl.when(k > 0)
            def _():
                chip = at.ahead(k)
                remote(sbuf.at[r, rows_at(chip, ROWS)], rbuf.at[r, rows_at(k, ROWS)], rs_s.at[r, k], rs_r.at[r, k],
                       at.peer(chip)).start()

        each(0, NY, send)

    each(0, NX, to_homes)

    def add(k, acc):
        here = rows_at(k, ROWS)
        remote(sbuf.at[r, here], rbuf.at[r, here], rs_s.at[r, k], rs_r.at[r, k], at.partner).wait_recv()
        return acc + rbuf[r, here, :].astype(F32)

    total = lax.fori_loop(1, CHIPS, add, sbuf[r, rows_at(at.chip, ROWS), :].astype(F32))
    row = (upstream() + total).astype(BF)
    rown[r] = row
    mine = rows_at(at.s, ROWS)
    rstack[r, mine, :] = row

    def down(d):
        @pl.when(at.s >= d)
        def _():
            remote(rown.at[r], rstack.at[r, mine], z_s.at[r, d], z_r.at[r, d], {"section": at.s - d}).start()

    each(1, at.sections, down)

    def up(d):
        @pl.when(at.s + d < at.sections)
        def _():
            remote(rown.at[r], rstack.at[r, rows_at(at.s + d, ROWS)], z_s.at[r, d], z_r.at[r, d],
                   {"section": at.s + d}).wait_recv()

    each(1, at.sections, up)


def round_drain(at, r, yown, ybuf, pbuf, drecv, sbuf, rbuf, rown, rstack, sems):
    (ag_s, ag_r, rel_s, rel_r, dd_s, dd_r, rs_s, rs_r, z_s, z_r) = sems
    gather_drain(at, yown.at[r], ybuf.at[r], ag_s.at[r], ag_r.at[r], rel_s.at[r], rel_r.at[r])

    def drain_partner(jj):
        part = rows_at(jj, 64)
        remote(pbuf.at[r, part], drecv.at[r, part], dd_s.at[r, jj], dd_r.at[r, jj], at.partner).wait_send()

    each(0, NX, drain_partner)

    def drain_homes(k):
        here = rows_at(k, ROWS)
        remote(sbuf.at[r, here], rbuf.at[r, here], rs_s.at[r, k], rs_r.at[r, k], at.partner).wait_send()

    each(1, CHIPS, drain_homes)

    def drain_z(d):
        @pl.when(at.s >= d)
        def _():
            remote(rown.at[r], rstack.at[r, rows_at(at.s, ROWS)], z_s.at[r, d], z_r.at[r, d],
                   {"section": at.s - d}).wait_send()

    each(1, at.sections, drain_z)


def signal_to(device):
    pl.semaphore_signal(pltpu.get_barrier_semaphore(), inc=1, device_id=device, device_id_type=MESH)


def first_kernel(ids_ref, gates_ref, tokens_hbm, og_hbm, wg_hbm, wu_hbm, wd_hbm,
                 w_ref, u_out, base0_out, sel_out, cu_out, cg_out, hid_out, dg_out, du_out, r_out, level_out, ftok_out,
                 xnat_hbm, ynat_hbm, base_hbm,
                 tok_ref, tokv, ogv, wg, wu, wd, xown, xbuf, xnat, tokall, psend, precv, base,
                 yown, ybuf, ynat, stack, pbuf, drecv, sbuf, rbuf, rown, rstack,
                 loc, x_s, x_r, xrel_s, xrel_r, id_s, id_r, pc_s, pc_r, bs_s, bs_r, *sems):
    at = Place()
    width = u_out.shape[1]
    s, sections = at.s, at.sections
    half = ogv.shape[1]

    load_tokens = pltpu.make_async_copy(tokens_hbm, tokv, loc.at[0])
    load_og = pltpu.make_async_copy(og_hbm, ogv, loc.at[1])
    load_g = pltpu.make_async_copy(wg_hbm, wg, loc.at[2])
    load_u = pltpu.make_async_copy(wu_hbm, wu, loc.at[3])
    load_d = pltpu.make_async_copy(wd_hbm, wd, loc.at[4])
    for load in (load_tokens, load_og, load_g, load_u, load_d):
        load.start()

    rstack[...] = jnp.zeros_like(rstack)

    def greet(k):
        signal_to(at.peer(at.ahead(k)))

    each(1, CHIPS, greet)
    signal_to(at.partner)

    def greet_z(d):
        signal_to({"section": lax.rem(s + d, sections)})

    each(1, sections, greet_z)

    hits = ids_ref[...] == 0
    live = jnp.sum(jnp.where(hits, 1.0, 0.0), axis=0, keepdims=True)
    pair_weight = jnp.sum(jnp.where(hits, gates_ref[...], 0.0), axis=0, keepdims=True)
    before = jnp.where(iota((128, 128), 0) < iota((128, 128), 1), 1.0, 0.0).astype(BF)
    live16 = jnp.broadcast_to(live, (ROWS, 128))
    slot = nn(live16.astype(BF), before)
    lane16, row16 = iota((ROWS, 128), 1), iota((ROWS, 128), 0)
    mine16 = (live16 > 0.5) & (slot == lax.rem(row16, CAP).astype(F32))
    token = jnp.max(jnp.where(mine16, lane16.astype(F32), -1.0), axis=1, keepdims=True)
    tok_ref[...] = jnp.broadcast_to(token, (ROWS, 128))
    share = jnp.sum(jnp.where(mine16, jnp.broadcast_to(pair_weight, (ROWS, 128)), 0.0), axis=1, keepdims=True)
    w_ref[...] = jnp.broadcast_to(share, (ROWS, 128))

    mine_z = rows_at(s, ROWS)
    pl.semaphore_wait(pltpu.get_barrier_semaphore(), CHIPS + sections - 1)

    def send_ids(d):
        remote(tok_ref, tokall.at[mine_z], id_s.at[d], id_r.at[d], {"section": lax.rem(s + d, sections)}).start()

    each(1, sections, send_ids)
    tokall[mine_z, :] = tok_ref[...]

    load_tokens.wait()
    hit = tok_ref[...] == lane16.astype(F32)
    block = jnp.zeros((ROWS, width), F32)
    for q in range(QUARTERS):
        select = jnp.where(hit & (lax.div(row16, CAP) == q), 1.0, 0.0).astype(BF)
        block = block + nn(select, tokv[:, q * width : (q + 1) * width])
    xown[...] = block.astype(BF)
    xg = (at, xown, xbuf, x_s, x_r, xrel_s, xrel_r)
    gather_start(*xg[:5])

    load_og.wait()

    def wait_ids(d):
        source = lax.rem(s + sections - d, sections)
        remote(tok_ref, tokall.at[rows_at(source, ROWS)], id_s.at[d], id_r.at[d], at.partner).wait_recv()

    each(1, sections, wait_ids)
    tok_f = tokall[...]
    row, lane = iota((128, 128), 0), iota((128, 128), 1)
    pick = (tok_f == lane.astype(F32)) & (lax.rem(lax.div(row, CAP), QUARTERS) == lax.div(s, 2))
    psend[...] = nn(jnp.where(pick, 1.0, 0.0).astype(BF), ogv[...]).astype(BF)

    def send_piece(d):
        to = lax.rem(s + d, sections)
        remote(psend.at[rows_at(to, ROWS)], precv.at[mine_z], pc_s.at[d], pc_r.at[d], {"section": to}).start()

    each(1, sections, send_piece)
    precv[mine_z, :] = psend[mine_z, :]

    other = tok_f.T
    layer_r, layer_l = lax.div(row, ROWS), lax.div(lane, ROWS)
    same = (tok_f == other) & (tok_f >= 0.0) & (lax.rem(lax.div(row, CAP), QUARTERS) == lax.rem(lax.div(lane, CAP), QUARTERS))
    above = jnp.where(same & (layer_l > layer_r), 1.0, 0.0)
    level_r = jnp.sum(above, axis=1, keepdims=True)
    level_l = jnp.sum(jnp.where(same & (layer_r > layer_l), 1.0, 0.0), axis=0, keepdims=True)
    chosen = jnp.where(level_l == level_r - 1.0, above, 0.0)
    take = jnp.where(iota((ROWS, 128), 1) == iota((ROWS, 128), 0) + s * ROWS, 1.0, 0.0).astype(BF)
    select_up = nn(take, chosen.astype(BF))
    level_own = nn(take, jnp.broadcast_to(level_r, (128, 128)).astype(BF))
    sel_out[...] = select_up.astype(BF)
    later = jnp.sum(jnp.where(same & (layer_r < layer_l) & (layer_r >= s), 1.0, 0.0), axis=0, keepdims=True)
    tok_l = jnp.max(other, axis=0, keepdims=True)
    lane1 = iota((1, 128), 1)
    ftok = jnp.where((later == 0.0) & (lax.div(lane1, ROWS) >= s), tok_l, -1.0)
    ftok_out[...] = jnp.broadcast_to(ftok, ftok_out.shape)
    deepest = jnp.max(level_r, axis=0, keepdims=True)

    def wait_piece(d):
        source = lax.rem(s + sections - d, sections)
        remote(psend.at[mine_z], precv.at[rows_at(source, ROWS)], pc_s.at[d], pc_r.at[d], at.partner).wait_recv()

    each(1, sections, wait_piece)

    for h in range(2):
        total = jnp.zeros((ROWS, half), F32)
        for p in range(h, 8, 2):
            total = total + precv[p * ROWS : (p + 1) * ROWS, :].astype(F32)
        base[:, h * half : (h + 1) * half] = total
    root = level_own[:, :1] == 0.0
    base0_out[...] = jnp.where(root, base[...], 0.0).astype(BF)
    weight = w_ref[:, :1]
    yown[0, :, :width] = (weight * base[...]).astype(BF)
    yown[0, :, width:] = jnp.broadcast_to(deepest, (ROWS, MARK)).astype(BF)

    def send_base():
        def go(d):
            to = lax.rem(s + d, sections)
            remote(ogv, base_hbm.at[:, rows_at(s, half)], bs_s.at[d], bs_r.at[d], {"section": to}).start()

        each(1, sections, go)
        pltpu.make_async_copy(ogv, base_hbm.at[:, rows_at(s, half)], loc.at[5]).start()

    def activations():
        send_base()
        gather_finish(*xg)
        to_rows(xbuf, xnat, width)
        pltpu.make_async_copy(xnat, xnat_hbm, loc.at[6]).start()
        load_g.wait()
        load_u.wait()
        gate = project(xnat, wg, width)
        up = project(xnat, wu, width)
        sig = 1.0 / (1.0 + jnp.exp(-gate))
        act = gate * sig
        hid_out[...] = (act * up).astype(BF)
        cu_out[...] = act
        cg_out[...] = up * sig * (1.0 + gate * (1.0 - sig))

    def read_level():
        marks = ybuf[0, :, width : width + MARK].astype(F32)
        level_out[0] = jnp.max(marks).astype(jnp.int32)

    shared = (yown, ybuf, ynat, stack, pbuf, drecv, sbuf, rbuf, rown, rstack, wg, wu, wd, cu_out, cg_out, dg_out, du_out, sems)
    one_round(at, 0, width, lambda: base[...], *shared, before_rows=activations, after_gather=read_level,
              weights_ready=load_d.wait)

    def follow(r):
        return nn(sel_out[...], rstack[r]) + base0_out[...].astype(F32)

    u_out[...] = follow(0).astype(BF)
    yown[1, :, :width] = (weight * u_out[...].astype(F32)).astype(BF)
    yown[1, :, width:] = jnp.zeros((ROWS, MARK), BF)
    one_round(at, 1, width, lambda: u_out[...].astype(F32), *shared)
    out_y = pltpu.make_async_copy(ynat, ynat_hbm, loc.at[7])
    out_y.start()
    u_out[...] = follow(1).astype(BF)
    r_out[...] = rstack[1]

    gather_drain(*xg)

    def drain_z(d):
        to = lax.rem(s + d, sections)
        source = lax.rem(s + sections - d, sections)
        remote(tok_ref, tokall.at[mine_z], id_s.at[d], id_r.at[d], at.partner).wait_send()
        remote(psend.at[rows_at(to, ROWS)], precv.at[mine_z], pc_s.at[d], pc_r.at[d], at.partner).wait_send()
        into = remote(ogv, base_hbm.at[:, rows_at(source, half)], bs_s.at[d], bs_r.at[d], at.partner)
        into.wait_send()
        into.wait_recv()

    each(1, sections, drain_z)
    for r in range(2):
        round_drain(at, r, yown, ybuf, pbuf, drecv, sbuf, rbuf, rown, rstack, sems)
    pltpu.make_async_copy(ogv, base_hbm.at[:, rows_at(s, half)], loc.at[5]).wait()
    pltpu.make_async_copy(xnat, xnat_hbm, loc.at[6]).wait()
    out_y.wait()


def next_kernel(u_ref, w_ref, base0_ref, sel_ref, cu_ref, cg_ref, wg_hbm, wu_hbm, wd_hbm,
                u_out, dg_out, du_out, r_out, ynat_hbm,
                wg, wu, wd, yown, ybuf, ynat, stack, pbuf, drecv, sbuf, rbuf, rown, rstack, loc, *sems):
    at = Place()
    width = u_out.shape[1]
    load_g = pltpu.make_async_copy(wg_hbm, wg, loc.at[0])
    load_u = pltpu.make_async_copy(wu_hbm, wu, loc.at[1])
    load_d = pltpu.make_async_copy(wd_hbm, wd, loc.at[2])
    for load in (load_d, load_g, load_u):
        load.start()

    rstack[...] = jnp.zeros_like(rstack)

    def greet(k):
        signal_to(at.peer(at.ahead(k)))

    each(1, CHIPS, greet)
    signal_to(at.partner)

    def greet_z(d):
        @pl.when(at.s + d < at.sections)
        def _():
            signal_to({"section": at.s + d})

    each(1, at.sections, greet_z)
    yown[0, :, :width] = (w_ref[:, :1] * u_ref[...].astype(F32)).astype(BF)
    yown[0, :, width:] = jnp.zeros((ROWS, MARK), BF)
    pl.semaphore_wait(pltpu.get_barrier_semaphore(), CHIPS + at.s)

    def loaded():
        for load in (load_d, load_g, load_u):
            load.wait()

    one_round(at, 0, width, lambda: u_ref[...].astype(F32), yown, ybuf, ynat, stack, pbuf, drecv, sbuf, rbuf, rown, rstack,
              wg, wu, wd, cu_ref, cg_ref, dg_out, du_out, sems, weights_ready=loaded)
    out_y = pltpu.make_async_copy(ynat, ynat_hbm, loc.at[3])
    out_y.start()
    u_out[...] = (nn(sel_ref[...], rstack[0]) + base0_ref[...].astype(F32)).astype(BF)
    r_out[...] = rstack[0]
    round_drain(at, 0, yown, ybuf, pbuf, drecv, sbuf, rbuf, rown, rstack, sems)
    out_y.wait()


def last_kernel(dg, du, hid, x, y, rows, ftok, base, grad_in, grad_gate, grad_up, grad_down):
    q = lax.div(pl.program_id(0), 2)

    def tn(a, b):
        return lax.dot_general(a, b, (((0,), (0,)), ((), ())), preferred_element_type=F32).astype(BF)

    grad_gate[0] = tn(dg[...], x[...])
    grad_up[0] = tn(du[...], x[...])
    grad_down[0] = tn(hid[...], y[...])
    tokens = grad_in.shape[1]
    lane = iota((tokens, 128), 1)
    hit = (ftok[:1, :] == iota((tokens, 128), 0).astype(F32)) & (lax.rem(lax.div(lane, CAP), QUARTERS) == q)
    select = jnp.where(hit, 1.0, 0.0)
    live = jnp.sum(select, axis=1, keepdims=True) > 0.0
    new = nn(select.astype(BF), rows[...])
    grad_in[0] = jnp.where(live, new, base[...].astype(F32)).astype(BF)


def round_scratch(rounds, width, units, slots):
    d = width * QUARTERS
    vm = pltpu.VMEM
    blocks = 2 * CHIPS * ROWS
    return [
        vm((rounds, ROWS, width + MARK), BF),
        vm((rounds, blocks, width + MARK), BF),
        vm((slots, d), BF),
        vm((blocks, width), BF),
        vm((rounds, blocks // 2, width), BF),
        vm((rounds, blocks // 2, width), BF),
        vm((rounds, blocks // 2, width), BF),
        vm((rounds, blocks // 2, width), BF),
        vm((rounds, ROWS, width), BF),
        vm((rounds, 8 * ROWS, width), BF),
    ]


def round_sems(rounds):
    sem = pltpu.SemaphoreType.DMA
    return [sem((rounds, CHIPS))] * 4 + [sem((rounds, NX))] * 2 + [sem((rounds, CHIPS))] * 2 + [sem((rounds, 8))] * 2


def on_device(saved_inputs, expert_ids, gate_weights, out_grad, gate_w, up_w, down_w):
    tokens, wg, wu, wd = saved_inputs[0], gate_w[0], up_w[0], down_w[0]
    count, d = tokens.shape
    units = wg.shape[0]
    width = d // QUARTERS
    slots = lax.axis_size("ep") * CAP
    ids, gates = expert_ids[0].T, gate_weights[0].T
    hbm = pl.BlockSpec(memory_space=pl.ANY)
    vmem = pl.BlockSpec(memory_space=pltpu.VMEM)
    sem = pltpu.SemaphoreType.DMA
    vm = pltpu.VMEM

    def shape(dims, dtype=BF):
        return jax.ShapeDtypeStruct(dims, dtype)

    block = (ROWS, width)
    weight, u, base0, select_up, cu, cg, hid, dg, du, rows, level, ftok, x, y, base = pl.pallas_call(
        first_kernel,
        name="first_rounds",
        out_shape=[shape((ROWS, 128), F32), shape(block), shape(block), shape((ROWS, 128)), shape((slots, units), F32), shape((slots, units), F32),
                   shape((slots, units)), shape((slots, units)), shape((slots, units)), shape((128, width)),
                   shape((1,), jnp.int32), shape((8, 128), F32), shape((slots, d)), shape((slots, d)), shape((count, d))],
        in_specs=[vmem] * 2 + [hbm] * 5,
        out_specs=[vmem] * 10 + [pl.BlockSpec(memory_space=pltpu.SMEM), vmem] + [hbm] * 3,
        scratch_shapes=[
            vm((ROWS, 128), F32), vm((count, d), BF), vm(out_grad.shape, BF), vm((units, d), BF), vm((units, d), BF), vm((units, d), BF),
            vm(block, BF), vm((2 * CHIPS * ROWS, width), BF), vm((slots, d), BF), vm((128, 128), F32),
            vm((128, out_grad.shape[1]), BF), vm((128, out_grad.shape[1]), BF), vm(block, F32),
        ] + round_scratch(2, width, units, slots) + [
            sem((8,)), sem((CHIPS,)), sem((CHIPS,)), sem((CHIPS,)), sem((CHIPS,)),
            sem((8,)), sem((8,)), sem((8,)), sem((8,)), sem((8,)), sem((8,)),
        ] + round_sems(2),
        compiler_params=pltpu.CompilerParams(collective_id=0, has_side_effects=True, vmem_limit_bytes=60 * 2**20),
    )(ids, gates, tokens, out_grad, wg, wu, wd)

    def more(_, state):
        u, dg, du, rows, y = state
        return tuple(pl.pallas_call(
            next_kernel,
            name="next_round",
            out_shape=[shape(block), shape((slots, units)), shape((slots, units)), shape((128, width)), shape((slots, d))],
            in_specs=[vmem] * 6 + [hbm] * 3,
            out_specs=[vmem] * 4 + [hbm],
            scratch_shapes=[vm((units, d), BF), vm((units, d), BF), vm((units, d), BF)]
            + round_scratch(1, width, units, slots) + [sem((4,))] + round_sems(1),
            compiler_params=pltpu.CompilerParams(collective_id=1, has_side_effects=True, vmem_limit_bytes=60 * 2**20),
        )(u, weight, base0, select_up, cu, cg, wg, wu, wd))

    u, dg, du, rows, y = lax.fori_loop(0, level[0] - 1, more, (u, dg, du, rows, y))

    half = width // 2
    full = pl.BlockSpec((slots, units), lambda i: (0, 0))
    cols = pl.BlockSpec((slots, half), lambda i: (0, i))
    grad = pl.BlockSpec((1, units, half), lambda i: (0, 0, i))
    return pl.pallas_call(
        last_kernel,
        name="gradients",
        grid=(2 * QUARTERS,),
        out_shape=[shape((1, count, d)), shape((1, units, d)), shape((1, units, d)), shape((1, units, d))],
        in_specs=[full, full, full, cols, cols, pl.BlockSpec((128, half), lambda i: (0, lax.rem(i, 2))),
                  pl.BlockSpec((8, 128), lambda i: (0, 0)), pl.BlockSpec((count, half), lambda i: (0, i))],
        out_specs=[pl.BlockSpec((1, count, half), lambda i: (0, 0, i)), grad, grad, grad],
        compiler_params=pltpu.CompilerParams(vmem_limit_bytes=60 * 2**20),
    )(dg, du, hid, x, y, rows, ftok, base)


def solution(mesh):
    split = P("section", "ep", None)
    return jax.shard_map(
        on_device,
        mesh=mesh,
        in_specs=(split, split, split, P("ep", "section"), split, split, split),
        out_specs=(split, split, split, split),
        check_vma=False,
    )
```

```python
import functools

import jax
import jax.numpy as jnp
from jax import lax
from jax.experimental import pallas as pl
from jax.experimental.pallas import tpu as pltpu
from jax.sharding import PartitionSpec as P

MESH = pl.DeviceIdType.MESH
CAP = 4
NX, NY = 4, 4
CHIPS = NX * NY
QUARTERS = 4
TILES = 2 * CHIPS * CAP // 16
ROWS = QUARTERS * CAP
MARK = 128
BF, F32 = jnp.bfloat16, jnp.float32


def iota(shape, dim):
    return lax.broadcasted_iota(jnp.int32, shape, dim)


def rows_at(index, size):
    return pl.ds(pl.multiple_of(index * size, size), size)


def swap_matrix():
    i, m = iota((64, 64), 0), iota((64, 64), 1)
    swapped = (lax.rem(lax.div(m, 4), 4) * 16) + (lax.div(m, 16) * 4) + lax.rem(m, 4)
    return jnp.where(i == swapped, 1.0, 0.0).astype(BF)


def nt(a, b):
    return lax.dot_general(a, b, (((1,), (1,)), ((), ())), preferred_element_type=F32)


def nn(a, b):
    return lax.dot_general(a, b, (((1,), (0,)), ((), ())), preferred_element_type=F32)


class Place:
    def __init__(self):
        self.s = lax.axis_index("section")
        self.sections = lax.axis_size("section")
        ep = lax.axis_index("ep")
        self.core = lax.rem(ep, 2)
        self.chip = lax.div(ep, 2)
        self.x = lax.div(self.chip, NY)
        self.y = lax.rem(self.chip, NY)
        self.partner = {"ep": self.chip * 2 + 1 - self.core}

    def ahead(self, k):
        i, j = lax.div(k, NY), lax.rem(k, NY)
        return lax.rem(self.x + i, NX) * NY + lax.rem(self.y + j, NY)

    def behind(self, k):
        i, j = lax.div(k, NY), lax.rem(k, NY)
        return lax.rem(self.x + NX - i, NX) * NY + lax.rem(self.y + NY - j, NY)

    def peer(self, chip):
        return {"ep": chip * 2 + self.core}

    def block(self, core, chip):
        return rows_at(core * CHIPS + chip, ROWS)


def remote(src, dst, send, recv, device):
    return pltpu.make_async_remote_copy(
        src_ref=src, dst_ref=dst, send_sem=send, recv_sem=recv, device_id=device, device_id_type=MESH
    )


def each(lo, hi, body):
    lax.fori_loop(lo, hi, lambda k, carry: (body(k), carry)[1], 0)


def gather_start(at, own, buf, send, recv):
    mine = at.block(at.core, at.chip)

    def go(k):
        remote(own, buf.at[mine], send.at[k], recv.at[k], at.peer(at.ahead(k))).start()

    each(1, CHIPS, go)
    remote(own, buf.at[mine], send.at[0], recv.at[0], at.partner).start()
    buf[mine, :] = own[...]


def gather_finish(at, own, buf, send, recv, relay_send, relay_recv):
    def forward(k):
        piece = at.block(at.core, at.behind(k))
        remote(own, buf.at[piece], send.at[k], recv.at[k], at.partner).wait_recv()
        remote(buf.at[piece], buf.at[piece], relay_send.at[k], relay_recv.at[k], at.partner).start()

    each(1, CHIPS, forward)
    other = at.block(1 - at.core, at.chip)
    remote(own, buf.at[other], send.at[0], recv.at[0], at.partner).wait_recv()

    def take(k):
        piece = at.block(1 - at.core, at.behind(k))
        remote(buf.at[piece], buf.at[piece], relay_send.at[k], relay_recv.at[k], at.partner).wait_recv()

    each(1, CHIPS, take)


def gather_drain(at, own, buf, send, recv, relay_send, relay_recv):
    def drain(k):
        remote(own, buf.at[at.block(at.core, at.chip)], send.at[k], recv.at[k], at.partner).wait_send()

    each(0, CHIPS, drain)

    def drain_relay(k):
        piece = at.block(at.core, at.behind(k))
        remote(buf.at[piece], buf.at[piece], relay_send.at[k], relay_recv.at[k], at.partner).wait_send()

    each(1, CHIPS, drain_relay)


class Wide:
    parts = QUARTERS

    def __init__(self, stack):
        self.stack, self.width = stack, stack.shape[1]

    def expand(self, buf, nat):
        swap, width = swap_matrix(), self.width

        def one(t):
            tile = nn(swap, buf[rows_at(t, 64), :width]).astype(BF)
            for q in range(QUARTERS):
                nat[rows_at(t, ROWS), q * width : (q + 1) * width] = tile[q * ROWS : (q + 1) * ROWS]

        each(0, TILES, one)

    def fill(self, q, value):
        for t in range(TILES):
            self.stack[rows_at(t * QUARTERS + q, ROWS), :] = value[t * ROWS : (t + 1) * ROWS]

    def pack(self, t):
        return nn(swap_matrix(), self.stack[rows_at(t, 64), :])


class Narrow:
    parts = 2 * QUARTERS

    def __init__(self, stack, place, place_t):
        self.stack, self.width = stack, stack.shape[1]
        self.place, self.place_t = place, place_t

    def expand(self, buf, nat):
        width = self.width

        def one(t):
            tile = nn(self.place[rows_at(t, 128), :64], buf[rows_at(t, 64), :]).astype(BF)
            for q in range(2 * QUARTERS):
                nat[rows_at(t, ROWS), q * width : (q + 1) * width] = tile[q * ROWS : (q + 1) * ROWS]

        each(0, TILES, one)

    def fill(self, q, value):
        for t in range(TILES):
            for h in range(2):
                self.stack[rows_at(t * 2 * QUARTERS + q * 2 + h, ROWS), :] = value[
                    t * ROWS : (t + 1) * ROWS, h * self.width : (h + 1) * self.width
                ]

    def pack(self, t):
        return nn(self.place_t[rows_at(t, 64), :], self.stack[rows_at(t, 128), :])


def project(nat, weight, width):
    def step(q, acc):
        cols = rows_at(q, width)
        return acc + nt(nat[:, cols], weight[:, cols])

    return lax.fori_loop(0, QUARTERS, step, jnp.zeros((nat.shape[0], weight.shape[0]), F32))


def one_round(at, form, upstream, bufs, weights, coefs, grads, sems, during_gather=None, after_gather=None,
              before_grads=None, during_sends=None):
    yown, ybuf, ynat, pbuf, drecv, sbuf, rbuf, rown, rstack = bufs
    (ag_s, ag_r, rel_s, rel_r, dd_s, dd_r, rs_s, rs_r, z_s, z_r) = sems
    wg, wu, wd = weights
    dg, du = grads
    width = wg.shape[1] // QUARTERS
    gather_start(at, yown, ybuf, ag_s, ag_r)
    if during_gather is not None:
        during_gather()
    gather_finish(at, yown, ybuf, ag_s, ag_r, rel_s, rel_r)
    if after_gather is not None:
        after_gather()
    form.expand(ybuf, ynat)
    if before_grads is not None:
        before_grads()
    grad_hidden = project(ynat, wd, width)
    du[...] = (grad_hidden * coefs[0][...]).astype(BF)
    dg[...] = (grad_hidden * coefs[1][...]).astype(BF)

    def back(q):
        cols = rows_at(q, width)
        form.fill(q, (nn(dg[...], wg[:, cols]) + nn(du[...], wu[:, cols])).astype(BF))

    each(0, QUARTERS, back)

    def to_partner(jj):
        j = lax.rem(at.x + jj, NX)
        part = rows_at(j, 64)
        pbuf[part, :] = form.pack((1 - at.core) * NX + j).astype(BF)
        remote(pbuf.at[part], drecv.at[part], dd_s.at[jj], dd_r.at[jj], at.partner).start()

    each(0, NX, to_partner)

    def to_homes(jj):
        j = lax.rem(at.x + jj, NX)
        part = rows_at(j, 64)
        mine = form.pack(at.core * NX + j)
        remote(pbuf.at[part], drecv.at[part], dd_s.at[jj], dd_r.at[jj], at.partner).wait_recv()
        sbuf[part, :] = (mine + drecv[part, :].astype(F32)).astype(BF)

        def send(m):
            k = jj * NY + m

            @pl.when(k > 0)
            def _():
                chip = at.ahead(k)
                remote(sbuf.at[rows_at(chip, ROWS)], rbuf.at[rows_at(k, ROWS)], rs_s.at[k], rs_r.at[k], at.peer(chip)).start()

        each(0, NY, send)

    each(0, NX, to_homes)
    if during_sends is not None:
        during_sends()

    def add(k, acc):
        here = rows_at(k, ROWS)
        remote(sbuf.at[here], rbuf.at[here], rs_s.at[k], rs_r.at[k], at.partner).wait_recv()
        return acc + rbuf[here, :].astype(F32)

    total = lax.fori_loop(1, CHIPS, add, sbuf[rows_at(at.chip, ROWS), :].astype(F32))
    row = (upstream() + total).astype(BF)
    rown[...] = row
    mine = rows_at(at.s, ROWS)
    rstack[mine, :] = row

    def down(d):
        @pl.when(at.s >= d)
        def _():
            remote(rown, rstack.at[mine], z_s.at[d], z_r.at[d], {"section": at.s - d}).start()

    each(1, at.sections, down)

    def up(d):
        @pl.when(at.s + d < at.sections)
        def _():
            remote(rown, rstack.at[rows_at(at.s + d, ROWS)], z_s.at[d], z_r.at[d], {"section": at.s + d}).wait_recv()

    each(1, at.sections, up)


def round_drain(at, bufs, sems):
    yown, ybuf, ynat, pbuf, drecv, sbuf, rbuf, rown, rstack = bufs
    (ag_s, ag_r, rel_s, rel_r, dd_s, dd_r, rs_s, rs_r, z_s, z_r) = sems
    gather_drain(at, yown, ybuf, ag_s, ag_r, rel_s, rel_r)

    def drain_partner(jj):
        part = rows_at(jj, 64)
        remote(pbuf.at[part], drecv.at[part], dd_s.at[jj], dd_r.at[jj], at.partner).wait_send()

    each(0, NX, drain_partner)

    def drain_homes(k):
        here = rows_at(k, ROWS)
        remote(sbuf.at[here], rbuf.at[here], rs_s.at[k], rs_r.at[k], at.partner).wait_send()

    each(1, CHIPS, drain_homes)

    def drain_z(d):
        @pl.when(at.s >= d)
        def _():
            remote(rown, rstack.at[rows_at(at.s, ROWS)], z_s.at[d], z_r.at[d], {"section": at.s - d}).wait_send()

    each(1, at.sections, drain_z)


def signal_to(device):
    pl.semaphore_signal(pltpu.get_barrier_semaphore(), inc=1, device_id=device, device_id_type=MESH)


def first_kernel(ids_ref, gates_ref, tokens_hbm, og_hbm, wg_hbm, wu_hbm, wd_hbm,
                 w_ref, u_out, base0_out, sel_out, cu_out, cg_out, hid_out, dg1_out, du1_out, dg_out, du_out, r_out,
                 wn_out, un_out, u0_out, seln_out, place, place_t, rn_out, ftok_out, counts_out,
                 xnat_hbm, y1_hbm, ynat_hbm, base_hbm,
                 tok_ref, tokv, ogv, wg, wu, wd, xown, xbuf, xnat, tokall, psend, precv, base, ynat1, stack, stackn, selw, *rest):
    wide, narrow, ynat, rest = rest[:8], rest[8:16], rest[16], rest[17:]
    loc, x_s, x_r, xrel_s, xrel_r, id_s, id_r, pc_s, pc_r, bs_s, bs_r = rest[:11]
    sems_w, sems_n = rest[11:21], rest[21:31]
    wide = wide[:2] + (ynat1,) + wide[2:]
    narrow = narrow[:2] + (ynat,) + narrow[2:]
    at = Place()
    width = u_out.shape[1]
    s, sections = at.s, at.sections
    half = ogv.shape[1]

    load_tokens = pltpu.make_async_copy(tokens_hbm, tokv, loc.at[0])
    load_og = pltpu.make_async_copy(og_hbm, ogv, loc.at[1])
    load_g = pltpu.make_async_copy(wg_hbm, wg, loc.at[2])
    load_u = pltpu.make_async_copy(wu_hbm, wu, loc.at[3])
    load_d = pltpu.make_async_copy(wd_hbm, wd, loc.at[4])
    for load in (load_tokens, load_og, load_g, load_u, load_d):
        load.start()

    for received in (wide[8], narrow[8]):
        received[...] = jnp.zeros_like(received)

    def greet(k):
        signal_to(at.peer(at.ahead(k)))

    each(1, CHIPS, greet)
    signal_to(at.partner)

    def greet_z(d):
        signal_to({"section": lax.rem(s + d, sections)})

    each(1, sections, greet_z)

    hits = ids_ref[...] == 0
    live = jnp.sum(jnp.where(hits, 1.0, 0.0), axis=0, keepdims=True)
    pair_weight = jnp.sum(jnp.where(hits, gates_ref[...], 0.0), axis=0, keepdims=True)
    before = jnp.where(iota((128, 128), 0) < iota((128, 128), 1), 1.0, 0.0).astype(BF)
    live16 = jnp.broadcast_to(live, (ROWS, 128))
    slot = nn(live16.astype(BF), before)
    lane16, row16 = iota((ROWS, 128), 1), iota((ROWS, 128), 0)
    mine16 = (live16 > 0.5) & (slot == lax.rem(row16, CAP).astype(F32))
    token = jnp.max(jnp.where(mine16, lane16.astype(F32), -1.0), axis=1, keepdims=True)
    tok_ref[...] = jnp.broadcast_to(token, (ROWS, 128))
    share = jnp.sum(jnp.where(mine16, jnp.broadcast_to(pair_weight, (ROWS, 128)), 0.0), axis=1, keepdims=True)
    w_ref[...] = jnp.broadcast_to(share, (ROWS, 128))

    mine_z = rows_at(s, ROWS)
    pl.semaphore_wait(pltpu.get_barrier_semaphore(), CHIPS + sections - 1)

    def send_ids(d):
        remote(tok_ref, tokall.at[mine_z], id_s.at[d], id_r.at[d], {"section": lax.rem(s + d, sections)}).start()

    each(1, sections, send_ids)
    tokall[mine_z, :] = tok_ref[...]

    load_tokens.wait()
    hit = tok_ref[...] == lane16.astype(F32)
    block = jnp.zeros((ROWS, width), F32)
    for q in range(QUARTERS):
        select = jnp.where(hit & (lax.div(row16, CAP) == q), 1.0, 0.0).astype(BF)
        block = block + nn(select, tokv[:, q * width : (q + 1) * width])
    xown[...] = block.astype(BF)
    xg = (at, xown, xbuf, x_s, x_r, xrel_s, xrel_r)
    gather_start(*xg[:5])

    load_og.wait()

    def wait_ids(d):
        source = lax.rem(s + sections - d, sections)
        remote(tok_ref, tokall.at[rows_at(source, ROWS)], id_s.at[d], id_r.at[d], at.partner).wait_recv()

    each(1, sections, wait_ids)
    tok_f = tokall[...]
    row, lane = iota((128, 128), 0), iota((128, 128), 1)
    pick = (tok_f == lane.astype(F32)) & (lax.rem(lax.div(row, CAP), QUARTERS) == lax.div(s, 2))
    psend[...] = nn(jnp.where(pick, 1.0, 0.0).astype(BF), ogv[...]).astype(BF)

    def send_piece(d):
        to = lax.rem(s + d, sections)
        remote(psend.at[rows_at(to, ROWS)], precv.at[mine_z], pc_s.at[d], pc_r.at[d], {"section": to}).start()

    each(1, sections, send_piece)
    precv[mine_z, :] = psend[mine_z, :]

    other = tok_f.T
    layer_r, layer_l = lax.div(row, ROWS), lax.div(lane, ROWS)
    part_r, part_l = lax.rem(lax.div(row, CAP), QUARTERS), lax.rem(lax.div(lane, CAP), QUARTERS)
    same = (tok_f == other) & (tok_f >= 0.0) & (part_r == part_l)
    above = jnp.where(same & (layer_l > layer_r), 1.0, 0.0)
    level_r = jnp.sum(above, axis=1, keepdims=True)
    level_l = jnp.sum(jnp.where(same & (layer_r > layer_l), 1.0, 0.0), axis=0, keepdims=True)
    dep_r, dep_l = level_r > 0.5, level_l > 0.5
    group = lax.div(row, CAP) == lax.div(lane, CAP)
    fellows = jnp.where(group & dep_l, 1.0, 0.0)
    busiest = jnp.max(jnp.sum(fellows, axis=1, keepdims=True), axis=0, keepdims=True)
    deepest = jnp.max(level_r, axis=0, keepdims=True)
    j_r = jnp.where(dep_r, jnp.sum(jnp.where(lane < row, fellows, 0.0), axis=1, keepdims=True), -1.0)
    take = jnp.where(lane16 == row16 + s * ROWS, 1.0, 0.0).astype(BF)
    level_own = nn(take, jnp.broadcast_to(level_r, (128, 128)).astype(BF))
    j_own = nn(take, jnp.broadcast_to(j_r, (128, 128)).astype(BF))

    def wait_piece(d):
        source = lax.rem(s + sections - d, sections)
        remote(psend.at[mine_z], precv.at[rows_at(source, ROWS)], pc_s.at[d], pc_r.at[d], at.partner).wait_recv()

    each(1, sections, wait_piece)

    for h in range(2):
        total = jnp.zeros((ROWS, half), F32)
        for p in range(h, 8, 2):
            total = total + precv[p * ROWS : (p + 1) * ROWS, :].astype(F32)
        base[:, h * half : (h + 1) * half] = total
    yown, ybuf = wide[0], wide[1]
    rstack, nstack = wide[8], narrow[8]
    root = level_own[:, :1] < 0.5
    weight = w_ref[:, :1]
    yown[:, :width] = jnp.where(root, weight * base[...], 0.0).astype(BF)
    marks = jnp.where(lane16 < 32, deepest, jnp.where(lane16 < 64, busiest, j_own))
    yown[:, width:] = marks.astype(BF)

    def send_base():
        def go(d):
            to = lax.rem(s + d, sections)
            remote(ogv, base_hbm.at[:, rows_at(s, half)], bs_s.at[d], bs_r.at[d], {"section": to}).start()

        each(1, sections, go)
        pltpu.make_async_copy(ogv, base_hbm.at[:, rows_at(s, half)], loc.at[5]).start()

    def tables():
        base0_out[...] = jnp.where(root, base[...], 0.0).astype(BF)
        chosen = jnp.where(level_l == level_r - 1.0, above, 0.0).astype(BF)
        sel_out[...] = nn(take, chosen).astype(BF)
        j_l = jnp.where(dep_l, jnp.sum(jnp.where(group & dep_r & (row < lane), 1.0, 0.0), axis=0, keepdims=True), -1.0)
        own = (lax.div(lane16, ROWS) == s) & (lax.div(row16, 4) == lax.rem(lax.div(lane16, CAP), QUARTERS))
        own = jnp.where(own & (j_l == lax.rem(row16, 2).astype(F32)), 1.0, 0.0).astype(BF)
        token_n = nn(own, (tok_f + 1.0).astype(BF)) - 1.0
        share_n = jnp.sum(jnp.where(token_n == lane16.astype(F32), jnp.broadcast_to(pair_weight, (ROWS, 128)), 0.0),
                          axis=1, keepdims=True)
        wn_out[...] = jnp.broadcast_to(share_n, (ROWS, 128))
        onto = nn(own, chosen)
        for h in range(2):
            from_wide = (lax.rem(lax.div(row16, 2), 2) == h) & (level_l < 0.5)
            selw[h * ROWS : (h + 1) * ROWS, :] = jnp.where(from_wide, onto, 0.0).astype(BF)
        shrink = (layer_r == layer_l) & (part_r == lax.div(lax.rem(lane, ROWS), 4)) & (j_r == lax.rem(lane, 2).astype(F32))
        shrink = jnp.where(shrink, 1.0, 0.0).astype(BF)
        eighth = lax.div(row16, 2) == lax.div(lax.rem(lane16, ROWS), 2)
        seln_out[...] = jnp.where(eighth, nn(onto.astype(BF), shrink), 0.0).astype(BF)
        later = jnp.sum(jnp.where(same & (layer_r < layer_l) & (layer_r >= s), 1.0, 0.0), axis=0, keepdims=True)
        lane1 = iota((1, 128), 1)
        tok_l = jnp.max(other, axis=0, keepdims=True)
        ftok = jnp.where((later < 0.5) & (lax.div(lane1, ROWS) >= s), tok_l, -1.0)
        ftok_n = nn(jnp.broadcast_to(jnp.where(dep_l, ftok + 1.0, 0.0), (ROWS, 128)).astype(BF), shrink) - 1.0
        ftok_out[0:8, :] = jnp.broadcast_to(ftok, (8, 128))
        ftok_out[8:16, :] = jnp.broadcast_to(jnp.where(dep_l, -1.0, ftok), (8, 128))
        ftok_out[16:24, :] = ftok_n[:8]

    def activations():
        send_base()
        tables()
        gather_finish(*xg)
        form_w.expand(xbuf, xnat)
        pltpu.make_async_copy(xnat, xnat_hbm, loc.at[6]).start()
        load_g.wait()
        load_u.wait()
        gate = project(xnat, wg, width)
        up = project(xnat, wu, width)
        sig = 1.0 / (1.0 + jnp.exp(-gate))
        act = gate * sig
        hid_out[...] = (act * up).astype(BF)
        cu_out[...] = act
        cg_out[...] = up * sig * (1.0 + gate * (1.0 - sig))

    def places():
        all_marks = ybuf[:, width : width + MARK].astype(F32)
        lanes = iota(all_marks.shape, 1)
        counts_out[0] = jnp.max(jnp.where(lanes < 32, all_marks, 0.0)).astype(jnp.int32)
        counts_out[1] = jnp.max(jnp.where((lanes >= 32) & (lanes < 64), all_marks, 0.0)).astype(jnp.int32)
        r64, c64 = iota((128, 64), 0), iota((128, 64), 1)
        slot_of = (lax.rem(lax.div(r64, 4), 4) == lax.div(c64, ROWS)) & (lax.rem(r64, 4) == lax.rem(c64, ROWS))
        slot_of = jnp.where(slot_of, 1.0, 0.0).astype(BF)
        fits = (lax.rem(lax.div(row, 4), 4) == lax.div(lane, ROWS)) & (lax.div(row, ROWS) == lax.rem(lax.div(lane, 2), 8))

        def one(t):
            slots = nn(slot_of, ybuf[rows_at(t, 64), width : width + MARK])
            e = jnp.where(fits & (slots[:, MARK - 1 :] == lax.rem(lane, 2).astype(F32)), 1.0, 0.0)
            place[rows_at(t, 128), :] = e.astype(BF)
            place_t[rows_at(t, 64), :] = e.T[:64].astype(BF)

        each(0, TILES, one)
        pltpu.make_async_copy(ynat1, y1_hbm, loc.at[8]).start()

    weights, coefs = (wg, wu, wd), (cu_out, cg_out)
    form_w, form_n = Wide(stack), Narrow(stackn, place, place_t)
    one_round(at, form_w, lambda: base[...], wide, weights, coefs, (dg1_out, du1_out), sems_w,
              during_gather=activations, before_grads=load_d.wait, during_sends=places)

    start = jnp.zeros(u0_out.shape, F32)
    for h in range(2):
        start = start + nn(selw[h * ROWS : (h + 1) * ROWS, :], rstack[:, h * half : (h + 1) * half])
    u0_out[...] = start.astype(BF)
    narrow[0][...] = (wn_out[:, :1] * start).astype(BF)

    def rest_of_wide():
        u_out[...] = (nn(sel_out[...], rstack[...]) + base0_out[...].astype(F32)).astype(BF)
        r_out[...] = rstack[...]

    def add_up():
        for total, first in ((dg_out, dg1_out), (du_out, du1_out), (ynat, ynat1)):
            total[...] = total[...] + first[...]
        pltpu.make_async_copy(ynat, ynat_hbm, loc.at[7]).start()

    one_round(at, form_n, lambda: u0_out[...].astype(F32), narrow, weights, coefs, (dg_out, du_out), sems_n,
              during_gather=rest_of_wide, during_sends=add_up)
    un_out[...] = (nn(seln_out[...], nstack[...]) + u0_out[...].astype(F32)).astype(BF)
    rn_out[...] = nstack[...]

    gather_drain(*xg)

    def drain_z(d):
        to = lax.rem(s + d, sections)
        source = lax.rem(s + sections - d, sections)
        remote(tok_ref, tokall.at[mine_z], id_s.at[d], id_r.at[d], at.partner).wait_send()
        remote(psend.at[rows_at(to, ROWS)], precv.at[mine_z], pc_s.at[d], pc_r.at[d], at.partner).wait_send()
        into = remote(ogv, base_hbm.at[:, rows_at(source, half)], bs_s.at[d], bs_r.at[d], at.partner)
        into.wait_send()
        into.wait_recv()

    each(1, sections, drain_z)
    round_drain(at, wide, sems_w)
    round_drain(at, narrow, sems_n)
    pltpu.make_async_copy(ogv, base_hbm.at[:, rows_at(s, half)], loc.at[5]).wait()
    pltpu.make_async_copy(xnat, xnat_hbm, loc.at[6]).wait()
    pltpu.make_async_copy(ynat, ynat_hbm, loc.at[7]).wait()
    pltpu.make_async_copy(ynat1, y1_hbm, loc.at[8]).wait()


def enter_round(at, wg_hbm, wu_hbm, wd_hbm, wg, wu, wd, loc, rstack):
    loads = [pltpu.make_async_copy(a, b, loc.at[i]) for i, (a, b) in enumerate(((wd_hbm, wd), (wg_hbm, wg), (wu_hbm, wu)))]
    for load in loads:
        load.start()
    rstack[...] = jnp.zeros_like(rstack)

    def greet(k):
        signal_to(at.peer(at.ahead(k)))

    each(1, CHIPS, greet)
    signal_to(at.partner)

    def greet_z(d):
        @pl.when(at.s + d < at.sections)
        def _():
            signal_to({"section": at.s + d})

    each(1, at.sections, greet_z)

    def loaded():
        for load in loads:
            load.wait()

    return loaded


def next_wide(u_ref, w_ref, base0_ref, sel_ref, cu_ref, cg_ref, wg_hbm, wu_hbm, wd_hbm,
              u_out, dg_out, du_out, r_out, ynat_hbm, wg, wu, wd, ynat, stack, *rest):
    at = Place()
    bufs, loc, sems = rest[:2] + (ynat,) + rest[2:8], rest[8], rest[9:]
    width = u_out.shape[1]
    yown, rstack = bufs[0], bufs[8]
    loaded = enter_round(at, wg_hbm, wu_hbm, wd_hbm, wg, wu, wd, loc, rstack)
    yown[:, :width] = (w_ref[:, :1] * u_ref[...].astype(F32)).astype(BF)
    yown[:, width:] = jnp.zeros((ROWS, MARK), BF)
    pl.semaphore_wait(pltpu.get_barrier_semaphore(), CHIPS + at.s)

    def put():
        pltpu.make_async_copy(ynat, ynat_hbm, loc.at[3]).start()

    one_round(at, Wide(stack), lambda: u_ref[...].astype(F32), bufs, (wg, wu, wd), (cu_ref, cg_ref), (dg_out, du_out), sems,
              before_grads=loaded, during_sends=put)
    u_out[...] = (nn(sel_ref[...], rstack[...]) + base0_ref[...].astype(F32)).astype(BF)
    r_out[...] = rstack[...]
    round_drain(at, bufs, sems)
    pltpu.make_async_copy(ynat, ynat_hbm, loc.at[3]).wait()


def next_narrow(u_ref, w_ref, u0_ref, sel_ref, place, place_t, cu_ref, cg_ref, dg1_ref, du1_ref, y1_hbm, wg_hbm, wu_hbm, wd_hbm,
                u_out, dg_out, du_out, r_out, ynat_hbm, wg, wu, wd, y1, ynat, stack, *rest):
    at = Place()
    bufs, loc, sems = rest[:2] + (ynat,) + rest[2:8], rest[8], rest[9:]
    yown, rstack = bufs[0], bufs[8]
    loaded = enter_round(at, wg_hbm, wu_hbm, wd_hbm, wg, wu, wd, loc, rstack)
    pltpu.make_async_copy(y1_hbm, y1, loc.at[4]).start()
    yown[...] = (w_ref[:, :1] * u_ref[...].astype(F32)).astype(BF)
    pl.semaphore_wait(pltpu.get_barrier_semaphore(), CHIPS + at.s)

    def add_up():
        pltpu.make_async_copy(y1_hbm, y1, loc.at[4]).wait()
        for total, first in ((dg_out, dg1_ref), (du_out, du1_ref), (ynat, y1)):
            total[...] = total[...] + first[...]
        pltpu.make_async_copy(ynat, ynat_hbm, loc.at[3]).start()

    one_round(at, Narrow(stack, place, place_t), lambda: u_ref[...].astype(F32), bufs, (wg, wu, wd), (cu_ref, cg_ref),
              (dg_out, du_out), sems, before_grads=loaded, during_sends=add_up)
    u_out[...] = (nn(sel_ref[...], rstack[...]) + u0_ref[...].astype(F32)).astype(BF)
    r_out[...] = rstack[...]
    round_drain(at, bufs, sems)
    pltpu.make_async_copy(ynat, ynat_hbm, loc.at[3]).wait()


def last_kernel(dg, du, hid, x, y, rows, rows_n, ftok, counts, base, grad_in, grad_gate, grad_up, grad_down, dt):
    q = pl.program_id(0)

    @pl.when(q == 0)
    def _():
        slots = dg.shape[0]
        unit = jnp.where(iota((slots, slots), 0) == iota((slots, slots), 1), 1.0, 0.0).astype(BF)
        for i, part in enumerate((dg, du, hid)):
            dt[i] = lax.dot_general(part[...], unit, (((0,), (0,)), ((), ())), preferred_element_type=F32).astype(BF)

    grad_gate[0] = nn(dt[0], x[...]).astype(BF)
    grad_up[0] = nn(dt[1], x[...]).astype(BF)
    grad_down[0] = nn(dt[2], y[...]).astype(BF)
    tokens, width = grad_in.shape[1:]
    lane = iota((tokens, 128), 1)
    token = iota((tokens, 128), 0).astype(F32)
    wide_only = counts[1] > 2
    ftok_w = jnp.where(wide_only, ftok[0:1, :], ftok[8:9, :])
    ftok_n = jnp.where(wide_only, -1.0, ftok[16:17, :])
    select = jnp.where((ftok_w == token) & (lax.rem(lax.div(lane, CAP), QUARTERS) == q), 1.0, 0.0)
    new = nn(select.astype(BF), rows[...])
    halves = []
    for h in range(2):
        select_n = jnp.where((ftok_n == token) & (lax.rem(lax.div(lane, 2), 8) == 2 * q + h), 1.0, 0.0)
        halves.append(nn(select_n.astype(BF), rows_n[...]))
    new = new + jnp.concatenate(halves, axis=1)
    live = jnp.sum(select + select_n, axis=1, keepdims=True) > 0.5
    grad_in[0] = jnp.where(live, new, base[...].astype(F32)).astype(BF)


def round_scratch(width, mark):
    blocks = 2 * CHIPS * ROWS
    shapes = [(ROWS, width + mark), (blocks, width + mark)] + [(blocks // 2, width)] * 4 + [(ROWS, width), (8 * ROWS, width)]
    return [pltpu.VMEM(dims, BF) for dims in shapes]


def round_sems():
    sem = pltpu.SemaphoreType.DMA
    return [sem((CHIPS,))] * 4 + [sem((NX,))] * 2 + [sem((CHIPS,))] * 2 + [sem((8,))] * 2


def on_device(saved_inputs, expert_ids, gate_weights, out_grad, gate_w, up_w, down_w):
    tokens, wg, wu, wd = saved_inputs[0], gate_w[0], up_w[0], down_w[0]
    count, d = tokens.shape
    units = wg.shape[0]
    width = d // QUARTERS
    half = width // 2
    slots = lax.axis_size("ep") * CAP
    ids, gates = expert_ids[0].T, gate_weights[0].T

    hbm = pl.BlockSpec(memory_space=pl.ANY)
    vmem = pl.BlockSpec(memory_space=pltpu.VMEM)
    smem = pl.BlockSpec(memory_space=pltpu.SMEM)
    sem = pltpu.SemaphoreType.DMA

    def vm(*dims, dtype=BF):
        return pltpu.VMEM(dims, dtype)

    def shape(*dims, dtype=BF):
        return jax.ShapeDtypeStruct(dims, dtype)

    def params(which):
        return pltpu.CompilerParams(collective_id=which, has_side_effects=True, vmem_limit_bytes=60 * 2**20)

    block, block_n, part = (ROWS, width), (ROWS, half), (slots, units)
    (weight, u, base0, select_up, cu, cg, hid, dg1, du1, dg, du, rows, weight_n, un, u0, select_n, place, place_t, rows_n, ftok,
     counts, x, y1, y, base) = pl.pallas_call(
        first_kernel,
        name="first_rounds",
        out_shape=[shape(ROWS, 128, dtype=F32), shape(*block), shape(*block), shape(ROWS, 128), shape(*part, dtype=F32),
                   shape(*part, dtype=F32), shape(*part), shape(*part), shape(*part), shape(*part), shape(*part),
                   shape(128, width), shape(ROWS, 128, dtype=F32), shape(*block_n), shape(*block_n), shape(ROWS, 128),
                   shape(TILES * 128, 128), shape(TILES * 64, 128), shape(128, half), shape(24, 128, dtype=F32),
                   shape(2, dtype=jnp.int32), shape(slots, d), shape(slots, d), shape(slots, d), shape(count, d)],
        in_specs=[vmem] * 2 + [hbm] * 5,
        out_specs=[vmem] * 20 + [smem] + [hbm] * 4,
        scratch_shapes=[
            vm(ROWS, 128, dtype=F32), vm(count, d), vm(*out_grad.shape), vm(units, d), vm(units, d), vm(units, d),
            vm(*block), vm(2 * CHIPS * ROWS, width), vm(slots, d), vm(128, 128, dtype=F32),
            vm(128, half), vm(128, half), vm(*block, dtype=F32), vm(slots, d), vm(TILES * 64, width), vm(TILES * 128, half),
            vm(2 * ROWS, 128),
        ] + round_scratch(width, MARK) + round_scratch(half, 0)[:8] + [vm(slots, d)] + [
            sem((9,)), sem((CHIPS,)), sem((CHIPS,)), sem((CHIPS,)), sem((CHIPS,)),
            sem((8,)), sem((8,)), sem((8,)), sem((8,)), sem((8,)), sem((8,)),
        ] + round_sems() + round_sems(),
        compiler_params=params(0),
    )(ids, gates, tokens, out_grad, wg, wu, wd)

    three = [vm(units, d)] * 3

    def more_narrow(_, state):
        un = state[0]
        return tuple(pl.pallas_call(
            next_narrow,
            name="next_narrow",
            out_shape=[shape(*block_n), shape(*part), shape(*part), shape(128, half), shape(slots, d)],
            in_specs=[vmem] * 10 + [hbm] * 4,
            out_specs=[vmem] * 4 + [hbm],
            scratch_shapes=three + [vm(slots, d), vm(slots, d), vm(TILES * 128, half)] + round_scratch(half, 0) + [sem((5,))]
            + round_sems(),
            compiler_params=params(1),
        )(un, weight_n, u0, select_n, place, place_t, cu, cg, dg1, du1, y1, wg, wu, wd))

    def more_wide(_, state):
        u = state[0]
        return tuple(pl.pallas_call(
            next_wide,
            name="next_wide",
            out_shape=[shape(*block), shape(*part), shape(*part), shape(128, width), shape(slots, d)],
            in_specs=[vmem] * 6 + [hbm] * 3,
            out_specs=[vmem] * 4 + [hbm],
            scratch_shapes=three + [vm(slots, d), vm(TILES * 64, width)] + round_scratch(width, MARK) + [sem((4,))] + round_sems(),
            compiler_params=params(2),
        )(u, weight, base0, select_up, cu, cg, wg, wu, wd))

    deepest, busiest = counts[0], counts[1]
    narrow_rounds = jnp.where(busiest > 2, 0, deepest - 1)
    wide_rounds = jnp.where(busiest > 2, deepest, 0)
    un, dg, du, rows_n, y = lax.fori_loop(0, narrow_rounds, more_narrow, (un, dg, du, rows_n, y))
    u, dg, du, rows, y = lax.fori_loop(0, wide_rounds, more_wide, (u, dg, du, rows, y))

    full = pl.BlockSpec(part, lambda i: (0, 0))
    cols = pl.BlockSpec((slots, width), lambda i: (0, i))
    grad = pl.BlockSpec((1, units, width), lambda i: (0, 0, i))
    return pl.pallas_call(
        last_kernel,
        name="gradients",
        grid=(QUARTERS,),
        out_shape=[shape(1, count, d), shape(1, units, d), shape(1, units, d), shape(1, units, d)],
        in_specs=[full, full, full, cols, cols, pl.BlockSpec((128, width), lambda i: (0, 0)),
                  pl.BlockSpec((128, half), lambda i: (0, 0)), pl.BlockSpec((24, 128), lambda i: (0, 0)), smem, cols],
        out_specs=[pl.BlockSpec((1, count, width), lambda i: (0, 0, i)), grad, grad, grad],
        scratch_shapes=[vm(3, units, slots)],
        compiler_params=pltpu.CompilerParams(vmem_limit_bytes=60 * 2**20),
    )(dg, du, hid, x, y, rows, rows_n, ftok, counts, base)


def solution(mesh):
    split = P("section", "ep", None)
    return jax.shard_map(
        on_device,
        mesh=mesh,
        in_specs=(split, split, split, P("ep", "section"), split, split, split),
        out_specs=(split, split, split, split),
        check_vma=False,
    )
```

```python
import functools

import jax
import jax.numpy as jnp
from jax import lax
from jax.experimental import pallas as pl
from jax.experimental.pallas import tpu as pltpu
from jax.sharding import PartitionSpec as P

MESH = pl.DeviceIdType.MESH
CAP = 4
NX, NY = 4, 4
CHIPS = NX * NY
SELF = (NX // 2) * NY + NY // 2
Z_ORDER = (4, 3, 5, 2, 6, 1, 7)
QUARTERS = 4
TILES = 2 * CHIPS * CAP // 16
ROWS = QUARTERS * CAP
MARK = 128
BF, F32 = jnp.bfloat16, jnp.float32


def iota(shape, dim):
    return lax.broadcasted_iota(jnp.int32, shape, dim)


def rows_at(index, size):
    return pl.ds(pl.multiple_of(index * size, size), size)


def swap_matrix():
    i, m = iota((64, 64), 0), iota((64, 64), 1)
    swapped = (lax.rem(lax.div(m, 4), 4) * 16) + (lax.div(m, 16) * 4) + lax.rem(m, 4)
    return jnp.where(i == swapped, 1.0, 0.0).astype(BF)


def nt(a, b):
    return lax.dot_general(a, b, (((1,), (1,)), ((), ())), preferred_element_type=F32)


def nn(a, b):
    return lax.dot_general(a, b, (((1,), (0,)), ((), ())), preferred_element_type=F32)


class Place:
    def __init__(self):
        self.s = lax.axis_index("section")
        self.sections = lax.axis_size("section")
        ep = lax.axis_index("ep")
        self.core = lax.rem(ep, 2)
        self.chip = lax.div(ep, 2)
        self.x = lax.div(self.chip, NY)
        self.y = lax.rem(self.chip, NY)
        self.partner = {"ep": self.chip * 2 + 1 - self.core}

    def ahead(self, k):
        i, j = lax.div(k, NY) + NX // 2, lax.rem(k, NY) + NY // 2
        return lax.rem(self.x + i, NX) * NY + lax.rem(self.y + j, NY)

    def behind(self, k):
        i, j = lax.div(k, NY) + NX // 2, lax.rem(k, NY) + NY // 2
        return lax.rem(self.x + 2 * NX - i, NX) * NY + lax.rem(self.y + 2 * NY - j, NY)

    def peer(self, chip):
        return {"ep": chip * 2 + self.core}

    def block(self, core, chip):
        return rows_at(core * CHIPS + chip, ROWS)


def remote(src, dst, send, recv, device):
    return pltpu.make_async_remote_copy(
        src_ref=src, dst_ref=dst, send_sem=send, recv_sem=recv, device_id=device, device_id_type=MESH
    )


def each(lo, hi, body):
    lax.fori_loop(lo, hi, lambda k, carry: (body(k), carry)[1], 0)


def each_other(body):
    each(0, SELF, body)
    each(SELF + 1, CHIPS, body)


def gather_start(at, own, buf, send, recv):
    mine = at.block(at.core, at.chip)

    def go(k):
        remote(own, buf.at[mine], send.at[k], recv.at[k], at.peer(at.ahead(k))).start()

    each_other(go)
    remote(own, buf.at[mine], send.at[SELF], recv.at[SELF], at.partner).start()
    buf[mine, :] = own[...]


def gather_finish(at, own, buf, send, recv, relay_send, relay_recv, form, nat):
    def row_of(i):
        return lax.rem(at.x + 2 * NX - (i + NX // 2), NX)

    def mine(i):
        def forward(j):
            k = i * NY + j

            @pl.when(k != SELF)
            def _():
                piece = at.block(at.core, at.behind(k))
                remote(own, buf.at[piece], send.at[k], recv.at[k], at.partner).wait_recv()
                remote(buf.at[piece], buf.at[piece], relay_send.at[k], relay_recv.at[k], at.partner).start()

        each(0, NY, forward)

    each(0, NX, mine)
    each(0, NX, lambda t: form.expand(buf, nat, at.core * NX + t))

    def theirs(i):
        def take(j):
            k = i * NY + j
            piece = at.block(1 - at.core, at.behind(k))

            @pl.when(k != SELF)
            def _():
                remote(buf.at[piece], buf.at[piece], relay_send.at[k], relay_recv.at[k], at.partner).wait_recv()

            @pl.when(k == SELF)
            def _():
                remote(own, buf.at[piece], send.at[k], recv.at[k], at.partner).wait_recv()

        each(0, NY, take)
        form.expand(buf, nat, (1 - at.core) * NX + row_of(i))

    each(0, NX, theirs)


def gather_drain(at, own, buf, send, recv, relay_send, relay_recv):
    def drain(k):
        remote(own, buf.at[at.block(at.core, at.chip)], send.at[k], recv.at[k], at.partner).wait_send()

    each(0, CHIPS, drain)

    def drain_relay(k):
        piece = at.block(at.core, at.behind(k))
        remote(buf.at[piece], buf.at[piece], relay_send.at[k], relay_recv.at[k], at.partner).wait_send()

    each_other(drain_relay)


class Wide:
    parts = QUARTERS

    def __init__(self, stack):
        self.stack, self.width = stack, stack.shape[1]

    def expand(self, buf, nat, t):
        width = self.width
        tile = nn(swap_matrix(), buf[rows_at(t, 64), :width]).astype(BF)
        for q in range(QUARTERS):
            nat[rows_at(t, ROWS), q * width : (q + 1) * width] = tile[q * ROWS : (q + 1) * ROWS]

    def fill(self, q, value):
        for t in range(TILES):
            self.stack[rows_at(t * QUARTERS + q, ROWS), :] = value[t * ROWS : (t + 1) * ROWS]

    def pack(self, t):
        return nn(swap_matrix(), self.stack[rows_at(t, 64), :])


class Narrow:
    parts = 2 * QUARTERS

    def __init__(self, stack, place, place_t):
        self.stack, self.width = stack, stack.shape[1]
        self.place, self.place_t = place, place_t

    def expand(self, buf, nat, t):
        width = self.width
        tile = nn(self.place[rows_at(t, 128), :64], buf[rows_at(t, 64), :]).astype(BF)
        for q in range(2 * QUARTERS):
            nat[rows_at(t, ROWS), q * width : (q + 1) * width] = tile[q * ROWS : (q + 1) * ROWS]

    def fill(self, q, value):
        for t in range(TILES):
            for h in range(2):
                self.stack[rows_at(t * 2 * QUARTERS + q * 2 + h, ROWS), :] = value[
                    t * ROWS : (t + 1) * ROWS, h * self.width : (h + 1) * self.width
                ]

    def pack(self, t):
        return nn(self.place_t[rows_at(t, 64), :], self.stack[rows_at(t, 128), :])


def project(nat, weight, width):
    def step(q, acc):
        cols = rows_at(q, width)
        return acc + nt(nat[:, cols], weight[:, cols])

    return lax.fori_loop(0, QUARTERS, step, jnp.zeros((nat.shape[0], weight.shape[0]), F32))


def one_round(at, form, upstream, bufs, weights, coefs, grads, sems, during_gather=None,
              before_grads=None, during_sends=None):
    yown, ybuf, ynat, pbuf, drecv, sbuf, rbuf, rown, rstack = bufs
    (ag_s, ag_r, rel_s, rel_r, dd_s, dd_r, rs_s, rs_r, z_s, z_r) = sems
    wg, wu, wd = weights
    dg, du = grads
    width = wg.shape[1] // QUARTERS
    gather_start(at, yown, ybuf, ag_s, ag_r)
    if during_gather is not None:
        during_gather()
    gather_finish(at, yown, ybuf, ag_s, ag_r, rel_s, rel_r, form, ynat)
    if before_grads is not None:
        before_grads()
    grad_hidden = project(ynat, wd, width)
    du[...] = (grad_hidden * coefs[0][...]).astype(BF)
    dg[...] = (grad_hidden * coefs[1][...]).astype(BF)

    def back(q):
        cols = rows_at(q, width)
        form.fill(q, (nn(dg[...], wg[:, cols]) + nn(du[...], wu[:, cols])).astype(BF))

    each(0, QUARTERS, back)

    def to_partner(jj):
        j = lax.rem(at.x + jj + NX // 2, NX)
        part = rows_at(j, 64)
        pbuf[part, :] = form.pack((1 - at.core) * NX + j).astype(BF)
        remote(pbuf.at[part], drecv.at[part], dd_s.at[jj], dd_r.at[jj], at.partner).start()

    each(0, NX, to_partner)

    def to_homes(jj):
        j = lax.rem(at.x + jj + NX // 2, NX)
        part = rows_at(j, 64)
        mine = form.pack(at.core * NX + j)
        remote(pbuf.at[part], drecv.at[part], dd_s.at[jj], dd_r.at[jj], at.partner).wait_recv()
        sbuf[part, :] = (mine + drecv[part, :].astype(F32)).astype(BF)

        def send(m):
            k = jj * NY + m

            @pl.when(k != SELF)
            def _():
                chip = at.ahead(k)
                remote(sbuf.at[rows_at(chip, ROWS)], rbuf.at[rows_at(k, ROWS)], rs_s.at[k], rs_r.at[k], at.peer(chip)).start()

        each(0, NY, send)

    each(0, NX, to_homes)
    if during_sends is not None:
        during_sends()

    def add(k, acc):
        here = rows_at(k, ROWS)
        remote(sbuf.at[here], rbuf.at[here], rs_s.at[k], rs_r.at[k], at.partner).wait_recv()
        return acc + rbuf[here, :].astype(F32)

    total = lax.fori_loop(0, SELF, add, sbuf[rows_at(at.chip, ROWS), :].astype(F32))
    total = lax.fori_loop(SELF + 1, CHIPS, add, total)
    row = (upstream() + total).astype(BF)
    rown[...] = row
    mine = rows_at(at.s, ROWS)
    rstack[mine, :] = row

    def down(d):
        @pl.when(at.s >= d)
        def _():
            remote(rown, rstack.at[mine], z_s.at[d], z_r.at[d], {"section": at.s - d}).start()

    for d in Z_ORDER:
        down(d)

    def up(d):
        @pl.when(at.s + d < at.sections)
        def _():
            remote(rown, rstack.at[rows_at(at.s + d, ROWS)], z_s.at[d], z_r.at[d], {"section": at.s + d}).wait_recv()

    for d in Z_ORDER:
        up(d)


def round_drain(at, bufs, sems):
    yown, ybuf, ynat, pbuf, drecv, sbuf, rbuf, rown, rstack = bufs
    (ag_s, ag_r, rel_s, rel_r, dd_s, dd_r, rs_s, rs_r, z_s, z_r) = sems
    gather_drain(at, yown, ybuf, ag_s, ag_r, rel_s, rel_r)

    def drain_partner(jj):
        part = rows_at(jj, 64)
        remote(pbuf.at[part], drecv.at[part], dd_s.at[jj], dd_r.at[jj], at.partner).wait_send()

    each(0, NX, drain_partner)

    def drain_homes(k):
        here = rows_at(k, ROWS)
        remote(sbuf.at[here], rbuf.at[here], rs_s.at[k], rs_r.at[k], at.partner).wait_send()

    each_other(drain_homes)

    def drain_z(d):
        @pl.when(at.s >= d)
        def _():
            remote(rown, rstack.at[rows_at(at.s, ROWS)], z_s.at[d], z_r.at[d], {"section": at.s - d}).wait_send()

    each(1, at.sections, drain_z)


def signal_to(device):
    pl.semaphore_signal(pltpu.get_barrier_semaphore(), inc=1, device_id=device, device_id_type=MESH)


def first_kernel(ids_ref, gates_ref, tokens_hbm, og_hbm, wg_hbm, wu_hbm, wd_hbm,
                 w_ref, u_out, base0_out, sel_out, cu_out, cg_out, hid_out, dg1_out, du1_out, dg_out, du_out, r_out,
                 wn_out, un_out, u0_out, seln_out, place, place_t, rn_out, ftok_out, narrow_out, wide_out,
                 xnat_hbm, y1_hbm, ynat_hbm, base_out,
                 tok_ref, tokv, ogv, wg, wu, wd, xown, xbuf, xnat, tokall, psend, precv, base, ynat1, ynat, stack, stackn, selw, *rest):
    wide, narrow, rest = rest[:8], rest[8:16], rest[16:]
    loc, x_s, x_r, xrel_s, xrel_r, id_s, id_r, pc_s, pc_r, bs_s, bs_r = rest[:11]
    sems_w, sems_n = rest[11:21], rest[21:31]
    wide = wide[:2] + (ynat1,) + wide[2:]
    narrow = narrow[:2] + (ynat,) + narrow[2:]
    at = Place()
    width = u_out.shape[1]
    s, sections = at.s, at.sections
    half = ogv.shape[1]

    load_tokens = pltpu.make_async_copy(tokens_hbm, tokv, loc.at[0])
    load_og = pltpu.make_async_copy(og_hbm, ogv, loc.at[1])
    load_g = pltpu.make_async_copy(wg_hbm, wg, loc.at[2])
    load_u = pltpu.make_async_copy(wu_hbm, wu, loc.at[3])
    load_d = pltpu.make_async_copy(wd_hbm, wd, loc.at[4])
    for load in (load_tokens, load_og, load_g, load_u, load_d):
        load.start()

    for received in (wide[8], narrow[8]):
        received[...] = jnp.zeros_like(received)

    def greet(k):
        signal_to(at.peer(at.ahead(k)))

    each_other(greet)
    signal_to(at.partner)

    def greet_z(d):
        signal_to({"section": lax.rem(s + d, sections)})

    each(1, sections, greet_z)

    hits = ids_ref[...] == 0
    live = jnp.sum(jnp.where(hits, 1.0, 0.0), axis=0, keepdims=True)
    pair_weight = jnp.sum(jnp.where(hits, gates_ref[...], 0.0), axis=0, keepdims=True)
    before = jnp.where(iota((128, 128), 0) < iota((128, 128), 1), 1.0, 0.0).astype(BF)
    live16 = jnp.broadcast_to(live, (ROWS, 128))
    slot = nn(live16.astype(BF), before)
    lane16, row16 = iota((ROWS, 128), 1), iota((ROWS, 128), 0)
    mine16 = (live16 > 0.5) & (slot == lax.rem(row16, CAP).astype(F32))
    token = jnp.max(jnp.where(mine16, lane16.astype(F32), -1.0), axis=1, keepdims=True)
    tok_ref[...] = jnp.broadcast_to(token, (ROWS, 128)).astype(BF)
    share = jnp.sum(jnp.where(mine16, jnp.broadcast_to(pair_weight, (ROWS, 128)), 0.0), axis=1, keepdims=True)
    w_ref[...] = jnp.broadcast_to(share, (ROWS, 128))

    mine_z = rows_at(s, ROWS)
    pl.semaphore_wait(pltpu.get_barrier_semaphore(), CHIPS + sections - 1)

    def send_ids(d):
        remote(tok_ref, tokall.at[mine_z], id_s.at[d], id_r.at[d], {"section": lax.rem(s + d, sections)}).start()

    for d in Z_ORDER:
        send_ids(d)
    tokall[mine_z, :] = tok_ref[...]

    load_tokens.wait()
    hit = token == lane16.astype(F32)
    block = jnp.zeros((ROWS, width), F32)
    for q in range(QUARTERS):
        select = jnp.where(hit & (lax.div(row16, CAP) == q), 1.0, 0.0).astype(BF)
        block = block + nn(select, tokv[:, q * width : (q + 1) * width])
    xown[...] = block.astype(BF)
    xg = (at, xown, xbuf, x_s, x_r, xrel_s, xrel_r)
    gather_start(*xg[:5])

    load_og.wait()

    def wait_ids(d):
        source = lax.rem(s + sections - d, sections)
        remote(tok_ref, tokall.at[rows_at(source, ROWS)], id_s.at[d], id_r.at[d], at.partner).wait_recv()

    for d in Z_ORDER:
        wait_ids(d)
    tok_f = tokall[...].astype(F32)
    row, lane = iota((128, 128), 0), iota((128, 128), 1)
    for_slot = tok_f == lane.astype(F32)
    pieces = jnp.zeros((128, 128), F32)
    for u in range(half // 128):
        pick = jnp.where(for_slot & (lax.rem(lax.div(row, CAP), QUARTERS) == u), 1.0, 0.0).astype(BF)
        pieces = pieces + nn(pick, ogv[:, u * 128 : (u + 1) * 128])
    psend[...] = pieces.astype(BF)

    def send_piece(d):
        to = lax.rem(s + d, sections)
        remote(psend.at[rows_at(to, ROWS)], precv.at[mine_z], pc_s.at[d], pc_r.at[d], {"section": to}).start()

    for d in Z_ORDER:
        send_piece(d)
    precv[mine_z, :] = psend[mine_z, :]

    other = tok_f.T
    layer_r, layer_l = lax.div(row, ROWS), lax.div(lane, ROWS)
    part_r, part_l = lax.rem(lax.div(row, CAP), QUARTERS), lax.rem(lax.div(lane, CAP), QUARTERS)
    same = (tok_f == other) & (tok_f >= 0.0) & (part_r == part_l)
    above = jnp.where(same & (layer_l > layer_r), 1.0, 0.0)
    level_r = jnp.sum(above, axis=1, keepdims=True)
    level_l = jnp.sum(jnp.where(same & (layer_r > layer_l), 1.0, 0.0), axis=0, keepdims=True)
    dep_r, dep_l = level_r > 0.5, level_l > 0.5
    group = lax.div(row, CAP) == lax.div(lane, CAP)
    fellows = jnp.where(group & dep_l, 1.0, 0.0)
    busiest = jnp.max(jnp.sum(fellows, axis=1, keepdims=True), axis=0, keepdims=True)
    deepest = jnp.max(level_r, axis=0, keepdims=True)
    j_r = jnp.where(dep_r, jnp.sum(jnp.where(lane < row, fellows, 0.0), axis=1, keepdims=True), -1.0)
    take = jnp.where(lane16 == row16 + s * ROWS, 1.0, 0.0).astype(BF)
    level_own = nn(take, jnp.broadcast_to(level_r, (128, 128)).astype(BF))
    j_own = nn(take, jnp.broadcast_to(j_r, (128, 128)).astype(BF))

    def wait_piece(d):
        source = lax.rem(s + sections - d, sections)
        remote(psend.at[mine_z], precv.at[rows_at(source, ROWS)], pc_s.at[d], pc_r.at[d], at.partner).wait_recv()

    for d in Z_ORDER:
        wait_piece(d)

    for h in range(2):
        for u in range(half // 128):
            source = (lax.div(lane16, ROWS) == 2 * lax.div(row16, CAP) + h) & (lax.rem(lax.div(lane16, CAP), QUARTERS) == u)
            gather = jnp.where(source & (lax.rem(lane16, CAP) == lax.rem(row16, CAP)), 1.0, 0.0).astype(BF)
            base[:, h * half + u * 128 : h * half + (u + 1) * 128] = nn(gather, precv[...])
    yown, ybuf = wide[0], wide[1]
    rstack, nstack = wide[8], narrow[8]
    root = level_own[:, :1] < 0.5
    weight = w_ref[:, :1]
    yown[:, :width] = jnp.where(root, weight * base[...], 0.0).astype(BF)
    marks = jnp.where(lane16 < 32, deepest, jnp.where(lane16 < 64, busiest, j_own))
    yown[:, width:] = marks.astype(BF)

    def send_base(steps):
        for d in steps:
            to = lax.rem(s + d, sections)
            remote(ogv, base_out.at[:, rows_at(s, half)], bs_s.at[d], bs_r.at[d], {"section": to}).start()

    def tables():
        base0_out[...] = jnp.where(root, base[...], 0.0).astype(BF)
        chosen = jnp.where(level_l == level_r - 1.0, above, 0.0).astype(BF)
        sel_out[...] = nn(take, chosen).astype(BF)
        j_l = jnp.where(dep_l, jnp.sum(jnp.where(group & dep_r & (row < lane), 1.0, 0.0), axis=0, keepdims=True), -1.0)
        own = (lax.div(lane16, ROWS) == s) & (lax.div(row16, 4) == lax.rem(lax.div(lane16, CAP), QUARTERS))
        own = jnp.where(own & (j_l == lax.rem(row16, 2).astype(F32)), 1.0, 0.0).astype(BF)
        token_n = nn(own, (tok_f + 1.0).astype(BF)) - 1.0
        share_n = jnp.sum(jnp.where(token_n == lane16.astype(F32), jnp.broadcast_to(pair_weight, (ROWS, 128)), 0.0),
                          axis=1, keepdims=True)
        wn_out[...] = jnp.broadcast_to(share_n, (ROWS, 128))
        onto = nn(own, chosen)
        for h in range(2):
            from_wide = (lax.rem(lax.div(row16, 2), 2) == h) & (level_l < 0.5)
            selw[h * ROWS : (h + 1) * ROWS, :] = jnp.where(from_wide, onto, 0.0).astype(BF)
        shrink = (layer_r == layer_l) & (part_r == lax.div(lax.rem(lane, ROWS), 4)) & (j_r == lax.rem(lane, 2).astype(F32))
        shrink = jnp.where(shrink, 1.0, 0.0).astype(BF)
        eighth = lax.div(row16, 2) == lax.div(lax.rem(lane16, ROWS), 2)
        seln_out[...] = jnp.where(eighth, nn(onto.astype(BF), shrink), 0.0).astype(BF)
        later = jnp.sum(jnp.where(same & (layer_r < layer_l) & (layer_r >= s), 1.0, 0.0), axis=0, keepdims=True)
        lane1 = iota((1, 128), 1)
        tok_l = jnp.max(other, axis=0, keepdims=True)
        ftok = jnp.where((later < 0.5) & (lax.div(lane1, ROWS) >= s), tok_l, -1.0)
        ftok_n = nn(jnp.broadcast_to(jnp.where(dep_l, ftok + 1.0, 0.0), (ROWS, 128)).astype(BF), shrink) - 1.0
        ftok_out[0:8, :] = jnp.broadcast_to(ftok, (8, 128))
        ftok_out[8:16, :] = jnp.broadcast_to(jnp.where(dep_l, -1.0, ftok), (8, 128))
        ftok_out[16:24, :] = ftok_n[:8]

    def activations():
        send_base(Z_ORDER)
        pltpu.make_async_copy(ogv, base_out.at[:, rows_at(s, half)], loc.at[5]).start()
        tables()
        gather_finish(*xg, form_w, xnat)
        pltpu.make_async_copy(xnat, xnat_hbm, loc.at[6]).start()
        load_g.wait()
        load_u.wait()
        gate = project(xnat, wg, width)
        up = project(xnat, wu, width)
        sig = 1.0 / (1.0 + jnp.exp(-gate))
        act = gate * sig
        hid_out[...] = (act * up).astype(BF)
        cu_out[...] = act
        cg_out[...] = up * sig * (1.0 + gate * (1.0 - sig))

    def places():
        all_marks = ybuf[:, width : width + MARK].astype(F32)
        lanes = iota(all_marks.shape, 1)
        depth = jnp.max(jnp.where(lanes < 32, all_marks, 0.0)).astype(jnp.int32)
        most = jnp.max(jnp.where((lanes >= 32) & (lanes < 64), all_marks, 0.0)).astype(jnp.int32)
        narrow_out[0] = jnp.where(most > 2, 0, depth - 1)
        wide_out[0] = jnp.where(most > 2, depth, 0)
        r64, c64 = iota((128, 64), 0), iota((128, 64), 1)
        slot_of = (lax.rem(lax.div(r64, 4), 4) == lax.div(c64, ROWS)) & (lax.rem(r64, 4) == lax.rem(c64, ROWS))
        slot_of = jnp.where(slot_of, 1.0, 0.0).astype(BF)
        fits = (lax.rem(lax.div(row, 4), 4) == lax.div(lane, ROWS)) & (lax.div(row, ROWS) == lax.rem(lax.div(lane, 2), 8))

        def one(t):
            slots = nn(slot_of, ybuf[rows_at(t, 64), width : width + MARK])
            e = jnp.where(fits & (slots[:, MARK - 1 :] == lax.rem(lane, 2).astype(F32)), 1.0, 0.0)
            place[rows_at(t, 128), :] = e.astype(BF)
            place_t[rows_at(t, 64), :] = e.T[:64].astype(BF)

        each(0, TILES, one)
        pltpu.make_async_copy(ynat1, y1_hbm, loc.at[8]).start()

    weights, coefs = (wg, wu, wd), (cu_out, cg_out)
    form_w, form_n = Wide(stack), Narrow(stackn, place, place_t)
    one_round(at, form_w, lambda: base[...], wide, weights, coefs, (dg1_out, du1_out), sems_w,
              during_gather=activations, before_grads=load_d.wait, during_sends=places)

    start = jnp.zeros(u0_out.shape, F32)
    for h in range(2):
        start = start + nn(selw[h * ROWS : (h + 1) * ROWS, :], rstack[:, h * half : (h + 1) * half])
    u0_out[...] = start.astype(BF)
    narrow[0][...] = (wn_out[:, :1] * start).astype(BF)

    def rest_of_wide():
        u_out[...] = (nn(sel_out[...], rstack[...]) + base0_out[...].astype(F32)).astype(BF)
        r_out[...] = rstack[...]

    def add_up():
        for total, first in ((dg_out, dg1_out), (du_out, du1_out), (ynat, ynat1)):
            total[...] = total[...] + first[...]
        pltpu.make_async_copy(ynat, ynat_hbm, loc.at[7]).start()

    one_round(at, form_n, lambda: u0_out[...].astype(F32), narrow, weights, coefs, (dg_out, du_out), sems_n,
              during_gather=rest_of_wide, during_sends=add_up)
    un_out[...] = (nn(seln_out[...], nstack[...]) + u0_out[...].astype(F32)).astype(BF)
    rn_out[...] = nstack[...]

    gather_drain(*xg)

    def drain_z(d):
        to = lax.rem(s + d, sections)
        source = lax.rem(s + sections - d, sections)
        remote(tok_ref, tokall.at[mine_z], id_s.at[d], id_r.at[d], at.partner).wait_send()
        remote(psend.at[rows_at(to, ROWS)], precv.at[mine_z], pc_s.at[d], pc_r.at[d], at.partner).wait_send()
        into = remote(ogv, base_out.at[:, rows_at(source, half)], bs_s.at[d], bs_r.at[d], at.partner)
        into.wait_send()
        into.wait_recv()

    each(1, sections, drain_z)
    round_drain(at, wide, sems_w)
    round_drain(at, narrow, sems_n)
    pltpu.make_async_copy(ogv, base_out.at[:, rows_at(s, half)], loc.at[5]).wait()
    pltpu.make_async_copy(xnat, xnat_hbm, loc.at[6]).wait()
    pltpu.make_async_copy(ynat, ynat_hbm, loc.at[7]).wait()
    pltpu.make_async_copy(ynat1, y1_hbm, loc.at[8]).wait()


def enter_round(at, wg_hbm, wu_hbm, wd_hbm, wg, wu, wd, loc, rstack):
    loads = [pltpu.make_async_copy(a, b, loc.at[i]) for i, (a, b) in enumerate(((wd_hbm, wd), (wg_hbm, wg), (wu_hbm, wu)))]
    for load in loads:
        load.start()
    rstack[...] = jnp.zeros_like(rstack)

    def greet(k):
        signal_to(at.peer(at.ahead(k)))

    each_other(greet)
    signal_to(at.partner)

    def greet_z(d):
        @pl.when(at.s + d < at.sections)
        def _():
            signal_to({"section": at.s + d})

    each(1, at.sections, greet_z)

    def loaded():
        for load in loads:
            load.wait()

    return loaded


def next_wide(u_ref, w_ref, base0_ref, sel_ref, cu_ref, cg_ref, wg_hbm, wu_hbm, wd_hbm,
              u_out, dg_out, du_out, r_out, ynat_hbm, wg, wu, wd, ynat, stack, *rest):
    at = Place()
    bufs, loc, sems = rest[:2] + (ynat,) + rest[2:8], rest[8], rest[9:]
    width = u_out.shape[1]
    yown, rstack = bufs[0], bufs[8]
    loaded = enter_round(at, wg_hbm, wu_hbm, wd_hbm, wg, wu, wd, loc, rstack)
    yown[:, :width] = (w_ref[:, :1] * u_ref[...].astype(F32)).astype(BF)
    yown[:, width:] = jnp.zeros((ROWS, MARK), BF)
    pl.semaphore_wait(pltpu.get_barrier_semaphore(), CHIPS + at.s)

    def put():
        pltpu.make_async_copy(ynat, ynat_hbm, loc.at[3]).start()

    one_round(at, Wide(stack), lambda: u_ref[...].astype(F32), bufs, (wg, wu, wd), (cu_ref, cg_ref), (dg_out, du_out), sems,
              before_grads=loaded, during_sends=put)
    u_out[...] = (nn(sel_ref[...], rstack[...]) + base0_ref[...].astype(F32)).astype(BF)
    r_out[...] = rstack[...]
    round_drain(at, bufs, sems)
    pltpu.make_async_copy(ynat, ynat_hbm, loc.at[3]).wait()


def next_narrow(u_hbm, w_ref, u0_ref, sel_ref, place, place_t, cu_ref, cg_ref, dg1_ref, du1_ref, y1_hbm, wg_hbm, wu_hbm, wd_hbm,
                u_hbm_out, dg_out, du_out, r_out, ynat_hbm, wg, wu, wd, y1, ynat, u_ref, stack, *rest):
    at = Place()
    bufs, loc, sems = rest[:2] + (ynat,) + rest[2:8], rest[8], rest[9:]
    yown, rstack = bufs[0], bufs[8]
    load_u = pltpu.make_async_copy(u_hbm, u_ref, loc.at[3])
    load_u.start()
    loaded = enter_round(at, wg_hbm, wu_hbm, wd_hbm, wg, wu, wd, loc, rstack)
    pltpu.make_async_copy(y1_hbm, y1, loc.at[4]).start()
    load_u.wait()
    yown[...] = (w_ref[:, :1] * u_ref[...].astype(F32)).astype(BF)
    pl.semaphore_wait(pltpu.get_barrier_semaphore(), CHIPS + at.s)

    def add_up():
        pltpu.make_async_copy(y1_hbm, y1, loc.at[4]).wait()
        for total, first in ((dg_out, dg1_ref), (du_out, du1_ref), (ynat, y1)):
            total[...] = total[...] + first[...]
        pltpu.make_async_copy(ynat, ynat_hbm, loc.at[5]).start()

    one_round(at, Narrow(stack, place, place_t), lambda: u_ref[...].astype(F32), bufs, (wg, wu, wd), (cu_ref, cg_ref),
              (dg_out, du_out), sems, before_grads=loaded, during_sends=add_up)
    u_ref[...] = (nn(sel_ref[...], rstack[...]) + u0_ref[...].astype(F32)).astype(BF)
    store_u = pltpu.make_async_copy(u_ref, u_hbm_out, loc.at[3])
    store_u.start()
    r_out[...] = rstack[...]
    round_drain(at, bufs, sems)
    store_u.wait()
    pltpu.make_async_copy(ynat, ynat_hbm, loc.at[5]).wait()


def last_kernel(dg, du, hid, x, y, rows, rows_n, ftok, wide_rounds, base, grad_in, grad_gate, grad_up, grad_down, dt):
    q = pl.program_id(0)

    @pl.when(q == 0)
    def _():
        slots = dg.shape[0]
        unit = jnp.where(iota((slots, slots), 0) == iota((slots, slots), 1), 1.0, 0.0).astype(BF)
        for i, part in enumerate((dg, du, hid)):
            dt[i] = lax.dot_general(part[...], unit, (((0,), (0,)), ((), ())), preferred_element_type=F32).astype(BF)

    grad_gate[0] = nn(dt[0], x[...]).astype(BF)
    grad_up[0] = nn(dt[1], x[...]).astype(BF)
    grad_down[0] = nn(dt[2], y[...]).astype(BF)
    tokens, width = grad_in.shape[1:]
    lane = iota((tokens, 128), 1)
    token = iota((tokens, 128), 0).astype(F32)
    wide_only = wide_rounds[0] > 0
    ftok_w = jnp.where(wide_only, ftok[0:1, :], ftok[8:9, :])
    ftok_n = jnp.where(wide_only, -1.0, ftok[16:17, :])
    select = jnp.where((ftok_w == token) & (lax.rem(lax.div(lane, CAP), QUARTERS) == q), 1.0, 0.0)
    new = nn(select.astype(BF), rows[...])
    halves = []
    for h in range(2):
        select_n = jnp.where((ftok_n == token) & (lax.rem(lax.div(lane, 2), 8) == 2 * q + h), 1.0, 0.0)
        halves.append(nn(select_n.astype(BF), rows_n[...]))
    new = new + jnp.concatenate(halves, axis=1)
    live = jnp.sum(select + select_n, axis=1, keepdims=True) > 0.5
    grad_in[0] = jnp.where(live, new, base[...].astype(F32)).astype(BF)


def round_scratch(width, mark):
    blocks = 2 * CHIPS * ROWS
    shapes = [(ROWS, width + mark), (blocks, width + mark)] + [(blocks // 2, width)] * 4 + [(ROWS, width), (8 * ROWS, width)]
    return [pltpu.VMEM(dims, BF) for dims in shapes]


def round_sems():
    sem = pltpu.SemaphoreType.DMA
    return [sem((CHIPS,))] * 4 + [sem((NX,))] * 2 + [sem((CHIPS,))] * 2 + [sem((8,))] * 2


def on_device(saved_inputs, expert_ids, gate_weights, out_grad, gate_w, up_w, down_w):
    tokens, wg, wu, wd = saved_inputs[0], gate_w[0], up_w[0], down_w[0]
    count, d = tokens.shape
    units = wg.shape[0]
    width = d // QUARTERS
    half = width // 2
    slots = lax.axis_size("ep") * CAP
    ids, gates = expert_ids[0].T, gate_weights[0].T

    hbm = pl.BlockSpec(memory_space=pltpu.HBM)
    vmem = pl.BlockSpec(memory_space=pltpu.VMEM)
    smem = pl.BlockSpec(memory_space=pltpu.SMEM)
    sem = pltpu.SemaphoreType.DMA

    def vm(*dims, dtype=BF):
        return pltpu.VMEM(dims, dtype)

    def shape(*dims, dtype=BF):
        return jax.ShapeDtypeStruct(dims, dtype)

    def params(which):
        return pltpu.CompilerParams(collective_id=which, has_side_effects=True, vmem_limit_bytes=60 * 2**20)

    block, block_n, part = (ROWS, width), (ROWS, half), (slots, units)
    (weight, u, base0, select_up, cu, cg, hid, dg1, du1, dg, du, rows, weight_n, un, u0, select_n, place, place_t, rows_n, ftok,
     narrow_rounds, wide_rounds, x, y1, y, base) = pl.pallas_call(
        first_kernel,
        name="first_rounds",
        out_shape=[shape(ROWS, 128, dtype=F32), shape(*block), shape(*block), shape(ROWS, 128), shape(*part, dtype=F32),
                   shape(*part, dtype=F32), shape(*part), shape(*part), shape(*part), shape(*part), shape(*part),
                   shape(128, width), shape(ROWS, 128, dtype=F32), shape(*block_n), shape(*block_n), shape(ROWS, 128),
                   shape(TILES * 128, 128), shape(TILES * 64, 128), shape(128, half), shape(24, 128, dtype=F32),
                   shape(1, dtype=jnp.int32), shape(1, dtype=jnp.int32), shape(slots, d), shape(slots, d), shape(slots, d), shape(count, d)],
        in_specs=[vmem] * 2 + [hbm] * 5,
        out_specs=[vmem] * 20 + [smem] * 2 + [hbm] * 4,
        scratch_shapes=[
            vm(ROWS, 128), vm(count, d), vm(*out_grad.shape), vm(units, d), vm(units, d), vm(units, d),
            vm(*block), vm(2 * CHIPS * ROWS, width), vm(slots, d), vm(128, 128),
            vm(128, 128), vm(128, 128), vm(*block, dtype=F32), vm(slots, d), vm(slots, d), vm(TILES * 64, width), vm(TILES * 128, half),
            vm(2 * ROWS, 128),
        ] + round_scratch(width, MARK) + round_scratch(half, 0) + [
            sem((9,)), sem((CHIPS,)), sem((CHIPS,)), sem((CHIPS,)), sem((CHIPS,)),
            sem((8,)), sem((8,)), sem((8,)), sem((8,)), sem((8,)), sem((8,)),
        ] + round_sems() + round_sems(),
        compiler_params=params(0),
    )(ids, gates, tokens, out_grad, wg, wu, wd)

    three = [vm(units, d)] * 3

    def more_narrow(_, state):
        un = state[0]
        return tuple(pl.pallas_call(
            next_narrow,
            name="next_narrow",
            out_shape=[shape(*block_n), shape(*part), shape(*part), shape(128, half), shape(slots, d)],
            in_specs=[hbm] + [vmem] * 9 + [hbm] * 4,
            out_specs=[hbm] + [vmem] * 3 + [hbm],
            input_output_aliases={0: 0},
            scratch_shapes=three + [vm(slots, d), vm(slots, d), vm(*block_n), vm(TILES * 128, half)] + round_scratch(half, 0) + [sem((6,))]
            + round_sems(),
            compiler_params=params(1),
        )(un, weight_n, u0, select_n, place, place_t, cu, cg, dg1, du1, y1, wg, wu, wd))

    def more_wide(_, state):
        u = state[0]
        return tuple(pl.pallas_call(
            next_wide,
            name="next_wide",
            out_shape=[shape(*block), shape(*part), shape(*part), shape(128, width), shape(slots, d)],
            in_specs=[vmem] * 6 + [hbm] * 3,
            out_specs=[vmem] * 4 + [hbm],
            scratch_shapes=three + [vm(slots, d), vm(TILES * 64, width)] + round_scratch(width, MARK) + [sem((4,))] + round_sems(),
            compiler_params=params(2),
        )(u, weight, base0, select_up, cu, cg, wg, wu, wd))

    un, dg, du, rows_n, y = lax.fori_loop(0, narrow_rounds[0], more_narrow, (un, dg, du, rows_n, y))
    u, dg, du, rows, y = lax.fori_loop(0, wide_rounds[0], more_wide, (u, dg, du, rows, y))

    full = pl.BlockSpec(part, lambda i: (0, 0))
    cols = pl.BlockSpec((slots, width), lambda i: (0, i))
    grad = pl.BlockSpec((1, units, width), lambda i: (0, 0, i))
    return pl.pallas_call(
        last_kernel,
        name="gradients",
        grid=(QUARTERS,),
        out_shape=[shape(1, count, d), shape(1, units, d), shape(1, units, d), shape(1, units, d)],
        in_specs=[full, full, full, cols, cols, pl.BlockSpec((128, width), lambda i: (0, 0)),
                  pl.BlockSpec((128, half), lambda i: (0, 0)), pl.BlockSpec((24, 128), lambda i: (0, 0)), smem, cols],
        out_specs=[pl.BlockSpec((1, count, width), lambda i: (0, 0, i)), grad, grad, grad],
        scratch_shapes=[vm(3, units, slots)],
        compiler_params=pltpu.CompilerParams(vmem_limit_bytes=32 * 2**20),
    )(dg, du, hid, x, y, rows, rows_n, ftok, wide_rounds, base)


def solution(mesh):
    split = P("section", "ep", None)
    return jax.shard_map(
        on_device,
        mesh=mesh,
        in_specs=(split, split, split, P("ep", "section"), split, split, split),
        out_specs=(split, split, split, split),
        check_vma=False,
    )
```

```python
import functools

import jax
import jax.numpy as jnp
from jax import lax
from jax.experimental import pallas as pl
from jax.experimental.pallas import tpu as pltpu
from jax.sharding import PartitionSpec as P

MESH = pl.DeviceIdType.MESH
CAP = 4
NX, NY = 4, 4
CHIPS = NX * NY
SELF = (NX // 2) * NY + NY // 2
Z_ORDER = (4, 3, 5, 2, 6, 1, 7)
QUARTERS = 4
TILES = 2 * CHIPS * CAP // 16
ROWS = QUARTERS * CAP
MARK = 128
HALVES = 2
BF, F32 = jnp.bfloat16, jnp.float32


def iota(shape, dim):
    return lax.broadcasted_iota(jnp.int32, shape, dim)


def rows_at(index, size):
    start = index * size
    return pl.ds(start if isinstance(start, int) else pl.multiple_of(start, size), size)


def swap_matrix():
    i, m = iota((64, 64), 0), iota((64, 64), 1)
    swapped = (lax.rem(lax.div(m, 4), 4) * 16) + (lax.div(m, 16) * 4) + lax.rem(m, 4)
    return jnp.where(i == swapped, 1.0, 0.0).astype(BF)


def nt(a, b):
    return lax.dot_general(a, b, (((1,), (1,)), ((), ())), preferred_element_type=F32)


def nn(a, b):
    return lax.dot_general(a, b, (((1,), (0,)), ((), ())), preferred_element_type=F32)


class Place:
    def __init__(self):
        self.s = lax.axis_index("section")
        self.sections = lax.axis_size("section")
        ep = lax.axis_index("ep")
        self.core = lax.rem(ep, 2)
        self.chip = lax.div(ep, 2)
        self.x = lax.div(self.chip, NY)
        self.y = lax.rem(self.chip, NY)
        self.partner = {"ep": self.chip * 2 + 1 - self.core}

    def ahead(self, k):
        i, j = k // NY + NX // 2, k % NY + NY // 2
        return lax.rem(self.x + i, NX) * NY + lax.rem(self.y + j, NY)

    def behind(self, k):
        i, j = k // NY + NX // 2, k % NY + NY // 2
        return lax.rem(self.x + 2 * NX - i, NX) * NY + lax.rem(self.y + 2 * NY - j, NY)

    def peer(self, chip):
        return {"ep": chip * 2 + self.core}

    def block(self, core, chip):
        return rows_at(core * CHIPS + chip, ROWS)


def remote(src, dst, send, recv, device):
    return pltpu.make_async_remote_copy(
        src_ref=src, dst_ref=dst, send_sem=send, recv_sem=recv, device_id=device, device_id_type=MESH
    )


def each(lo, hi, body):
    lax.fori_loop(lo, hi, lambda k, carry: (body(k), carry)[1], 0)


def each_other(body):
    each(0, SELF, body)
    each(SELF + 1, CHIPS, body)


OTHERS = tuple(k for k in range(CHIPS) if k != SELF)


def unrolled(body):
    for k in OTHERS:
        body(k)


class Gather:
    def __init__(self, at, own, buf, sems):
        self.at, self.own, self.buf = at, own, buf
        self.send, self.recv, self.relay_send, self.relay_recv = sems

    def direct(self, k, block, device):
        return remote(self.own, self.buf.at[block], self.send.at[0], self.recv.at[k // NY], device)

    def relay(self, rows):
        here = self.buf.at[rows]
        return remote(here, here, self.relay_send.at[0], self.relay_recv.at[0], self.at.partner)

    def start(self):
        at = self.at
        mine = at.block(at.core, at.chip)
        self.buf[mine, :] = self.own[...]
        unrolled(lambda k: self.direct(k, mine, at.peer(at.ahead(k))).start())

    def forward(self):
        at = self.at
        for i in range(NX):
            count = (NY - 1 if i == SELF // NY else NY) * ROWS
            some = self.buf.at[pl.ds(0, count)]
            remote(some, some, self.send.at[0], self.recv.at[i], at.partner).wait_recv()
            x = lax.rem(at.x + 2 * NX - (i + NX // 2), NX)
            self.relay(rows_at(at.core * NX + x, NY * ROWS)).start()

    def take(self, expand):
        at = self.at
        each(0, NX, lambda t: expand(at.core * NX + t))
        self.relay(pl.ds(0, CHIPS * ROWS)).wait_recv()
        each(0, NX, lambda t: expand((1 - at.core) * NX + t))

    def drain(self):
        some = self.buf.at[pl.ds(0, (CHIPS - 1) * ROWS)]
        remote(some, some, self.send.at[0], self.recv.at[0], self.at.partner).wait_send()
        self.relay(pl.ds(0, CHIPS * ROWS)).wait_send()


def lay_out(tile, nat, t, first, width):
    rows = tile.shape[0] // ROWS
    for q in range(rows):
        nat[rows_at(t, ROWS), first + q * width : first + (q + 1) * width] = tile[q * ROWS : (q + 1) * ROWS]


class Wide:
    def __init__(self, stack):
        self.stack, self.width = stack, stack.shape[1]

    def expand(self, buf, nat, h, t):
        tile = nn(swap_matrix(), buf[rows_at(t, 64), : self.width]).astype(BF)
        lay_out(tile, nat, t, h * QUARTERS * self.width, self.width)

    def fill(self, h, c, value):
        for t in range(TILES):
            for sub in range(2):
                self.stack[rows_at((h * TILES + t) * QUARTERS + c * 2 + sub, ROWS), :] = value[
                    t * ROWS : (t + 1) * ROWS, sub * self.width : (sub + 1) * self.width
                ]

    def pack(self, h, t):
        return nn(swap_matrix(), self.stack[rows_at(h * TILES + t, 64), :])


class Narrow:
    def __init__(self, stack, place, place_t):
        self.stack, self.width = stack, stack.shape[1]
        self.place, self.place_t = place, place_t

    def expand(self, buf, nat, h, t):
        tile = nn(self.place[rows_at(t, 128), :64], buf[rows_at(t, 64), :]).astype(BF)
        lay_out(tile, nat, t, h * 2 * QUARTERS * self.width, self.width)

    def fill(self, h, c, value):
        for t in range(TILES):
            for sub in range(4):
                self.stack[rows_at((h * TILES + t) * 2 * QUARTERS + c * 4 + sub, ROWS), :] = value[
                    t * ROWS : (t + 1) * ROWS, sub * self.width : (sub + 1) * self.width
                ]

    def pack(self, h, t):
        return nn(self.place_t[rows_at(t, 64), :], self.stack[rows_at(h * TILES + t, 128), :])


def project(nat, weight, width, lo=0, hi=QUARTERS):
    def step(q, acc):
        cols = rows_at(q, width)
        return acc + nt(nat[:, cols], weight[:, cols])

    return lax.fori_loop(lo, hi, step, jnp.zeros((nat.shape[0], weight.shape[0]), F32))


class Round:
    def __init__(self, at, form, bufs, sems, mark):
        self.at, self.form = at, form
        self.yown, self.ybuf, self.pbuf, self.drecv, self.sbuf, self.rbuf, self.rown, self.rstack = bufs
        self.dd_s, self.dd_r, self.rs_s, self.rs_r, self.z_s, self.z_r = sems[4:]
        self.gathers = []
        for h in range(HALVES):
            lanes = pl.ds(0, form.width + (mark if h == 0 else 0))
            self.gathers.append(Gather(at, self.yown.at[h, :, lanes], self.ybuf.at[h, :, lanes], [x.at[h] for x in sems[:4]]))

    def swap_copy(self, h, jj, j):
        part = rows_at(j, 64)
        return remote(self.pbuf.at[h, part], self.drecv.at[h, part], self.dd_s.at[h, jj], self.dd_r.at[h, jj], self.at.partner)

    def all_homes(self, h):
        rows = pl.ds(0, (CHIPS - 1) * ROWS)
        return remote(self.sbuf.at[h, rows], self.rbuf.at[h, rows], self.rs_s.at[h], self.rs_r.at[h], self.at.partner)

    def some_down(self, h, count):
        here = self.rstack.at[h, pl.ds(0, count * ROWS)]
        return remote(here, here, self.z_s.at[h], self.z_r.at[h], {"section": lax.rem(self.at.s + 1, self.at.sections)})

    def home_copy(self, h, k, chip, device):
        return remote(self.sbuf.at[h, rows_at(chip, ROWS)], self.rbuf.at[h, rows_at(k, ROWS)], self.rs_s.at[h],
                      self.rs_r.at[h], device)

    def down_copy(self, h, d, source, device):
        return remote(self.rown.at[h], self.rstack.at[h, rows_at(source, ROWS)], self.z_s.at[h], self.z_r.at[h], device)

    def run(self, upstream, nat, weights, coefs, grads, during_gather=None, before_grads=None, during_sends=None, on_rows=None):
        at, form = self.at, self.form
        wg, wu, wd = weights
        dg, du = grads
        width = wg.shape[1] // QUARTERS
        if during_gather is not None:
            during_gather()
        for gather in self.gathers:
            gather.forward()
        if before_grads is not None:
            before_grads()
        grad_hidden = None
        for h, gather in enumerate(self.gathers):
            gather.take(functools.partial(form.expand, self.ybuf.at[h], nat, h))
            some = project(nat, wd, width, 2 * h, 2 * h + 2)
            grad_hidden = some if h == 0 else grad_hidden + some
        du[...] = (grad_hidden * coefs[0][...]).astype(BF)
        dg[...] = (grad_hidden * coefs[1][...]).astype(BF)

        for h in range(HALVES):

            def back(c):
                cols = rows_at(2 * h + c, width)
                form.fill(h, c, (nn(dg[...], wg[:, cols]) + nn(du[...], wu[:, cols])).astype(BF))

            each(0, 2, back)

            def to_partner(jj):
                j = lax.rem(at.x + jj + NX // 2, NX)
                self.pbuf[h, rows_at(j, 64), :] = form.pack(h, (1 - at.core) * NX + j).astype(BF)
                self.swap_copy(h, jj, j).start()

            for jj in range(NX):
                to_partner(jj)

        for h in range(HALVES):

            def to_homes(jj):
                j = lax.rem(at.x + jj + NX // 2, NX)
                part = rows_at(j, 64)
                mine = form.pack(h, at.core * NX + j)
                self.swap_copy(h, jj, j).wait_recv()
                self.sbuf[h, part, :] = (mine + self.drecv[h, part, :].astype(F32)).astype(BF)

                for m in range(NY):
                    k = jj * NY + m
                    if k != SELF:
                        chip = at.ahead(k)
                        self.home_copy(h, k, chip, at.peer(chip)).start()

            for jj in range(NX):
                to_homes(jj)
        if during_sends is not None:
            during_sends()

        for h in range(HALVES):

            self.all_homes(h).wait_recv()
            total = self.sbuf[h, rows_at(at.chip, ROWS), :].astype(F32)
            for k in OTHERS:
                total = total + self.rbuf[h, rows_at(k, ROWS), :].astype(F32)
            row = (upstream(h) + total).astype(BF)
            self.rown[h] = row
            self.rstack[h, rows_at(at.s, ROWS), :] = row
            for d in Z_ORDER:

                @pl.when(at.s >= d)
                def _():
                    self.down_copy(h, d, at.s, {"section": at.s - d}).start()

        for h in range(HALVES):
            for count in Z_ORDER:

                @pl.when(at.s + count == at.sections - 1)
                def _():
                    self.some_down(h, count).wait_recv()

            if on_rows is not None:
                on_rows(h)

    def drain(self):
        at = self.at
        for h in range(HALVES):
            self.gathers[h].drain()
            each(0, NX, lambda jj: self.swap_copy(h, jj, jj).wait_send())
            self.all_homes(h).wait_send()
            for count in Z_ORDER:

                @pl.when(at.s == count)
                def _():
                    self.some_down(h, count).wait_send()


class Copies:
    def __init__(self, sems):
        self.sems, self.used, self.pending = sems, 0, []

    def start(self, *pairs):
        made = []
        for source, target in pairs:
            made.append(pltpu.make_async_copy(source, target, self.sems.at[self.used]))
            made[-1].start()
            self.used += 1
        self.pending += made
        return made

    def wait(self, made):
        for copy in made:
            copy.wait()
            self.pending.remove(copy)

    def finish(self):
        self.wait(list(self.pending))


def signal_to(device):
    pl.semaphore_signal(pltpu.get_barrier_semaphore(), inc=1, device_id=device, device_id_type=MESH)


def first_kernel(ids_hbm, gates_hbm, tokens_hbm, og_hbm, wg_hbm, wu_hbm, wd_hbm, *refs):
    outs, (narrow_out, wide_out), refs = refs[:24], refs[24:26], refs[26:]
    (w_hbm, u_hbm, base0_hbm, sel_hbm, cu_hbm, cg_hbm, hid_hbm, dg1_hbm, du1_hbm, dg_hbm, du_hbm, r_hbm, wn_hbm, un_hbm, u0_hbm,
     seln_hbm, place_hbm, place_t_hbm, rn_hbm, ftok_hbm, xnat_hbm, y1_hbm, ynat_hbm, base_out) = outs
    (w_ref, u_out, base0_out, sel_out, cu_out, cg_out, hid_out, dg1_out, du1_out, dg_out, du_out, wn_out, un_out, u0_out,
     seln_out, place, place_t, ftok_out) = refs[:18]
    (ids_ref, gates_ref, tok_ref, tokv, ogv, wg, wu, wd, xown, xbuf, xnat, tokall, psend, precv, base, ynat1, ynat, stack, stackn,
     selw) = refs[18:38]
    wide_bufs, narrow_bufs, refs = refs[38:46], refs[46:54], refs[54:]
    loc, x_s, x_r, xrel_s, xrel_r, id_s, id_r, pc_s, pc_r, bs_s, bs_r = refs[:11]
    at = Place()
    s, sections = at.s, at.sections
    half = ogv.shape[1]
    width = 2 * half
    wide = Round(at, Wide(stack), wide_bufs, refs[11:21], MARK)
    narrow = Round(at, Narrow(stackn, place, place_t), narrow_bufs, refs[21:31], 0)
    x_gather = Gather(at, xown, xbuf, (x_s, x_r, xrel_s, xrel_r))
    local = Copies(loc)
    load_ids = local.start((ids_hbm, ids_ref), (gates_hbm, gates_ref))
    load_tokens = local.start((tokens_hbm, tokv))
    load_og = local.start((og_hbm, ogv))
    load_gu = local.start((wg_hbm, wg), (wu_hbm, wu))
    load_d = local.start((wd_hbm, wd))

    for received in (wide.rstack, narrow.rstack):
        received[...] = jnp.zeros_like(received)

    def greet(k):
        signal_to(at.peer(at.ahead(k)))

    each_other(greet)
    signal_to(at.partner)

    def greet_z(d):
        signal_to({"section": lax.rem(s + d, sections)})

    each(1, sections, greet_z)

    local.wait(load_ids)
    hits = ids_ref[...] == 0
    live = jnp.sum(jnp.where(hits, 1.0, 0.0), axis=0, keepdims=True)
    pair_weight = jnp.sum(jnp.where(hits, gates_ref[...], 0.0), axis=0, keepdims=True)
    before = jnp.where(iota((128, 128), 0) < iota((128, 128), 1), 1.0, 0.0).astype(BF)
    live16 = jnp.broadcast_to(live, (ROWS, 128))
    slot = nn(live16.astype(BF), before)
    lane16, row16 = iota((ROWS, 128), 1), iota((ROWS, 128), 0)
    mine16 = (live16 > 0.5) & (slot == lax.rem(row16, CAP).astype(F32))
    token = jnp.max(jnp.where(mine16, lane16.astype(F32), -1.0), axis=1, keepdims=True)
    tok_ref[...] = jnp.broadcast_to(token, (ROWS, 128)).astype(BF)
    share = jnp.sum(jnp.where(mine16, jnp.broadcast_to(pair_weight, (ROWS, 128)), 0.0), axis=1, keepdims=True)
    w_ref[...] = jnp.broadcast_to(share, (ROWS, 128))

    mine_z = rows_at(s, ROWS)
    pl.semaphore_wait(pltpu.get_barrier_semaphore(), CHIPS + sections - 1)

    def send_ids(d):
        remote(tok_ref, tokall.at[mine_z], id_s.at[0], id_r.at[0], {"section": lax.rem(s + d, sections)}).start()

    for d in Z_ORDER:
        send_ids(d)
    tokall[mine_z, :] = tok_ref[...]

    local.wait(load_tokens)
    hit = token == lane16.astype(F32)
    block = jnp.zeros((ROWS, width), F32)
    for q in range(QUARTERS):
        select = jnp.where(hit & (lax.div(row16, CAP) == q), 1.0, 0.0).astype(BF)
        block = block + nn(select, tokv[:, q * width : (q + 1) * width])
    xown[...] = block.astype(BF)
    x_gather.start()

    local.wait(load_og)

    others = (sections - 1) * ROWS

    def all_ids():
        some = tokall.at[pl.ds(0, others)]
        return remote(some, some, id_s.at[0], id_r.at[0], at.partner)

    def all_pieces():
        some = precv.at[pl.ds(0, others)]
        return remote(some, some, pc_s.at[0], pc_r.at[0], at.partner)

    def all_base():
        some = base_out.at[:, pl.ds(0, (sections - 1) * half)]
        return remote(some, some, bs_s.at[0], bs_r.at[0], at.partner)

    all_ids().wait_recv()
    tok_f = tokall[...].astype(F32)
    row, lane = iota((128, 128), 0), iota((128, 128), 1)
    for_slot = tok_f == lane.astype(F32)
    pieces = jnp.zeros((128, 128), F32)
    for u in range(half // 128):
        pick = jnp.where(for_slot & (lax.rem(lax.div(row, CAP), QUARTERS) == u), 1.0, 0.0).astype(BF)
        pieces = pieces + nn(pick, ogv[:, u * 128 : (u + 1) * 128])
    psend[...] = pieces.astype(BF)

    def send_piece(d):
        to = lax.rem(s + d, sections)
        remote(psend.at[rows_at(to, ROWS)], precv.at[mine_z], pc_s.at[0], pc_r.at[0], {"section": to}).start()

    for d in Z_ORDER:
        send_piece(d)
    precv[mine_z, :] = psend[mine_z, :]

    other = tok_f.T
    layer_r, layer_l = lax.div(row, ROWS), lax.div(lane, ROWS)
    part_r, part_l = lax.rem(lax.div(row, CAP), QUARTERS), lax.rem(lax.div(lane, CAP), QUARTERS)
    same = (tok_f == other) & (tok_f >= 0.0) & (part_r == part_l)
    above = jnp.where(same & (layer_l > layer_r), 1.0, 0.0)
    level_r = jnp.sum(above, axis=1, keepdims=True)
    level_l = jnp.sum(jnp.where(same & (layer_r > layer_l), 1.0, 0.0), axis=0, keepdims=True)
    dep_r, dep_l = level_r > 0.5, level_l > 0.5
    group = lax.div(row, CAP) == lax.div(lane, CAP)
    fellows = jnp.where(group & dep_l, 1.0, 0.0)
    busiest = jnp.max(jnp.sum(fellows, axis=1, keepdims=True), axis=0, keepdims=True)
    deepest = jnp.max(level_r, axis=0, keepdims=True)
    j_r = jnp.where(dep_r, jnp.sum(jnp.where(lane < row, fellows, 0.0), axis=1, keepdims=True), -1.0)
    take = jnp.where(lane16 == row16 + s * ROWS, 1.0, 0.0).astype(BF)
    level_own = nn(take, jnp.broadcast_to(level_r, (128, 128)).astype(BF))
    j_own = nn(take, jnp.broadcast_to(j_r, (128, 128)).astype(BF))

    all_pieces().wait_recv()
    root = level_own[:, :1] < 0.5
    weight = w_ref[:, :1]
    marks = jnp.where(lane16 < 32, deepest, jnp.where(lane16 < 64, busiest, j_own))
    wide.yown[0, :, half:] = marks.astype(BF)
    for h in range(HALVES):
        for u in range(half // 128):
            source = (lax.div(lane16, ROWS) == h * QUARTERS + lax.div(row16, CAP)) & (
                lax.rem(lax.div(lane16, CAP), QUARTERS) == u)
            pick = jnp.where(source & (lax.rem(lane16, CAP) == lax.rem(row16, CAP)), 1.0, 0.0).astype(BF)
            base[h, :, u * 128 : (u + 1) * 128] = nn(pick, precv[...])
        wide.yown[h, :, :half] = jnp.where(root, weight * base[h], 0.0).astype(BF)
        wide.gathers[h].start()

    def send_base(steps):
        for d in steps:
            to = lax.rem(s + d, sections)
            remote(ogv, base_out.at[:, rows_at(s, half)], bs_s.at[0], bs_r.at[0], {"section": to}).start()

    def tables():
        for h in range(HALVES):
            base0_out[h] = jnp.where(root, base[h], 0.0).astype(BF)
        chosen = jnp.where(level_l == level_r - 1.0, above, 0.0).astype(BF)
        sel_out[...] = nn(take, chosen).astype(BF)
        j_l = jnp.where(dep_l, jnp.sum(jnp.where(group & dep_r & (row < lane), 1.0, 0.0), axis=0, keepdims=True), -1.0)
        own = (lax.div(lane16, ROWS) == s) & (lax.div(row16, 4) == lax.rem(lax.div(lane16, CAP), QUARTERS))
        own = jnp.where(own & (j_l == lax.rem(row16, 2).astype(F32)), 1.0, 0.0).astype(BF)
        token_n = nn(own, (tok_f + 1.0).astype(BF)) - 1.0
        share_n = jnp.sum(jnp.where(token_n == lane16.astype(F32), jnp.broadcast_to(pair_weight, (ROWS, 128)), 0.0),
                          axis=1, keepdims=True)
        wn_out[...] = jnp.broadcast_to(share_n, (ROWS, 128))
        onto = nn(own, chosen)
        for h in range(2):
            from_wide = (lax.rem(lax.div(row16, 2), 2) == h) & (level_l < 0.5)
            selw[h * ROWS : (h + 1) * ROWS, :] = jnp.where(from_wide, onto, 0.0).astype(BF)
        shrink = (layer_r == layer_l) & (part_r == lax.div(lax.rem(lane, ROWS), 4)) & (j_r == lax.rem(lane, 2).astype(F32))
        shrink = jnp.where(shrink, 1.0, 0.0).astype(BF)
        eighth = lax.div(row16, 2) == lax.div(lax.rem(lane16, ROWS), 2)
        seln_out[...] = jnp.where(eighth, nn(onto.astype(BF), shrink), 0.0).astype(BF)
        later = jnp.sum(jnp.where(same & (layer_r < layer_l) & (layer_r >= s), 1.0, 0.0), axis=0, keepdims=True)
        lane1 = iota((1, 128), 1)
        tok_l = jnp.max(other, axis=0, keepdims=True)
        ftok = jnp.where((later < 0.5) & (lax.div(lane1, ROWS) >= s), tok_l, -1.0)
        ftok_n = nn(jnp.broadcast_to(jnp.where(dep_l, ftok + 1.0, 0.0), (ROWS, 128)).astype(BF), shrink) - 1.0
        ftok_out[0:8, :] = jnp.broadcast_to(ftok, (8, 128))
        ftok_out[8:16, :] = jnp.broadcast_to(jnp.where(dep_l, -1.0, ftok), (8, 128))
        ftok_out[16:24, :] = ftok_n[:8]

    def expand_x(t):
        lay_out(nn(swap_matrix(), xbuf[rows_at(t, 64), :]).astype(BF), xnat, t, 0, width)

    def activations():
        send_base(Z_ORDER)
        local.start((ogv, base_out.at[:, rows_at(s, half)]))
        tables()
        local.start((w_ref, w_hbm), (base0_out, base0_hbm), (sel_out, sel_hbm), (wn_out, wn_hbm), (seln_out, seln_hbm),
                    (ftok_out, ftok_hbm))
        x_gather.forward()
        x_gather.take(expand_x)
        local.start((xnat, xnat_hbm))
        local.wait(load_gu)
        gate = project(xnat, wg, width)
        up = project(xnat, wu, width)
        sig = 1.0 / (1.0 + jnp.exp(-gate))
        act = gate * sig
        hid_out[...] = (act * up).astype(BF)
        cu_out[...] = act
        cg_out[...] = up * sig * (1.0 + gate * (1.0 - sig))
        local.start((hid_out, hid_hbm), (cu_out, cu_hbm), (cg_out, cg_hbm))

    def places():
        all_marks = wide.ybuf[0, :, half:].astype(F32)
        lanes = iota(all_marks.shape, 1)
        depth = jnp.max(jnp.where(lanes < 32, all_marks, 0.0)).astype(jnp.int32)
        most = jnp.max(jnp.where((lanes >= 32) & (lanes < 64), all_marks, 0.0)).astype(jnp.int32)
        narrow_out[0] = jnp.where(most > 2, 0, depth - 1)
        wide_out[0] = jnp.where(most > 2, depth, 0)
        r64, c64 = iota((128, 64), 0), iota((128, 64), 1)
        slot_of = (lax.rem(lax.div(r64, 4), 4) == lax.div(c64, ROWS)) & (lax.rem(r64, 4) == lax.rem(c64, ROWS))
        slot_of = jnp.where(slot_of, 1.0, 0.0).astype(BF)
        fits = (lax.rem(lax.div(row, 4), 4) == lax.div(lane, ROWS)) & (lax.div(row, ROWS) == lax.rem(lax.div(lane, 2), 8))

        def one(t):
            slots = nn(slot_of, wide.ybuf[0, rows_at(t, 64), half:])
            e = jnp.where(fits & (slots[:, MARK - 1 :] == lax.rem(lane, 2).astype(F32)), 1.0, 0.0)
            place[rows_at(t, 128), :] = e.astype(BF)
            place_t[rows_at(t, 64), :] = e.T[:64].astype(BF)

        each(0, TILES, one)
        local.start((ynat1, y1_hbm), (place, place_hbm), (place_t, place_t_hbm), (dg1_out, dg1_hbm), (du1_out, du1_hbm))

    def first_narrow(h):
        start = jnp.zeros((ROWS, half // 2), F32)
        parts = []
        for sub in range(2):
            parts.append(nn(selw[sub * ROWS : (sub + 1) * ROWS, :], wide.rstack[h, :, sub * half // 2 : (sub + 1) * half // 2]))
        start = parts[0] + parts[1]
        u0_out[h] = start.astype(BF)
        narrow.yown[h] = (wn_out[:, :1] * start).astype(BF)
        narrow.gathers[h].start()

    weights, coefs = (wg, wu, wd), (cu_out, cg_out)
    wide.run(lambda h: base[h], ynat1, weights, coefs, (dg1_out, du1_out), during_gather=activations,
             before_grads=lambda: local.wait(load_d), during_sends=places, on_rows=first_narrow)

    def rest_of_wide():
        for h in range(HALVES):
            u_out[h] = (nn(sel_out[...], wide.rstack[h]) + base0_out[h].astype(F32)).astype(BF)
        local.start((u_out, u_hbm), (u0_out, u0_hbm), (wide.rstack, r_hbm))

    def add_up():
        for total, first in ((dg_out, dg1_out), (du_out, du1_out), (ynat, ynat1)):
            total[...] = total[...] + first[...]
        local.start((dg_out, dg_hbm), (du_out, du_hbm), (ynat, ynat_hbm))

    def follow(h):
        un_out[h] = (nn(seln_out[...], narrow.rstack[h]) + u0_out[h].astype(F32)).astype(BF)

    narrow.run(lambda h: u0_out[h].astype(F32), ynat, weights, coefs, (dg_out, du_out),
               during_gather=rest_of_wide, during_sends=add_up, on_rows=follow)
    local.start((un_out, un_hbm), (narrow.rstack, rn_hbm))

    x_gather.drain()

    all_ids().wait_send()
    all_pieces().wait_send()
    all_base().wait_send()
    all_base().wait_recv()
    wide.drain()
    narrow.drain()
    local.finish()


def enter_round(at, rstack):
    rstack[...] = jnp.zeros_like(rstack)
    each_other(lambda k: signal_to(at.peer(at.ahead(k))))
    signal_to(at.partner)

    def greet_z(d):
        @pl.when(at.s + d < at.sections)
        def _():
            signal_to({"section": at.s + d})

    each(1, at.sections, greet_z)


def next_wide(*refs):
    ins, outs, refs = refs[:9], refs[9:14], refs[14:]
    held, (dg, du, ynat, stack), bufs, loc, sems = refs[:9], refs[9:13], refs[13:21], refs[21], refs[22:]
    u_ref, w_ref, base0_ref, sel_ref, cu_ref, cg_ref, wg, wu, wd = held
    u_hbm, dg_hbm, du_hbm, r_hbm, ynat_hbm = outs
    at = Place()
    half = u_ref.shape[2]
    this = Round(at, Wide(stack), bufs, sems, MARK)
    local = Copies(loc)
    first = local.start(*zip(ins[:2], held[:2]))
    others = local.start(*zip(ins[2:], held[2:]))
    enter_round(at, this.rstack)
    local.wait(first)
    this.yown[0, :, half:] = jnp.zeros((ROWS, MARK), BF)
    for h in range(HALVES):
        this.yown[h, :, :half] = (w_ref[:, :1] * u_ref[h].astype(F32)).astype(BF)
    pl.semaphore_wait(pltpu.get_barrier_semaphore(), CHIPS + at.s)
    for gather in this.gathers:
        gather.start()

    def put():
        local.start((dg, dg_hbm), (du, du_hbm), (ynat, ynat_hbm))

    def follow(h):
        u_ref[h] = (nn(sel_ref[...], this.rstack[h]) + base0_ref[h].astype(F32)).astype(BF)

    this.run(lambda h: u_ref[h].astype(F32), ynat, (wg, wu, wd), (cu_ref, cg_ref), (dg, du),
             during_gather=lambda: local.wait(others), during_sends=put, on_rows=follow)
    local.start((u_ref, u_hbm), (this.rstack, r_hbm))
    this.drain()
    local.finish()


def next_narrow(*refs):
    ins, outs, refs = refs[:14], refs[14:19], refs[19:]
    held, (dg, du, ynat, stack), bufs, loc, sems = refs[:14], refs[14:18], refs[18:26], refs[26], refs[27:]
    u_ref, w_ref, u0_ref, sel_ref, place, place_t, cu_ref, cg_ref, dg1, du1, y1, wg, wu, wd = held
    u_hbm, dg_hbm, du_hbm, r_hbm, ynat_hbm = outs
    at = Place()
    this = Round(at, Narrow(stack, place, place_t), bufs, sems, 0)
    local = Copies(loc)
    first = local.start(*zip(ins[:2], held[:2]))
    others = local.start(*zip(ins[2:], held[2:]))
    enter_round(at, this.rstack)
    local.wait(first)
    for h in range(HALVES):
        this.yown[h] = (w_ref[:, :1] * u_ref[h].astype(F32)).astype(BF)
    pl.semaphore_wait(pltpu.get_barrier_semaphore(), CHIPS + at.s)
    for gather in this.gathers:
        gather.start()

    def add_up():
        for total, one in ((dg, dg1), (du, du1), (ynat, y1)):
            total[...] = total[...] + one[...]
        local.start((dg, dg_hbm), (du, du_hbm), (ynat, ynat_hbm))

    def follow(h):
        u_ref[h] = (nn(sel_ref[...], this.rstack[h]) + u0_ref[h].astype(F32)).astype(BF)

    this.run(lambda h: u_ref[h].astype(F32), ynat, (wg, wu, wd), (cu_ref, cg_ref), (dg, du),
             during_gather=lambda: local.wait(others), during_sends=add_up, on_rows=follow)
    local.start((u_ref, u_hbm), (this.rstack, r_hbm))
    this.drain()
    local.finish()


def last_kernel(dg, du, hid, x, y, rows, rows_n, ftok, wide_rounds, base, grad_in, grad_gate, grad_up, grad_down, dt):
    q = pl.program_id(0)

    @pl.when(q == 0)
    def _():
        slots = dg.shape[0]
        unit = jnp.where(iota((slots, slots), 0) == iota((slots, slots), 1), 1.0, 0.0).astype(BF)
        for i, part in enumerate((dg, du, hid)):
            dt[i] = lax.dot_general(part[...], unit, (((0,), (0,)), ((), ())), preferred_element_type=F32).astype(BF)

    grad_gate[0] = nn(dt[0], x[...]).astype(BF)
    grad_up[0] = nn(dt[1], x[...]).astype(BF)
    grad_down[0] = nn(dt[2], y[...]).astype(BF)
    tokens, width = grad_in.shape[1:]
    lane = iota((tokens, 128), 1)
    token = iota((tokens, 128), 0).astype(F32)
    wide_only = wide_rounds[0] > 0
    ftok_w = jnp.where(wide_only, ftok[0:1, :], ftok[8:9, :])
    ftok_n = jnp.where(wide_only, -1.0, ftok[16:17, :])
    part = lax.rem(q, 2)
    news, live = [], jnp.zeros((tokens, 1), F32)
    for sub in range(2):
        mine = lax.rem(lax.div(lane, CAP), QUARTERS) == 2 * part + sub
        select = jnp.where((ftok_w == token) & mine, 1.0, 0.0)
        new = nn(select.astype(BF), rows[0])
        news_n = []
        for half in range(2):
            mine_n = lax.rem(lax.div(lane, 2), 2 * QUARTERS) == 4 * part + 2 * sub + half
            select_n = jnp.where((ftok_n == token) & mine_n, 1.0, 0.0)
            news_n.append(nn(select_n.astype(BF), rows_n[0]))
        news.append(new + jnp.concatenate(news_n, axis=1))
    live = jnp.sum(select + select_n, axis=1, keepdims=True) > 0.5
    grad_in[0] = jnp.where(live, jnp.concatenate(news, axis=1), base[...].astype(F32)).astype(BF)


def round_scratch(width, mark):
    blocks = 2 * CHIPS * ROWS
    shapes = [(ROWS, width + mark), (blocks, width + mark)] + [(blocks // 2, width)] * 4 + [(ROWS, width), (8 * ROWS, width)]
    return [pltpu.VMEM((HALVES, *dims), BF) for dims in shapes]


def round_sems():
    sem = pltpu.SemaphoreType.DMA
    return [sem((HALVES, n)) for n in (1, NX, 1, 1, NX, NX)] + [sem((HALVES,))] * 4


def on_device(saved_inputs, expert_ids, gate_weights, out_grad, gate_w, up_w, down_w):
    tokens, wg, wu, wd = saved_inputs[0], gate_w[0], up_w[0], down_w[0]
    count, d = tokens.shape
    units = wg.shape[0]
    eighth, sixteenth = d // (2 * QUARTERS), d // (4 * QUARTERS)
    slots = lax.axis_size("ep") * CAP
    ids, gates = expert_ids[0].T, gate_weights[0].T

    hbm = pl.BlockSpec(memory_space=pltpu.HBM)
    smem = pl.BlockSpec(memory_space=pltpu.SMEM)
    sem = pltpu.SemaphoreType.DMA

    def params(which):
        return pltpu.CompilerParams(collective_id=which, has_side_effects=True, vmem_limit_bytes=67043328)

    def vmem_of(shapes):
        return [pltpu.VMEM(x.shape, x.dtype) for x in shapes]

    def shape(*dims, dtype=BF):
        return jax.ShapeDtypeStruct(dims, dtype)

    wide_block, narrow_block, part = shape(HALVES, ROWS, eighth), shape(HALVES, ROWS, sixteenth), shape(slots, units)
    wide_rows, narrow_rows = shape(HALVES, 128, eighth), shape(HALVES, 128, sixteenth)
    coef, select, share, full = shape(slots, units, dtype=F32), shape(ROWS, 128), shape(ROWS, 128, dtype=F32), shape(slots, d)
    weight_shape, trips = shape(units, d), shape(1, dtype=jnp.int32)
    places = [shape(TILES * 128, 128), shape(TILES * 64, 128)]
    wide_stack, narrow_stack = shape(HALVES * TILES * 64, eighth), shape(HALVES * TILES * 128, sixteenth)

    before = [share, wide_block, wide_block, select, coef, coef, part, part, part, part, part]
    after = [share, narrow_block, narrow_block, select, *places]
    ftok_shape = shape(24, 128, dtype=F32)
    (weight, u, base0, select_up, cu, cg, hid, dg1, du1, dg, du, rows, weight_n, un, u0, select_n, place, place_t, rows_n, ftok,
     x, y1, y, base, narrow_trips, wide_trips) = pl.pallas_call(
        first_kernel,
        name="first_rounds",
        out_shape=before + [wide_rows] + after + [narrow_rows, ftok_shape, full, full, full, shape(count, d)]
        + [trips, trips],
        in_specs=[hbm] * 7,
        out_specs=[hbm] * 24 + [smem] * 2,
        scratch_shapes=vmem_of(before + after + [ftok_shape])
        + vmem_of([ids, gates, select, shape(count, d), out_grad, weight_shape, weight_shape, weight_shape,
                   shape(ROWS, 2 * eighth), shape(2 * CHIPS * ROWS, 2 * eighth), full, shape(128, 128), shape(128, 128),
                   shape(128, 128), shape(HALVES, ROWS, eighth, dtype=F32), full, full, wide_stack, narrow_stack,
                   shape(2 * ROWS, 128)])
        + round_scratch(eighth, MARK) + round_scratch(sixteenth, 0)
        + [sem((32,)), sem((1,)), sem((NX,))] + [sem((1,))] * 8 + round_sems() + round_sems(),
        compiler_params=params(0),
    )(ids, gates, tokens, out_grad, wg, wu, wd)

    def more(body, name, which, block, stacked, args, held, stack, mark):
        return tuple(pl.pallas_call(
            body,
            name=name,
            out_shape=[block, part, part, stacked, full],
            in_specs=[hbm] * len(args),
            out_specs=[hbm] * 5,
            input_output_aliases={0: 0},
            scratch_shapes=vmem_of(held + [part, part, full, stack]) + round_scratch(stack.shape[1], mark)
            + [sem((len(args) + 5,))] + round_sems(),
            compiler_params=params(which),
        )(*args))

    def more_narrow(_, state):
        args = (state[0], weight_n, u0, select_n, place, place_t, cu, cg, dg1, du1, y1, wg, wu, wd)
        held = [narrow_block, share, narrow_block, select, *places, coef, coef, part, part, full] + [weight_shape] * 3
        return more(next_narrow, "next_narrow", 1, narrow_block, narrow_rows, args, held, narrow_stack, 0)

    def more_wide(_, state):
        args = (state[0], weight, base0, select_up, cu, cg, wg, wu, wd)
        held = [wide_block, share, wide_block, select, coef, coef] + [weight_shape] * 3
        return more(next_wide, "next_wide", 2, wide_block, wide_rows, args, held, wide_stack, MARK)

    un, dg, du, rows_n, y = lax.fori_loop(0, narrow_trips[0], more_narrow, (un, dg, du, rows_n, y))
    u, dg, du, rows, y = lax.fori_loop(0, wide_trips[0], more_wide, (u, dg, du, rows, y))

    whole = pl.BlockSpec((slots, units), lambda i: (0, 0))
    cols = pl.BlockSpec((slots, 2 * eighth), lambda i: (0, i))
    grad = pl.BlockSpec((1, units, 2 * eighth), lambda i: (0, 0, i))
    return pl.pallas_call(
        last_kernel,
        name="gradients",
        grid=(QUARTERS,),
        out_shape=[shape(1, count, d), shape(1, units, d), shape(1, units, d), shape(1, units, d)],
        in_specs=[whole, whole, whole, cols, cols, pl.BlockSpec((1, 128, eighth), lambda i: (lax.div(i, 2), 0, 0)),
                  pl.BlockSpec((1, 128, sixteenth), lambda i: (lax.div(i, 2), 0, 0)), pl.BlockSpec((24, 128), lambda i: (0, 0)),
                  smem, cols],
        out_specs=[pl.BlockSpec((1, count, 2 * eighth), lambda i: (0, 0, i)), grad, grad, grad],
        scratch_shapes=[pltpu.VMEM((3, units, slots), BF)],
        compiler_params=pltpu.CompilerParams(vmem_limit_bytes=67043328),
    )(dg, du, hid, x, y, rows, rows_n, ftok, wide_trips, base)


def solution(mesh):
    split = P("section", "ep", None)
    return jax.shard_map(
        on_device,
        mesh=mesh,
        in_specs=(split, split, split, P("ep", "section"), split, split, split),
        out_specs=(split, split, split, split),
        check_vma=False,
    )
```

```python
import functools

import jax
import jax.numpy as jnp
from jax import lax
from jax.experimental import pallas as pl
from jax.experimental.pallas import tpu as pltpu
from jax.sharding import PartitionSpec as P

MESH = pl.DeviceIdType.MESH
CAP = 4
NX, NY = 4, 4
CHIPS = NX * NY
SELF = (NX // 2) * NY + NY // 2
Z_ORDER = (4, 3, 5, 2, 6, 1, 7)
QUARTERS = 4
TILES = 2 * CHIPS * CAP // 16
ROWS = QUARTERS * CAP
MARK = 128
HALVES = 2
BF, F32 = jnp.bfloat16, jnp.float32


def iota(shape, dim):
    return lax.broadcasted_iota(jnp.int32, shape, dim)


def rows_at(index, size):
    start = index * size
    return pl.ds(start if isinstance(start, int) else pl.multiple_of(start, size), size)


def swap_matrix():
    i, m = iota((64, 64), 0), iota((64, 64), 1)
    swapped = (lax.rem(lax.div(m, 4), 4) * 16) + (lax.div(m, 16) * 4) + lax.rem(m, 4)
    return jnp.where(i == swapped, 1.0, 0.0).astype(BF)


def nt(a, b):
    return lax.dot_general(a, b, (((1,), (1,)), ((), ())), preferred_element_type=F32)


def nn(a, b):
    return lax.dot_general(a, b, (((1,), (0,)), ((), ())), preferred_element_type=F32)


class Place:
    def __init__(self):
        self.s = lax.axis_index("section")
        self.sections = lax.axis_size("section")
        ep = lax.axis_index("ep")
        self.core = lax.rem(ep, 2)
        self.chip = lax.div(ep, 2)
        self.x = lax.div(self.chip, NY)
        self.y = lax.rem(self.chip, NY)
        self.partner = {"ep": self.chip * 2 + 1 - self.core}

    def ahead(self, k):
        i, j = k // NY + NX // 2, k % NY + NY // 2
        return lax.rem(self.x + i, NX) * NY + lax.rem(self.y + j, NY)

    def behind(self, k):
        i, j = k // NY + NX // 2, k % NY + NY // 2
        return lax.rem(self.x + 2 * NX - i, NX) * NY + lax.rem(self.y + 2 * NY - j, NY)

    def peer(self, chip):
        return {"ep": chip * 2 + self.core}

    def block(self, core, chip):
        return rows_at(core * CHIPS + chip, ROWS)


def remote(src, dst, send, recv, device):
    return pltpu.make_async_remote_copy(
        src_ref=src, dst_ref=dst, send_sem=send, recv_sem=recv, device_id=device, device_id_type=MESH
    )


def each(lo, hi, body):
    lax.fori_loop(lo, hi, lambda k, carry: (body(k), carry)[1], 0)


def each_other(body):
    each(0, SELF, body)
    each(SELF + 1, CHIPS, body)


OTHERS = tuple(k for k in range(CHIPS) if k != SELF)


def unrolled(body):
    for k in OTHERS:
        body(k)


class Gather:
    def __init__(self, at, own, buf, sems):
        self.at, self.own, self.buf = at, own, buf
        self.send, self.recv, self.relay_send, self.relay_recv = sems

    def direct(self, k, block, device):
        return remote(self.own, self.buf.at[block], self.send.at[0], self.recv.at[k // NY], device)

    def relay(self, rows):
        here = self.buf.at[rows]
        return remote(here, here, self.relay_send.at[0], self.relay_recv.at[0], self.at.partner)

    def start(self):
        at = self.at
        mine = at.block(at.core, at.chip)
        self.buf[mine, :] = self.own[...]
        unrolled(lambda k: self.direct(k, mine, at.peer(at.ahead(k))).start())

    def forward(self):
        at = self.at
        for i in range(NX):
            count = (NY - 1 if i == SELF // NY else NY) * ROWS
            some = self.buf.at[pl.ds(0, count)]
            remote(some, some, self.send.at[0], self.recv.at[i], at.partner).wait_recv()
            x = lax.rem(at.x + 2 * NX - (i + NX // 2), NX)
            self.relay(rows_at(at.core * NX + x, NY * ROWS)).start()

    def take(self, expand):
        at = self.at
        each(0, NX, lambda t: expand(at.core * NX + t))
        self.relay(pl.ds(0, CHIPS * ROWS)).wait_recv()
        each(0, NX, lambda t: expand((1 - at.core) * NX + t))

    def drain(self):
        some = self.buf.at[pl.ds(0, (CHIPS - 1) * ROWS)]
        remote(some, some, self.send.at[0], self.recv.at[0], self.at.partner).wait_send()
        self.relay(pl.ds(0, CHIPS * ROWS)).wait_send()


def lay_out(tile, nat, t, first, width):
    rows = tile.shape[0] // ROWS
    for q in range(rows):
        nat[rows_at(t, ROWS), first + q * width : first + (q + 1) * width] = tile[q * ROWS : (q + 1) * ROWS]


class Wide:
    def __init__(self, stack):
        self.stack, self.width = stack, stack.shape[1]

    def expand(self, buf, nat, h, t):
        tile = nn(swap_matrix(), buf[rows_at(t, 64), : self.width]).astype(BF)
        lay_out(tile, nat, t, h * QUARTERS * self.width, self.width)

    def fill(self, h, c, value):
        for t in range(TILES):
            for sub in range(2):
                self.stack[rows_at((h * TILES + t) * QUARTERS + c * 2 + sub, ROWS), :] = value[
                    t * ROWS : (t + 1) * ROWS, sub * self.width : (sub + 1) * self.width
                ]

    def pack(self, h, t):
        return nn(swap_matrix(), self.stack[rows_at(h * TILES + t, 64), :])


class Narrow:
    def __init__(self, stack, place, place_t):
        self.stack, self.width = stack, stack.shape[1]
        self.place, self.place_t = place, place_t

    def expand(self, buf, nat, h, t):
        tile = nn(self.place[rows_at(t, 128), :64], buf[rows_at(t, 64), :]).astype(BF)
        lay_out(tile, nat, t, h * 2 * QUARTERS * self.width, self.width)

    def fill(self, h, c, value):
        for t in range(TILES):
            for sub in range(4):
                self.stack[rows_at((h * TILES + t) * 2 * QUARTERS + c * 4 + sub, ROWS), :] = value[
                    t * ROWS : (t + 1) * ROWS, sub * self.width : (sub + 1) * self.width
                ]

    def pack(self, h, t):
        return nn(self.place_t[rows_at(t, 64), :], self.stack[rows_at(h * TILES + t, 128), :])


def project(nat, weight, width, lo=0, hi=QUARTERS):
    def step(q, acc):
        cols = rows_at(q, width)
        return acc + nt(nat[:, cols], weight[:, cols])

    return lax.fori_loop(lo, hi, step, jnp.zeros((nat.shape[0], weight.shape[0]), F32))


class Round:
    def __init__(self, at, form, bufs, sems, mark):
        self.at, self.form = at, form
        self.yown, self.ybuf, self.pbuf, self.drecv, self.sbuf, self.rbuf, self.rown, self.rstack = bufs
        self.dd_s, self.dd_r, self.rs_s, self.rs_r, self.z_s, self.z_r = sems[4:]
        self.gathers = []
        for h in range(HALVES):
            lanes = pl.ds(0, form.width + (mark if h == 0 else 0))
            self.gathers.append(Gather(at, self.yown.at[h, :, lanes], self.ybuf.at[h, :, lanes], [x.at[h] for x in sems[:4]]))

    def swap_copy(self, h, jj, j):
        part = rows_at(j, 64)
        return remote(self.pbuf.at[h, part], self.drecv.at[h, part], self.dd_s.at[h, jj], self.dd_r.at[h, jj], self.at.partner)

    def all_homes(self, h):
        rows = pl.ds(0, (CHIPS - 1) * ROWS)
        return remote(self.sbuf.at[h, rows], self.rbuf.at[h, rows], self.rs_s.at[h], self.rs_r.at[h], self.at.partner)

    def some_down(self, h, count):
        here = self.rstack.at[h, pl.ds(0, count * ROWS)]
        return remote(here, here, self.z_s.at[h], self.z_r.at[h], {"section": lax.rem(self.at.s + 1, self.at.sections)})

    def home_copy(self, h, k, chip, device):
        return remote(self.sbuf.at[h, rows_at(chip, ROWS)], self.rbuf.at[h, rows_at(k, ROWS)], self.rs_s.at[h],
                      self.rs_r.at[h], device)

    def down_copy(self, h, d, source, device):
        return remote(self.rown.at[h], self.rstack.at[h, rows_at(source, ROWS)], self.z_s.at[h], self.z_r.at[h], device)

    def run(self, upstream, nat, weights, coefs, grads, during_gather=None, before_grads=None, during_sends=None, on_rows=None):
        at, form = self.at, self.form
        wg, wu, wd = weights
        dg, du = grads
        width = wg.shape[1] // QUARTERS
        if during_gather is not None:
            during_gather()
        for gather in self.gathers:
            gather.forward()
        if before_grads is not None:
            before_grads()
        grad_hidden = None
        for h, gather in enumerate(self.gathers):
            gather.take(functools.partial(form.expand, self.ybuf.at[h], nat, h))
            some = project(nat, wd, width, 2 * h, 2 * h + 2)
            grad_hidden = some if h == 0 else grad_hidden + some
        du[...] = (grad_hidden * coefs[0][...]).astype(BF)
        dg[...] = (grad_hidden * coefs[1][...]).astype(BF)

        for h in range(HALVES):

            def back(c):
                cols = rows_at(2 * h + c, width)
                form.fill(h, c, (nn(dg[...], wg[:, cols]) + nn(du[...], wu[:, cols])).astype(BF))

            each(0, 2, back)

            def to_partner(jj):
                j = lax.rem(at.x + jj + NX // 2, NX)
                self.pbuf[h, rows_at(j, 64), :] = form.pack(h, (1 - at.core) * NX + j).astype(BF)
                self.swap_copy(h, jj, j).start()

            for jj in range(NX):
                to_partner(jj)

        for h in range(HALVES):

            def to_homes(jj):
                j = lax.rem(at.x + jj + NX // 2, NX)
                part = rows_at(j, 64)
                mine = form.pack(h, at.core * NX + j)
                self.swap_copy(h, jj, j).wait_recv()
                self.sbuf[h, part, :] = (mine + self.drecv[h, part, :].astype(F32)).astype(BF)

                for m in range(NY):
                    k = jj * NY + m
                    if k != SELF:
                        chip = at.ahead(k)
                        self.home_copy(h, k, chip, at.peer(chip)).start()

            for jj in range(NX):
                to_homes(jj)
        if during_sends is not None:
            during_sends()

        for h in range(HALVES):

            self.all_homes(h).wait_recv()
            total = self.sbuf[h, rows_at(at.chip, ROWS), :].astype(F32)
            for k in OTHERS:
                total = total + self.rbuf[h, rows_at(k, ROWS), :].astype(F32)
            row = (upstream(h) + total).astype(BF)
            self.rown[h] = row
            self.rstack[h, rows_at(at.s, ROWS), :] = row
            for d in Z_ORDER:

                @pl.when(at.s >= d)
                def _():
                    self.down_copy(h, d, at.s, {"section": at.s - d}).start()

        for h in range(HALVES):
            for count in Z_ORDER:

                @pl.when(at.s + count == at.sections - 1)
                def _():
                    self.some_down(h, count).wait_recv()

            if on_rows is not None:
                on_rows(h)

    def drain(self):
        at = self.at
        for h in range(HALVES):
            self.gathers[h].drain()
            each(0, NX, lambda jj: self.swap_copy(h, jj, jj).wait_send())
            self.all_homes(h).wait_send()
            for count in Z_ORDER:

                @pl.when(at.s == count)
                def _():
                    self.some_down(h, count).wait_send()


class Copies:
    def __init__(self, sems):
        self.sems, self.used, self.pending = sems, 0, []

    def start(self, *pairs):
        made = []
        for source, target in pairs:
            made.append(pltpu.make_async_copy(source, target, self.sems.at[self.used]))
            made[-1].start()
            self.used += 1
        self.pending += made
        return made

    def wait(self, made):
        for copy in made:
            copy.wait()
            self.pending.remove(copy)

    def finish(self):
        self.wait(list(self.pending))


def signal_to(device):
    pl.semaphore_signal(pltpu.get_barrier_semaphore(), inc=1, device_id=device, device_id_type=MESH)


def first_kernel(ids_hbm, gates_hbm, tokens_hbm, og_hbm, wg_hbm, wu_hbm, wd_hbm, *refs):
    outs, (narrow_out, wide_out), refs = refs[:24], refs[24:26], refs[26:]
    (w_hbm, u_hbm, base0_hbm, sel_hbm, cu_hbm, cg_hbm, hid_hbm, dg1_hbm, du1_hbm, dg_hbm, du_hbm, r_hbm, wn_hbm, un_hbm, u0_hbm,
     seln_hbm, place_hbm, place_t_hbm, rn_hbm, ftok_hbm, xnat_hbm, y1_hbm, ynat_hbm, base_out) = outs
    (w_ref, u_out, base0_out, sel_out, cu_out, cg_out, hid_out, dg1_out, du1_out, dg_out, du_out, wn_out, un_out, u0_out,
     seln_out, place, place_t, ftok_out) = refs[:18]
    (ids_ref, gates_ref, tok_ref, tokv, ogv, wg, wu, wd, xown, xbuf, xnat, tokall, psend, precv, base, ynat1, ynat, stack, stackn,
     selw) = refs[18:38]
    wide_bufs, narrow_bufs, refs = refs[38:46], refs[46:54], refs[54:]
    loc, x_s, x_r, xrel_s, xrel_r, id_s, id_r, pc_s, pc_r, bs_s, bs_r = refs[:11]
    at = Place()
    s, sections = at.s, at.sections
    half = ogv.shape[1]
    width = 2 * half
    wide = Round(at, Wide(stack), wide_bufs, refs[11:21], MARK)
    narrow = Round(at, Narrow(stackn, place, place_t), narrow_bufs, refs[21:31], 0)
    x_gather = Gather(at, xown, xbuf, (x_s, x_r, xrel_s, xrel_r))
    local = Copies(loc)
    load_ids = local.start((ids_hbm, ids_ref), (gates_hbm, gates_ref))
    load_tokens = local.start((tokens_hbm, tokv))
    load_og = local.start((og_hbm, ogv))
    load_gu = local.start((wg_hbm, wg), (wu_hbm, wu))
    load_d = local.start((wd_hbm, wd))

    for received in (wide.rstack, narrow.rstack):
        received[...] = jnp.zeros_like(received)

    def greet(k):
        signal_to(at.peer(at.ahead(k)))

    each_other(greet)
    signal_to(at.partner)

    def greet_z(d):
        signal_to({"section": lax.rem(s + d, sections)})

    each(1, sections, greet_z)

    local.wait(load_ids)
    hits = ids_ref[...] == 0
    live = jnp.sum(jnp.where(hits, 1.0, 0.0), axis=0, keepdims=True)
    pair_weight = jnp.sum(jnp.where(hits, gates_ref[...], 0.0), axis=0, keepdims=True)
    before = jnp.where(iota((128, 128), 0) < iota((128, 128), 1), 1.0, 0.0).astype(BF)
    live16 = jnp.broadcast_to(live, (ROWS, 128))
    slot = nn(live16.astype(BF), before)
    lane16, row16 = iota((ROWS, 128), 1), iota((ROWS, 128), 0)
    mine16 = (live16 > 0.5) & (slot == lax.rem(row16, CAP).astype(F32))
    token = jnp.max(jnp.where(mine16, lane16.astype(F32), -1.0), axis=1, keepdims=True)
    tok_ref[...] = jnp.broadcast_to(token, (ROWS, 128)).astype(BF)
    share = jnp.sum(jnp.where(mine16, jnp.broadcast_to(pair_weight, (ROWS, 128)), 0.0), axis=1, keepdims=True)
    w_ref[...] = jnp.broadcast_to(share, (ROWS, 128))

    mine_z = rows_at(s, ROWS)
    pl.semaphore_wait(pltpu.get_barrier_semaphore(), CHIPS + sections - 1)

    def send_ids(d):
        remote(tok_ref, tokall.at[mine_z], id_s.at[0], id_r.at[0], {"section": lax.rem(s + d, sections)}).start()

    for d in Z_ORDER:
        send_ids(d)
    tokall[mine_z, :] = tok_ref[...]

    local.wait(load_tokens)
    hit = token == lane16.astype(F32)
    block = jnp.zeros((ROWS, width), F32)
    for q in range(QUARTERS):
        select = jnp.where(hit & (lax.div(row16, CAP) == q), 1.0, 0.0).astype(BF)
        block = block + nn(select, tokv[:, q * width : (q + 1) * width])
    xown[...] = block.astype(BF)
    x_gather.start()

    local.wait(load_og)

    others = (sections - 1) * ROWS

    def all_ids():
        some = tokall.at[pl.ds(0, others)]
        return remote(some, some, id_s.at[0], id_r.at[0], at.partner)

    def all_pieces():
        some = precv.at[pl.ds(0, others)]
        return remote(some, some, pc_s.at[0], pc_r.at[0], at.partner)

    def all_base():
        some = base_out.at[:, pl.ds(0, (sections - 1) * half)]
        return remote(some, some, bs_s.at[0], bs_r.at[0], at.partner)

    all_ids().wait_recv()
    tok_f = tokall[...].astype(F32)
    row, lane = iota((128, 128), 0), iota((128, 128), 1)
    for_slot = tok_f == lane.astype(F32)
    pieces = jnp.zeros((128, 128), F32)
    for u in range(half // 128):
        pick = jnp.where(for_slot & (lax.rem(lax.div(row, CAP), QUARTERS) == u), 1.0, 0.0).astype(BF)
        pieces = pieces + nn(pick, ogv[:, u * 128 : (u + 1) * 128])
    psend[...] = pieces.astype(BF)

    def send_piece(d):
        to = lax.rem(s + d, sections)
        remote(psend.at[rows_at(to, ROWS)], precv.at[mine_z], pc_s.at[0], pc_r.at[0], {"section": to}).start()

    for d in Z_ORDER:
        send_piece(d)
    precv[mine_z, :] = psend[mine_z, :]

    other = tok_f.T
    layer_r, layer_l = lax.div(row, ROWS), lax.div(lane, ROWS)
    part_r, part_l = lax.rem(lax.div(row, CAP), QUARTERS), lax.rem(lax.div(lane, CAP), QUARTERS)
    same = (tok_f == other) & (tok_f >= 0.0) & (part_r == part_l)
    above = jnp.where(same & (layer_l > layer_r), 1.0, 0.0)
    level_r = jnp.sum(above, axis=1, keepdims=True)
    level_l = jnp.sum(jnp.where(same & (layer_r > layer_l), 1.0, 0.0), axis=0, keepdims=True)
    dep_r, dep_l = level_r > 0.5, level_l > 0.5
    group = lax.div(row, CAP) == lax.div(lane, CAP)
    fellows = jnp.where(group & dep_l, 1.0, 0.0)
    busiest = jnp.max(jnp.sum(fellows, axis=1, keepdims=True), axis=0, keepdims=True)
    deepest = jnp.max(level_r, axis=0, keepdims=True)
    j_r = jnp.where(dep_r, jnp.sum(jnp.where(lane < row, fellows, 0.0), axis=1, keepdims=True), -1.0)
    take = jnp.where(lane16 == row16 + s * ROWS, 1.0, 0.0).astype(BF)
    level_own = nn(take, jnp.broadcast_to(level_r, (128, 128)).astype(BF))
    j_own = nn(take, jnp.broadcast_to(j_r, (128, 128)).astype(BF))

    all_pieces().wait_recv()
    root = level_own[:, :1] < 0.5
    weight = w_ref[:, :1]
    marks = jnp.where(lane16 < 32, deepest, jnp.where(lane16 < 64, busiest, j_own))
    wide.yown[0, :, half:] = marks.astype(BF)
    for h in range(HALVES):
        for u in range(half // 128):
            source = (lax.div(lane16, ROWS) == h * QUARTERS + lax.div(row16, CAP)) & (
                lax.rem(lax.div(lane16, CAP), QUARTERS) == u)
            pick = jnp.where(source & (lax.rem(lane16, CAP) == lax.rem(row16, CAP)), 1.0, 0.0).astype(BF)
            base[h, :, u * 128 : (u + 1) * 128] = nn(pick, precv[...])
        wide.yown[h, :, :half] = jnp.where(root, weight * base[h], 0.0).astype(BF)
        wide.gathers[h].start()

    def send_base(steps):
        for d in steps:
            to = lax.rem(s + d, sections)
            remote(ogv, base_out.at[:, rows_at(s, half)], bs_s.at[0], bs_r.at[0], {"section": to}).start()

    def tables():
        for h in range(HALVES):
            base0_out[h] = jnp.where(root, base[h], 0.0).astype(BF)
        chosen = jnp.where(level_l == level_r - 1.0, above, 0.0).astype(BF)
        sel_out[...] = nn(take, chosen).astype(BF)
        j_l = jnp.where(dep_l, jnp.sum(jnp.where(group & dep_r & (row < lane), 1.0, 0.0), axis=0, keepdims=True), -1.0)
        own = (lax.div(lane16, ROWS) == s) & (lax.div(row16, 4) == lax.rem(lax.div(lane16, CAP), QUARTERS))
        own = jnp.where(own & (j_l == lax.rem(row16, 2).astype(F32)), 1.0, 0.0).astype(BF)
        token_n = nn(own, (tok_f + 1.0).astype(BF)) - 1.0
        share_n = jnp.sum(jnp.where(token_n == lane16.astype(F32), jnp.broadcast_to(pair_weight, (ROWS, 128)), 0.0),
                          axis=1, keepdims=True)
        wn_out[...] = jnp.broadcast_to(share_n, (ROWS, 128))
        onto = nn(own, chosen)
        for h in range(2):
            from_wide = (lax.rem(lax.div(row16, 2), 2) == h) & (level_l < 0.5)
            selw[h * ROWS : (h + 1) * ROWS, :] = jnp.where(from_wide, onto, 0.0).astype(BF)
        shrink = (layer_r == layer_l) & (part_r == lax.div(lax.rem(lane, ROWS), 4)) & (j_r == lax.rem(lane, 2).astype(F32))
        shrink = jnp.where(shrink, 1.0, 0.0).astype(BF)
        eighth = lax.div(row16, 2) == lax.div(lax.rem(lane16, ROWS), 2)
        seln_out[...] = jnp.where(eighth, nn(onto.astype(BF), shrink), 0.0).astype(BF)
        later = jnp.sum(jnp.where(same & (layer_r < layer_l) & (layer_r >= s), 1.0, 0.0), axis=0, keepdims=True)
        lane1 = iota((1, 128), 1)
        tok_l = jnp.max(other, axis=0, keepdims=True)
        ftok = jnp.where((later < 0.5) & (lax.div(lane1, ROWS) >= s), tok_l, -1.0)
        ftok_n = nn(jnp.broadcast_to(jnp.where(dep_l, ftok + 1.0, 0.0), (ROWS, 128)).astype(BF), shrink) - 1.0
        ftok_out[0:8, :] = jnp.broadcast_to(ftok, (8, 128))
        ftok_out[8:16, :] = jnp.broadcast_to(jnp.where(dep_l, -1.0, ftok), (8, 128))
        ftok_out[16:24, :] = ftok_n[:8]

    def expand_x(t):
        lay_out(nn(swap_matrix(), xbuf[rows_at(t, 64), :]).astype(BF), xnat, t, 0, width)

    def activations():
        send_base(Z_ORDER)
        local.start((ogv, base_out.at[:, rows_at(s, half)]))
        tables()
        local.start((w_ref, w_hbm), (base0_out, base0_hbm), (sel_out, sel_hbm), (wn_out, wn_hbm), (seln_out, seln_hbm),
                    (ftok_out, ftok_hbm))
        x_gather.forward()
        x_gather.take(expand_x)
        local.start((xnat, xnat_hbm))
        local.wait(load_gu)
        gate = project(xnat, wg, width)
        up = project(xnat, wu, width)
        sig = 1.0 / (1.0 + jnp.exp(-gate))
        act = gate * sig
        hid_out[...] = (act * up).astype(BF)
        cu_out[...] = act
        cg_out[...] = up * sig * (1.0 + gate * (1.0 - sig))
        local.start((hid_out, hid_hbm), (cu_out, cu_hbm), (cg_out, cg_hbm))

    def places():
        all_marks = wide.ybuf[0, :, half:].astype(F32)
        lanes = iota(all_marks.shape, 1)
        depth = jnp.max(jnp.where(lanes < 32, all_marks, 0.0)).astype(jnp.int32)
        most = jnp.max(jnp.where((lanes >= 32) & (lanes < 64), all_marks, 0.0)).astype(jnp.int32)
        narrow_out[0] = jnp.where(most > 2, 0, depth - 1)
        wide_out[0] = jnp.where(most > 2, depth, 0)
        r64, c64 = iota((128, 64), 0), iota((128, 64), 1)
        slot_of = (lax.rem(lax.div(r64, 4), 4) == lax.div(c64, ROWS)) & (lax.rem(r64, 4) == lax.rem(c64, ROWS))
        slot_of = jnp.where(slot_of, 1.0, 0.0).astype(BF)
        fits = (lax.rem(lax.div(row, 4), 4) == lax.div(lane, ROWS)) & (lax.div(row, ROWS) == lax.rem(lax.div(lane, 2), 8))

        def one(t):
            slots = nn(slot_of, wide.ybuf[0, rows_at(t, 64), half:])
            e = jnp.where(fits & (slots[:, MARK - 1 :] == lax.rem(lane, 2).astype(F32)), 1.0, 0.0)
            place[rows_at(t, 128), :] = e.astype(BF)
            place_t[rows_at(t, 64), :] = e.T[:64].astype(BF)

        each(0, TILES, one)
        local.start((ynat1, y1_hbm), (place, place_hbm), (place_t, place_t_hbm), (dg1_out, dg1_hbm), (du1_out, du1_hbm))

    def first_narrow(h):
        start = jnp.zeros((ROWS, half // 2), F32)
        parts = []
        for sub in range(2):
            parts.append(nn(selw[sub * ROWS : (sub + 1) * ROWS, :], wide.rstack[h, :, sub * half // 2 : (sub + 1) * half // 2]))
        start = parts[0] + parts[1]
        u0_out[h] = start.astype(BF)
        narrow.yown[h] = (wn_out[:, :1] * start).astype(BF)
        narrow.gathers[h].start()

    weights, coefs = (wg, wu, wd), (cu_out, cg_out)
    wide.run(lambda h: base[h], ynat1, weights, coefs, (dg1_out, du1_out), during_gather=activations,
             before_grads=lambda: local.wait(load_d), during_sends=places, on_rows=first_narrow)

    def rest_of_wide():
        for h in range(HALVES):
            u_out[h] = (nn(sel_out[...], wide.rstack[h]) + base0_out[h].astype(F32)).astype(BF)
        local.start((u_out, u_hbm), (u0_out, u0_hbm), (wide.rstack, r_hbm))

    def add_up():
        for total, first in ((dg_out, dg1_out), (du_out, du1_out), (ynat, ynat1)):
            total[...] = total[...] + first[...]
        local.start((dg_out, dg_hbm), (du_out, du_hbm), (ynat, ynat_hbm))

    def follow(h):
        un_out[h] = (nn(seln_out[...], narrow.rstack[h]) + u0_out[h].astype(F32)).astype(BF)

    narrow.run(lambda h: u0_out[h].astype(F32), ynat, weights, coefs, (dg_out, du_out),
               during_gather=rest_of_wide, during_sends=add_up, on_rows=follow)
    local.start((un_out, un_hbm), (narrow.rstack, rn_hbm))

    x_gather.drain()

    all_ids().wait_send()
    all_pieces().wait_send()
    all_base().wait_send()
    all_base().wait_recv()
    wide.drain()
    narrow.drain()
    local.finish()


def enter_round(at, rstack):
    rstack[...] = jnp.zeros_like(rstack)
    each_other(lambda k: signal_to(at.peer(at.ahead(k))))
    signal_to(at.partner)

    def greet_z(d):
        @pl.when(at.s + d < at.sections)
        def _():
            signal_to({"section": at.s + d})

    each(1, at.sections, greet_z)


def next_wide(*refs):
    ins, outs, refs = refs[:9], refs[9:14], refs[14:]
    held, (dg, du, ynat, stack), bufs, loc, sems = refs[:9], refs[9:13], refs[13:21], refs[21], refs[22:]
    u_ref, w_ref, base0_ref, sel_ref, cu_ref, cg_ref, wg, wu, wd = held
    u_hbm, dg_hbm, du_hbm, r_hbm, ynat_hbm = outs
    at = Place()
    half = u_ref.shape[2]
    this = Round(at, Wide(stack), bufs, sems, MARK)
    local = Copies(loc)
    first = local.start(*zip(ins[:2], held[:2]))
    others = local.start(*zip(ins[2:], held[2:]))
    enter_round(at, this.rstack)
    local.wait(first)
    this.yown[0, :, half:] = jnp.zeros((ROWS, MARK), BF)
    for h in range(HALVES):
        this.yown[h, :, :half] = (w_ref[:, :1] * u_ref[h].astype(F32)).astype(BF)
    pl.semaphore_wait(pltpu.get_barrier_semaphore(), CHIPS + at.s)
    for gather in this.gathers:
        gather.start()

    def put():
        local.start((dg, dg_hbm), (du, du_hbm), (ynat, ynat_hbm))

    def follow(h):
        u_ref[h] = (nn(sel_ref[...], this.rstack[h]) + base0_ref[h].astype(F32)).astype(BF)

    this.run(lambda h: u_ref[h].astype(F32), ynat, (wg, wu, wd), (cu_ref, cg_ref), (dg, du),
             during_gather=lambda: local.wait(others), during_sends=put, on_rows=follow)
    local.start((u_ref, u_hbm), (this.rstack, r_hbm))
    this.drain()
    local.finish()


def next_narrow(*refs):
    ins, outs, refs = refs[:14], refs[14:19], refs[19:]
    held, (dg, du, ynat, stack), bufs, loc, sems = refs[:14], refs[14:18], refs[18:26], refs[26], refs[27:]
    u_ref, w_ref, u0_ref, sel_ref, place, place_t, cu_ref, cg_ref, dg1, du1, y1, wg, wu, wd = held
    u_hbm, dg_hbm, du_hbm, r_hbm, ynat_hbm = outs
    at = Place()
    this = Round(at, Narrow(stack, place, place_t), bufs, sems, 0)
    local = Copies(loc)
    first = local.start(*zip(ins[:2], held[:2]))
    others = local.start(*zip(ins[2:], held[2:]))
    enter_round(at, this.rstack)
    local.wait(first)
    for h in range(HALVES):
        this.yown[h] = (w_ref[:, :1] * u_ref[h].astype(F32)).astype(BF)
    pl.semaphore_wait(pltpu.get_barrier_semaphore(), CHIPS + at.s)
    for gather in this.gathers:
        gather.start()

    def add_up():
        for total, one in ((dg, dg1), (du, du1), (ynat, y1)):
            total[...] = total[...] + one[...]
        local.start((dg, dg_hbm), (du, du_hbm), (ynat, ynat_hbm))

    def follow(h):
        u_ref[h] = (nn(sel_ref[...], this.rstack[h]) + u0_ref[h].astype(F32)).astype(BF)

    this.run(lambda h: u_ref[h].astype(F32), ynat, (wg, wu, wd), (cu_ref, cg_ref), (dg, du),
             during_gather=lambda: local.wait(others), during_sends=add_up, on_rows=follow)
    local.start((u_ref, u_hbm), (this.rstack, r_hbm))
    this.drain()
    local.finish()


def last_kernel(*refs):
    ins, wide_trips, outs, refs = refs[:9], refs[9], refs[10:14], refs[14:]
    dg, du, hid, ftok, rows, rows_n, x, y, base, grad_in, grad_gate, grad_up, grad_down, sems = refs
    count, d = base.shape
    width = d // QUARTERS
    local = Copies(sems)
    small = local.start(*zip(ins[:3], (dg, du, hid)))
    loads = []
    for q in range(QUARTERS):
        cols = slice(q * width, (q + 1) * width)
        loads.append([local.start((ins[i].at[:, cols], held.at[:, cols])) for i, held in ((6, x), (7, y))])
    rest = local.start(*zip(ins[3:6], (ftok, rows, rows_n)), (ins[8], base))

    slots = dg.shape[0]
    unit = jnp.where(iota((slots, slots), 0) == iota((slots, slots), 1), 1.0, 0.0).astype(BF)

    def across(part):
        return lax.dot_general(part[...], unit, (((0,), (0,)), ((), ())), preferred_element_type=F32).astype(BF)

    local.wait(small)
    gate_t, up_t, hid_t = across(dg), across(du), across(hid)
    for q in range(QUARTERS):
        cols = slice(q * width, (q + 1) * width)
        local.wait(loads[q][0])
        grad_gate[:, cols] = nn(gate_t, x[:, cols]).astype(BF)
        local.start((grad_gate.at[:, cols], outs[1].at[0, :, cols]))
        grad_up[:, cols] = nn(up_t, x[:, cols]).astype(BF)
        local.start((grad_up.at[:, cols], outs[2].at[0, :, cols]))
        local.wait(loads[q][1])
        grad_down[:, cols] = nn(hid_t, y[:, cols]).astype(BF)
        local.start((grad_down.at[:, cols], outs[3].at[0, :, cols]))

    local.wait(rest)
    lane, token = iota((count, 128), 1), iota((count, 128), 0).astype(F32)
    wide_only = wide_trips[0] > 0
    ftok_w = jnp.where(wide_only, ftok[0:1, :], ftok[8:9, :])
    ftok_n = jnp.where(wide_only, -1.0, ftok[16:17, :])
    hit_w, hit_n = ftok_w == token, ftok_n == token
    for h in range(HALVES):
        for p in range(QUARTERS):
            select = jnp.where(hit_w & (lax.rem(lax.div(lane, CAP), QUARTERS) == p), 1.0, 0.0)
            new = nn(select.astype(BF), rows[h])
            news_n = []
            for sub in range(2):
                select_n = jnp.where(hit_n & (lax.rem(lax.div(lane, 2), 2 * QUARTERS) == 2 * p + sub), 1.0, 0.0)
                news_n.append(nn(select_n.astype(BF), rows_n[h]))
            live = jnp.sum(select + select_n, axis=1, keepdims=True) > 0.5
            at = (h * QUARTERS + p) * width // 2
            cols = slice(at, at + width // 2)
            new = new + jnp.concatenate(news_n, axis=1)
            grad_in[:, cols] = jnp.where(live, new, base[:, cols].astype(F32)).astype(BF)
        cols = slice(h * d // 2, (h + 1) * d // 2)
        local.start((grad_in.at[:, cols], outs[0].at[0, :, cols]))
    local.finish()


def round_scratch(width, mark):
    blocks = 2 * CHIPS * ROWS
    shapes = [(ROWS, width + mark), (blocks, width + mark)] + [(blocks // 2, width)] * 4 + [(ROWS, width), (8 * ROWS, width)]
    return [pltpu.VMEM((HALVES, *dims), BF) for dims in shapes]


def round_sems():
    sem = pltpu.SemaphoreType.DMA
    return [sem((HALVES, n)) for n in (1, NX, 1, 1, NX, NX)] + [sem((HALVES,))] * 4


def on_device(saved_inputs, expert_ids, gate_weights, out_grad, gate_w, up_w, down_w):
    tokens, wg, wu, wd = saved_inputs[0], gate_w[0], up_w[0], down_w[0]
    count, d = tokens.shape
    units = wg.shape[0]
    eighth, sixteenth = d // (2 * QUARTERS), d // (4 * QUARTERS)
    slots = lax.axis_size("ep") * CAP
    ids, gates = expert_ids[0].T, gate_weights[0].T

    hbm = pl.BlockSpec(memory_space=pltpu.HBM)
    smem = pl.BlockSpec(memory_space=pltpu.SMEM)
    sem = pltpu.SemaphoreType.DMA

    def params(which):
        return pltpu.CompilerParams(collective_id=which, has_side_effects=True, vmem_limit_bytes=67043328)

    def vmem_of(shapes):
        return [pltpu.VMEM(x.shape, x.dtype) for x in shapes]

    def shape(*dims, dtype=BF):
        return jax.ShapeDtypeStruct(dims, dtype)

    wide_block, narrow_block, part = shape(HALVES, ROWS, eighth), shape(HALVES, ROWS, sixteenth), shape(slots, units)
    wide_rows, narrow_rows = shape(HALVES, 128, eighth), shape(HALVES, 128, sixteenth)
    coef, select, share, full = shape(slots, units, dtype=F32), shape(ROWS, 128), shape(ROWS, 128, dtype=F32), shape(slots, d)
    weight_shape, trips = shape(units, d), shape(1, dtype=jnp.int32)
    places = [shape(TILES * 128, 128), shape(TILES * 64, 128)]
    wide_stack, narrow_stack = shape(HALVES * TILES * 64, eighth), shape(HALVES * TILES * 128, sixteenth)

    before = [share, wide_block, wide_block, select, coef, coef, part, part, part, part, part]
    after = [share, narrow_block, narrow_block, select, *places]
    ftok_shape = shape(24, 128, dtype=F32)
    (weight, u, base0, select_up, cu, cg, hid, dg1, du1, dg, du, rows, weight_n, un, u0, select_n, place, place_t, rows_n, ftok,
     x, y1, y, base, narrow_trips, wide_trips) = pl.pallas_call(
        first_kernel,
        name="first_rounds",
        out_shape=before + [wide_rows] + after + [narrow_rows, ftok_shape, full, full, full, shape(count, d)]
        + [trips, trips],
        in_specs=[hbm] * 7,
        out_specs=[hbm] * 24 + [smem] * 2,
        scratch_shapes=vmem_of(before + after + [ftok_shape])
        + vmem_of([ids, gates, select, shape(count, d), out_grad, weight_shape, weight_shape, weight_shape,
                   shape(ROWS, 2 * eighth), shape(2 * CHIPS * ROWS, 2 * eighth), full, shape(128, 128), shape(128, 128),
                   shape(128, 128), shape(HALVES, ROWS, eighth, dtype=F32), full, full, wide_stack, narrow_stack,
                   shape(2 * ROWS, 128)])
        + round_scratch(eighth, MARK) + round_scratch(sixteenth, 0)
        + [sem((32,)), sem((1,)), sem((NX,))] + [sem((1,))] * 8 + round_sems() + round_sems(),
        compiler_params=params(0),
    )(ids, gates, tokens, out_grad, wg, wu, wd)

    def more(body, name, which, block, stacked, args, held, stack, mark):
        return tuple(pl.pallas_call(
            body,
            name=name,
            out_shape=[block, part, part, stacked, full],
            in_specs=[hbm] * len(args),
            out_specs=[hbm] * 5,
            input_output_aliases={0: 0},
            scratch_shapes=vmem_of(held + [part, part, full, stack]) + round_scratch(stack.shape[1], mark)
            + [sem((len(args) + 5,))] + round_sems(),
            compiler_params=params(which),
        )(*args))

    def more_narrow(_, state):
        args = (state[0], weight_n, u0, select_n, place, place_t, cu, cg, dg1, du1, y1, wg, wu, wd)
        held = [narrow_block, share, narrow_block, select, *places, coef, coef, part, part, full] + [weight_shape] * 3
        return more(next_narrow, "next_narrow", 1, narrow_block, narrow_rows, args, held, narrow_stack, 0)

    def more_wide(_, state):
        args = (state[0], weight, base0, select_up, cu, cg, wg, wu, wd)
        held = [wide_block, share, wide_block, select, coef, coef] + [weight_shape] * 3
        return more(next_wide, "next_wide", 2, wide_block, wide_rows, args, held, wide_stack, MARK)

    un, dg, du, rows_n, y = lax.fori_loop(0, narrow_trips[0], more_narrow, (un, dg, du, rows_n, y))
    u, dg, du, rows, y = lax.fori_loop(0, wide_trips[0], more_wide, (u, dg, du, rows, y))

    tokens_shape = shape(count, d)
    return pl.pallas_call(
        last_kernel,
        name="gradients",
        out_shape=[shape(1, count, d), shape(1, units, d), shape(1, units, d), shape(1, units, d)],
        in_specs=[hbm] * 9 + [smem],
        out_specs=[hbm] * 4,
        scratch_shapes=vmem_of([part, part, part, ftok_shape, wide_rows, narrow_rows, full, full, tokens_shape, tokens_shape,
                                weight_shape, weight_shape, weight_shape]) + [sem((2 * QUARTERS + 3 * QUARTERS + 9,))],
        compiler_params=pltpu.CompilerParams(vmem_limit_bytes=67043328),
    )(dg, du, hid, ftok, rows, rows_n, x, y, base, wide_trips)


def solution(mesh):
    split = P("section", "ep", None)
    return jax.shard_map(
        on_device,
        mesh=mesh,
        in_specs=(split, split, split, P("ep", "section"), split, split, split),
        out_specs=(split, split, split, split),
        check_vma=False,
    )
```
